128 devices in a mesh: dp: 128 (over z, y, x, core).
Axes of the slice: x: 4, y: 4, z: 4, core: 2. Of those that a mesh axis runs over, the one named last changes fastest.
Arguments:
- features: bfloat16 [8192, 256], P('dp')
- w_in: bfloat16 [256, 1024], replicated
- w_out: bfloat16 [1024, 128], replicated
- item_table: bfloat16 [1048576, 128], P('dp')
- cand_ids: int32 [131072], replicated
- log_q: float32 [131072], replicated
- targets: int32 [8192], P('dp')
Outputs:
- output 1: float32 [], replicated
- output 2: float32 [1048576, 128], P('dp')
- output 3: float32 [256, 1024], replicated
- output 4: float32 [1024, 128], replicated
All inputs are finite; a program needn't handle non-finite values.
Results may differ from the reference program's by a relative error of at most 0.001.
Values are sent between devices in bfloat16 or wider.
A program may use at most 1 GiB of HBM per device.

```python
import jax
import jax.numpy as jnp
from jax import lax

IN_DIM = 256
HID_DIM = 1024
EMB_DIM = 128
NUM_ITEMS = 1048576
GROUPS = 128
TOK_DEV = 64
CAND_DEV = 1024
TOKENS = 8192
NUM_CANDS = 131072
BLOCK_ROWS = 8192


def draw_ids(id_key):
    key_perm, key_blk_a, key_blk_b, key_hit, key_row = jax.random.split(id_key, 5)
    perm_keys = jax.random.split(key_perm, GROUPS)
    local_rows = jax.vmap(lambda perm_key: jax.random.permutation(perm_key, BLOCK_ROWS)[:CAND_DEV])(perm_keys)
    block_base = BLOCK_ROWS * jnp.arange(GROUPS, dtype=jnp.int32)
    cand_ids = (local_rows.astype(jnp.int32) + block_base[:, None]).reshape(NUM_CANDS)
    tok_pos = jnp.arange(TOKENS, dtype=jnp.int32)
    skew_block = jnp.minimum(jax.random.randint(key_blk_a, (TOKENS,), 0, GROUPS), jax.random.randint(key_blk_b, (TOKENS,), 0, GROUPS))
    owner_block = jnp.where(tok_pos < GROUPS, tok_pos, skew_block)
    hit_slot = owner_block * CAND_DEV + jax.random.randint(key_hit, (TOKENS,), 0, CAND_DEV)
    row_pair = jax.random.randint(key_row, (2, TOKENS), 0, BLOCK_ROWS)
    plain_row = owner_block * BLOCK_ROWS + jnp.minimum(row_pair[0], row_pair[1])
    targets = jnp.where(tok_pos % 4 == 1, cand_ids[hit_slot], plain_row)
    return cand_ids, targets.astype(jnp.int32)


def setup_inputs(seed: int = 0) -> dict:
    root_key = jax.random.key(seed)
    key_x, key_w1, key_w2, key_tab, key_lq, key_ids = jax.random.split(root_key, 6)
    cand_ids, targets = draw_ids(key_ids)
    features = jax.random.normal(key_x, (TOKENS, IN_DIM), jnp.float32).astype(jnp.bfloat16)
    w_in = (jax.random.normal(key_w1, (IN_DIM, HID_DIM), jnp.float32) * IN_DIM ** -0.5).astype(jnp.bfloat16)
    w_out = (jax.random.normal(key_w2, (HID_DIM, EMB_DIM), jnp.float32) * HID_DIM ** -0.5).astype(jnp.bfloat16)
    item_table = (jax.random.normal(key_tab, (NUM_ITEMS, EMB_DIM), jnp.float32) * (2.0 * EMB_DIM ** -0.5)).astype(jnp.bfloat16)
    log_q = jax.random.uniform(key_lq, (NUM_CANDS,), jnp.float32, -4.0, 0.0)
    return {"features": features, "w_in": w_in, "w_out": w_out, "item_table": item_table, "cand_ids": cand_ids, "log_q": log_q, "targets": targets}


def reference(features, w_in, w_out, item_table, cand_ids, log_q, targets):
    cand_rows = item_table[cand_ids]
    feat_blocks = features.reshape(GROUPS, TOK_DEV, IN_DIM)
    tgt_blocks = targets.reshape(GROUPS, TOK_DEV)

    def block_step(carry, block_in):
        grad_cand, grad_w_in, grad_w_out, loss_sum = carry
        feat_blk, tgt_blk = block_in
        pre_act = jnp.dot(feat_blk, w_in, preferred_element_type=jnp.float32)
        act_val, gelu_back = jax.vjp(jax.nn.gelu, pre_act)
        act_b = act_val.astype(jnp.bfloat16)
        query = jnp.dot(act_b, w_out, preferred_element_type=jnp.float32).astype(jnp.bfloat16)
        query_f = query.astype(jnp.float32)
        tgt_rows = item_table[tgt_blk].astype(jnp.float32)
        tgt_logit = jnp.sum(query_f * tgt_rows, axis=1)
        cand_logit = jnp.dot(query, cand_rows.T, preferred_element_type=jnp.float32) - log_q[None, :]
        cand_logit = jnp.where(cand_ids[None, :] == tgt_blk[:, None], -1e9, cand_logit)
        top_val = jnp.maximum(jnp.max(cand_logit, axis=1), tgt_logit)
        exp_sum = jnp.sum(jnp.exp(cand_logit - top_val[:, None]), axis=1) + jnp.exp(tgt_logit - top_val)
        log_norm = top_val + jnp.log(exp_sum)
        grad_tgt = (jnp.exp(tgt_logit - log_norm) - 1.0) / TOKENS
        cand_grad = (jnp.exp(cand_logit - log_norm[:, None]) / TOKENS).astype(jnp.bfloat16)
        d_query = (grad_tgt[:, None] * tgt_rows + jnp.dot(cand_grad, cand_rows, preferred_element_type=jnp.float32)).astype(jnp.bfloat16)
        d_act = jnp.dot(d_query, w_out.T, preferred_element_type=jnp.float32)
        d_pre = gelu_back(d_act)[0].astype(jnp.bfloat16)
        grad_cand = grad_cand + jnp.dot(cand_grad.T, query, preferred_element_type=jnp.float32)
        grad_w_in = grad_w_in + jnp.dot(feat_blk.T, d_pre, preferred_element_type=jnp.float32)
        grad_w_out = grad_w_out + jnp.dot(act_b.T, d_query, preferred_element_type=jnp.float32)
        loss_sum = loss_sum + jnp.sum(log_norm - tgt_logit)
        return (grad_cand, grad_w_in, grad_w_out, loss_sum), grad_tgt[:, None] * query_f

    start_carry = (jnp.zeros((NUM_CANDS, EMB_DIM), jnp.float32), jnp.zeros((IN_DIM, HID_DIM), jnp.float32), jnp.zeros((HID_DIM, EMB_DIM), jnp.float32), jnp.zeros((), jnp.float32))
    end_carry, tgt_grad = lax.scan(block_step, start_carry, (feat_blocks, tgt_blocks))
    grad_cand, grad_w_in, grad_w_out, loss_sum = end_carry
    grad_table = jnp.zeros((NUM_ITEMS, EMB_DIM), jnp.float32).at[cand_ids].add(grad_cand).at[targets].add(tgt_grad.reshape(TOKENS, EMB_DIM))
    return loss_sum / TOKENS, grad_table, grad_w_in, grad_w_out
```

```python
import functools
import jax
import jax.numpy as jnp
from jax import lax
from jax.experimental import pallas as pl
from jax.experimental.pallas import tpu as pltpu
from jax.sharding import PartitionSpec as P

MESH = pl.DeviceIdType.MESH
F32, BF16 = jnp.float32, jnp.bfloat16
COORD = {"core": (1, 2), "x": (2, 4), "y": (8, 4), "z": (32, 4)}
ORDERS = (("x", "y", "z"), ("y", "z", "x"), ("z", "x", "y"))
NDEV = 128
NPEER = 10


def coord(me, axis):
    stride, radix = COORD[axis]
    return (me // stride) % radix


def peer(me, axis, k):
    stride, radix = COORD[axis]
    c = coord(me, axis)
    return me + ((c + k) % radix - c) * stride


def block_index(me, order):
    idx, weight = 0, 1
    for axis in order:
        idx = idx + coord(me, axis) * weight
        weight *= COORD[axis][1]
    return idx


def entry_barrier(me):
    barrier = pltpu.get_barrier_semaphore()
    for axis in COORD:
        for k in range(1, COORD[axis][1]):
            pl.semaphore_signal(barrier, inc=1, device_id=(peer(me, axis, k),), device_id_type=MESH)
    pl.semaphore_wait(barrier, NPEER)


def remote(src, dst, send, recv, dev):
    return pltpu.make_async_remote_copy(src_ref=src, dst_ref=dst, send_sem=send, recv_sem=recv, device_id=(dev,), device_id_type=MESH)


def gather_streams(me, streams, bulk, send_sem, recv_sem):
    pending, sent = [None] * len(streams), []
    for phase in range(4):
        for s, (ref, off, unit, order) in enumerate(streams):
            if pending[s]:
                for c in pending[s]:
                    c.wait_recv()
            if phase == 3:
                continue
            span = 4 ** phase
            idx = block_index(me, order)
            where = ref.at[pl.ds(off + (idx - idx % span) * unit, span * unit)]
            pending[s] = []
            for k in range(1, 4):
                n = s * 9 + phase * 3 + k - 1
                c = remote(where, where, send_sem.at[n], recv_sem.at[n], peer(me, order[phase], k))
                c.start()
                pending[s].append(c)
                sent.append(c)
    last = []
    for i, (ref, count) in enumerate(bulk):
        n = len(streams) * 9 + i
        where = ref.at[pl.ds(coord(me, "core") * count, count)]
        c = remote(where, where, send_sem.at[n], recv_sem.at[n], peer(me, "core", 1))
        c.start()
        last.append(c)
    for c in last:
        c.wait_recv()
    return sent + last


def add_rows(ref, start, rref, base, count, parts):
    def add(i, carry):
        acc = ref[start + i]
        for k in range(parts):
            acc = acc + rref[base + k * count + i]
        ref[start + i] = acc
        return carry

    lax.fori_loop(0, count, add, 0, unroll=4)


def scatter_streams(me, ref, half, rref, streams, send_sem, recv_sem):
    mine = coord(me, "core")
    c = remote(ref.at[pl.ds((1 - mine) * half, half)], rref.at[pl.ds(0, half)], send_sem.at[0], recv_sem.at[0], peer(me, "core", 1))
    c.start()
    sent = [c]
    c.wait_recv()
    add_rows(ref, mine * half, rref, 0, half, 1)
    pending, rbase = [None] * 3, half
    for step in range(4):
        for s, (off, unit, order) in enumerate(streams):
            idx = block_index(me, order)
            if pending[s]:
                for c in pending[s][0]:
                    c.wait_recv()
                add_rows(ref, pending[s][1], rref, pending[s][2], pending[s][3], 3)
            if step == 3:
                continue
            span = 4 ** (2 - step)
            axis = order[2 - step]
            start = mine * half + off + (idx - idx % (4 * span)) * unit
            d = coord(me, axis)
            copies = []
            for k in range(1, 4):
                n = 1 + s * 9 + step * 3 + k - 1
                src = ref.at[pl.ds(start + (d + k) % 4 * span * unit, span * unit)]
                dst = rref.at[pl.ds(rbase + (k - 1) * span * unit, span * unit)]
                c = remote(src, dst, send_sem.at[n], recv_sem.at[n], peer(me, axis, k))
                c.start()
                copies.append(c)
            sent += copies
            pending[s] = (copies, start + d * span * unit, rbase, span * unit)
            rbase += 3 * span * unit
    return sent


def gelu_parts(a):
    c = 0.7978845608028654
    inner = jnp.tanh(c * (a + 0.044715 * (a * a * a)))
    half = 0.5 * (1.0 + inner)
    return a * half, half + 0.5 * a * (1.0 - inner * inner) * (c * (1.0 + 3.0 * 0.044715 * (a * a)))


def nt_dot(a, b):
    return lax.dot_general(a, b, (((1,), (1,)), ((), ())), preferred_element_type=F32)


def tn_dot(a, b):
    return lax.dot_general(a, b, (((0,), (0,)), ((), ())), preferred_element_type=F32)


H_OFF = (0, 192, 384)
H_UNIT = (3, 3, 2)
H_FIRST = (0, 3, 6)


def query_kernel(x_ref, win_ref, wout_ref, tgt_ref, h_ref, tall_ref, pre_ref, send_sem, recv_sem):
    me = lax.axis_index("dp")
    entry_barrier(me)
    pre = jnp.dot(x_ref[...], win_ref[...], preferred_element_type=F32)
    pre_ref[...] = pre
    act = gelu_parts(pre)[0].astype(BF16)
    query = jnp.dot(act, wout_ref[...], preferred_element_type=F32)
    core = coord(me, "core")
    streams = []
    for s in range(3):
        idx = block_index(me, ORDERS[s])
        for g in range(H_UNIT[s]):
            row = 8 * (H_FIRST[s] + g)
            h_ref[core * 512 + H_OFF[s] + idx * H_UNIT[s] + g] = query[row : row + 8, :].astype(BF16)
        streams.append((h_ref, core * 512 + H_OFF[s], H_UNIT[s], ORDERS[s]))
    tall_ref[core * 64 + block_index(me, ORDERS[2])] = tgt_ref[...]
    streams.append((tall_ref, core * 64, 1, ORDERS[2]))
    for c in gather_streams(me, streams, [(h_ref, 512), (tall_ref, 64)], send_sem, recv_sem):
        c.wait_send()


def stats_kernel(st_ref, out_ref, recv, cur, send_sem, recv_sem):
    me = lax.axis_index("dp")
    entry_barrier(me)
    sent = []
    pending = [None] * 3
    for phase in range(5):
        for s in range(3):
            g0, ng = H_FIRST[s], H_UNIT[s]
            if phase:
                for c in pending[s]:
                    c.wait_recv()
                base = 8 * (0, 3, 6, 9)[phase - 1]
                npart = len(pending[s])

                def merge(g, carry, phase=phase, base=base, npart=npart):
                    old = st_ref[g] if phase == 1 else cur[8 * (phase - 2) + g]
                    parts = [recv[base + 8 * k + g] for k in range(npart)]
                    top, z = old[0], old[2]
                    for p in parts:
                        top = jnp.maximum(top, p[0])
                        z = jnp.maximum(z, p[2])
                    total = old[1] * jnp.exp(old[0] - top)
                    for p in parts:
                        total = total + p[1] * jnp.exp(p[0] - top)
                    row = 8 * (phase - 1) + g
                    cur[row, 0] = top
                    cur[row, 1] = total
                    cur[row, 2] = z
                    return carry

                lax.fori_loop(g0, g0 + ng, merge, 0)
            if phase == 4:
                continue
            axis = (ORDERS[s] + ("core",))[phase]
            src = st_ref.at[pl.ds(g0, ng)] if phase == 0 else cur.at[pl.ds(8 * (phase - 1) + g0, ng)]
            base = 8 * (0, 3, 6, 9)[phase]
            pending[s] = []
            for k in range(1, COORD[axis][1]):
                n = s * NPEER + phase * 3 + k - 1
                c = remote(src, recv.at[pl.ds(base + 8 * (k - 1) + g0, ng)], send_sem.at[n], recv_sem.at[n], peer(me, axis, k))
                c.start()
                pending[s].append(c)
                sent.append(c)
    for g in range(8):
        m, t, z = cur[24 + g, 0], cur[24 + g, 1], cur[24 + g, 2]
        top = jnp.maximum(m, z)
        out_ref[0, 8 * g : 8 * g + 8, :] = top + jnp.log(t * jnp.exp(m - top) + jnp.exp(z - top))
        out_ref[1, 8 * g : 8 * g + 8, :] = z
    for c in sent:
        c.wait_send()


def grad_kernel(dq_ref, x_ref, wout_ref, pre_ref, dwin_ref, dwout_ref, acc, recv, tiles, trecv, whole, send_sem, recv_sem):
    me = lax.axis_index("dp")
    entry_barrier(me)

    def fill(i, carry):
        acc[i] = dq_ref[i]
        return carry

    lax.fori_loop(0, 1024, fill, 0, unroll=8)
    streams = [(H_OFF[s], H_UNIT[s], ORDERS[s]) for s in range(3)]
    sent = scatter_streams(me, acc, 512, recv, streams, send_sem.at[0], recv_sem.at[0])
    core = coord(me, "core")
    rows = []
    for s in range(3):
        idx = block_index(me, ORDERS[s])
        for g in range(H_UNIT[s]):
            rows.append(acc[core * 512 + H_OFF[s] + idx * H_UNIT[s] + g])
    dh = jnp.concatenate(rows, axis=0).astype(BF16)
    act, slope = gelu_parts(pre_ref[...])
    d_pre = (slope * nt_dot(dh, wout_ref[...])).astype(BF16)
    dw_out = tn_dot(act.astype(BF16), dh)
    tiles[0:128] = dw_out.reshape(128, 8, 128)
    dw_in = tn_dot(x_ref[...], d_pre)
    for j in range(8):
        tiles[128 + 32 * j : 160 + 32 * j] = dw_in[:, 128 * j : 128 * j + 128].reshape(32, 8, 128)
    streams = [(64 * s, 1, ORDERS[s]) for s in range(3)]
    sent2 = scatter_streams(me, tiles, 192, trecv, streams, send_sem.at[1], recv_sem.at[1])
    for c in sent + sent2:
        c.wait_send()
    streams = []
    for s in range(3):
        own = core * 192 + 64 * s + block_index(me, ORDERS[s])
        whole[own] = tiles[own]
        streams.append((whole, core * 192 + 64 * s, 1, ORDERS[s]))
    sent = gather_streams(me, streams, [(whole, 192)], send_sem.at[2], recv_sem.at[2])
    dwout_ref[...] = whole[0:128].reshape(1024, 128)
    for j in range(8):
        dwin_ref[:, 128 * j : 128 * j + 128] = whole[128 + 32 * j : 160 + 32 * j].reshape(256, 128)
    for c in sent:
        c.wait_send()


def vmem(n):
    return [pl.BlockSpec(memory_space=pltpu.VMEM)] * n


def params(cid):
    return pltpu.CompilerParams(collective_id=cid, has_side_effects=True, vmem_limit_bytes=48 * 1024 * 1024)


def dma(*shape):
    return pltpu.SemaphoreType.DMA(shape)


def solution(mesh):
    num_dev = mesh.shape["dp"]

    def local_step(features, w_in, w_out, table_blk, cand_ids, log_q, targets):
        dev_index = lax.axis_index("dp")
        block_rows = table_blk.shape[0]
        cand_dev = cand_ids.shape[0] // num_dev
        tok_total = features.shape[0] * num_dev
        tgt_row = jnp.pad(targets[None, :], ((0, 0), (0, 64)))
        h_all, tall, pre = pl.pallas_call(
            query_kernel,
            out_shape=[jax.ShapeDtypeStruct((1024, 8, 128), BF16), jax.ShapeDtypeStruct((128, 1, 128), jnp.int32), jax.ShapeDtypeStruct((64, 1024), F32)],
            in_specs=vmem(4), out_specs=vmem(3),
            scratch_shapes=[dma(4 * NPEER), dma(4 * NPEER)],
            compiler_params=params(0), name="query_gather",
        )(features, w_in, w_out, tgt_row)
        query_all = h_all.reshape(8192, 128)
        t5 = tall[:, 0, :64].reshape(2, 4, 4, 4, 64)
        tgt_all = jnp.concatenate([
            t5.transpose(0, 3, 1, 2, 4)[..., 0:24].reshape(2, -1),
            t5.transpose(0, 2, 3, 1, 4)[..., 24:48].reshape(2, -1),
            t5[..., 48:64].reshape(2, -1)], axis=1).reshape(-1)
        row_base = dev_index * block_rows
        tgt_local = tgt_all - row_base
        tgt_own = (tgt_local >= 0) & (tgt_local < block_rows)
        tgt_index = jnp.clip(tgt_local, 0, block_rows - 1)
        tgt_rows = table_blk[tgt_index]
        own_cands = lax.dynamic_slice_in_dim(cand_ids, dev_index * cand_dev, cand_dev)
        own_logq = lax.dynamic_slice_in_dim(log_q, dev_index * cand_dev, cand_dev)
        cand_index = own_cands - row_base
        cand_rows = table_blk[cand_index]
        tgt_dot = jnp.einsum("td,td->t", query_all, tgt_rows, preferred_element_type=F32)
        z_own = jnp.where(tgt_own, tgt_dot, -jnp.inf)
        cand_logit = jnp.einsum("td,cd->tc", query_all, cand_rows, preferred_element_type=F32) - own_logq[None, :]
        cand_logit = jnp.where(own_cands[None, :] == tgt_all[:, None], -1e9, cand_logit)
        top = jnp.max(cand_logit, axis=1)
        part = jnp.sum(jnp.exp(cand_logit - top[:, None]), axis=1)
        stats = jnp.stack([v.reshape(8, 8, 128) for v in (top, part, z_own)], axis=1)
        norm = pl.pallas_call(
            stats_kernel,
            out_shape=jax.ShapeDtypeStruct((2, 64, 128), F32),
            in_specs=vmem(1), out_specs=vmem(1)[0],
            scratch_shapes=[pltpu.VMEM((80, 3, 8, 128), F32), pltpu.VMEM((32, 3, 8, 128), F32), dma(3 * NPEER), dma(3 * NPEER)],
            compiler_params=params(1), name="stats_reduce",
        )(stats)
        log_norm, tgt_logit = norm[0].reshape(8192), norm[1].reshape(8192)
        loss = jnp.sum(log_norm - tgt_logit) / tok_total
        grad_tgt = (jnp.exp(tgt_logit - log_norm) - 1.0) / tok_total
        cand_grad = (jnp.exp(cand_logit - log_norm[:, None]) / tok_total).astype(BF16)
        own_grad = jnp.where(tgt_own, grad_tgt, 0.0)
        dq_part = own_grad[:, None] * tgt_rows + jnp.einsum("tc,cd->td", cand_grad, cand_rows, preferred_element_type=F32)
        grad_w_in, grad_w_out = pl.pallas_call(
            grad_kernel,
            out_shape=[jax.ShapeDtypeStruct((256, 1024), F32), jax.ShapeDtypeStruct((1024, 128), F32)],
            in_specs=vmem(4), out_specs=vmem(2),
            scratch_shapes=[
                pltpu.VMEM((1024, 8, 128), F32), pltpu.VMEM((8 * 127 + 8, 8, 128), F32),
                pltpu.VMEM((384, 8, 128), F32), pltpu.VMEM((3 * 127, 8, 128), F32), pltpu.VMEM((384, 8, 128), F32),
                dma(3, 3 * NPEER), dma(3, 3 * NPEER)],
            compiler_params=params(2), name="grad_reduce",
        )(dq_part.reshape(1024, 8, 128), features, w_out, pre)
        grad_cand = jnp.einsum("tc,td->cd", cand_grad, query_all, preferred_element_type=F32)
        grad_blk = jnp.zeros(table_blk.shape, F32).at[cand_index].add(grad_cand).at[tgt_index].add(own_grad[:, None] * query_all)
        return loss, grad_blk, grad_w_in, grad_w_out

    return jax.shard_map(local_step, mesh=mesh, in_specs=(P("dp", None), P(), P(), P("dp", None), P(), P(), P("dp")), out_specs=(P(), P("dp", None), P(), P()), check_vma=False)
```

```python
import functools
import jax
import jax.numpy as jnp
from jax import lax
from jax.experimental import pallas as pl
from jax.experimental.pallas import tpu as pltpu
from jax.sharding import PartitionSpec as P

MESH = pl.DeviceIdType.MESH
F32, BF16 = jnp.float32, jnp.bfloat16
COORD = {"core": (1, 2), "x": (2, 4), "y": (8, 4), "z": (32, 4)}
ORDERS = (("x", "y", "z"), ("y", "z", "x"), ("z", "x", "y"))
NDEV = 128
NPEER = 10
LANE, TOK, ALL, KILO, WIDE = 128, 64, 8192, 1024, 256


def one(i):
    return pl.ds(i, 1)


def coord(me, axis):
    stride, radix = COORD[axis]
    return (me // stride) % radix


def peer(me, axis, k):
    stride, radix = COORD[axis]
    c = coord(me, axis)
    return me + ((c + k) % radix - c) * stride


def block_index(me, order):
    idx, weight = 0, 1
    for axis in order:
        idx = idx + coord(me, axis) * weight
        weight *= COORD[axis][1]
    return idx


def entry_barrier(me):
    barrier = pltpu.get_barrier_semaphore()
    for axis in COORD:
        for k in range(1, COORD[axis][1]):
            pl.semaphore_signal(barrier, inc=1, device_id=(peer(me, axis, k),), device_id_type=MESH)
    pl.semaphore_wait(barrier, NPEER)


def remote(src, dst, send, recv, dev):
    return pltpu.make_async_remote_copy(src_ref=src, dst_ref=dst, send_sem=send, recv_sem=recv, device_id=(dev,), device_id_type=MESH)


def gather_streams(me, streams, bulk, send_sem, recv_sem):
    pending, sent = [None] * len(streams), []
    for phase in range(4):
        for s, (ref, off, unit, order) in enumerate(streams):
            if pending[s]:
                for c in pending[s]:
                    c.wait_recv()
            if phase == 3:
                continue
            span = 4 ** phase
            idx = block_index(me, order)
            where = ref.at[pl.ds(off + (idx - idx % span) * unit, span * unit)]
            pending[s] = []
            for k in range(1, 4):
                n = s * 9 + phase * 3 + k - 1
                c = remote(where, where, send_sem.at[n], recv_sem.at[n], peer(me, order[phase], k))
                c.start()
                pending[s].append(c)
                sent.append(c)
    last = []
    for i, (ref, count) in enumerate(bulk):
        n = len(streams) * 9 + i
        where = ref.at[pl.ds(coord(me, "core") * count, count)]
        c = remote(where, where, send_sem.at[n], recv_sem.at[n], peer(me, "core", 1))
        c.start()
        last.append(c)
    for c in last:
        c.wait_recv()
    return sent + last


def add_rows(ref, start, rref, base, count, parts):
    def add(i, carry):
        acc = ref[start + i]
        for k in range(parts):
            acc = acc + rref[base + k * count + i]
        ref[start + i] = acc
        return carry

    lax.fori_loop(0, count, add, 0, unroll=4)


def scatter_streams(me, ref, half, rref, streams, send_sem, recv_sem):
    mine = coord(me, "core")
    c = remote(ref.at[pl.ds((1 - mine) * half, half)], rref.at[pl.ds(0, half)], send_sem.at[0], recv_sem.at[0], peer(me, "core", 1))
    c.start()
    sent = [c]
    c.wait_recv()
    add_rows(ref, mine * half, rref, 0, half, 1)
    pending, rbase = [None] * 3, half
    for step in range(4):
        for s, (off, unit, order) in enumerate(streams):
            idx = block_index(me, order)
            if pending[s]:
                for c in pending[s][0]:
                    c.wait_recv()
                add_rows(ref, pending[s][1], rref, pending[s][2], pending[s][3], 3)
            if step == 3:
                continue
            span = 4 ** (2 - step)
            axis = order[2 - step]
            start = mine * half + off + (idx - idx % (4 * span)) * unit
            d = coord(me, axis)
            copies = []
            for k in range(1, 4):
                n = 1 + s * 9 + step * 3 + k - 1
                src = ref.at[pl.ds(start + (d + k) % 4 * span * unit, span * unit)]
                dst = rref.at[pl.ds(rbase + (k - 1) * span * unit, span * unit)]
                c = remote(src, dst, send_sem.at[n], recv_sem.at[n], peer(me, axis, k))
                c.start()
                copies.append(c)
            sent += copies
            pending[s] = (copies, start + d * span * unit, rbase, span * unit)
            rbase += 3 * span * unit
    return sent


def gelu_parts(a):
    c = 0.7978845608028654
    inner = jnp.tanh(c * (a + 0.044715 * (a * a * a)))
    half = 0.5 * (1.0 + inner)
    return a * half, half + 0.5 * a * (1.0 - inner * inner) * (c * (1.0 + 3.0 * 0.044715 * (a * a)))


def nt_dot(a, b):
    return lax.dot_general(a, b, (((1,), (1,)), ((), ())), preferred_element_type=F32)


def tn_dot(a, b):
    return lax.dot_general(a, b, (((0,), (0,)), ((), ())), preferred_element_type=F32)


H_OFF = (0, 192, 384)
H_UNIT = (3, 3, 2)
H_FIRST = (0, 3, 6)


def query_kernel(x_ref, win_ref, wout_ref, tgt_ref, h_ref, tall_ref, pre_ref, send_sem, recv_sem):
    me = lax.axis_index("dp")
    entry_barrier(me)
    pre = jnp.dot(x_ref[...], win_ref[...], preferred_element_type=F32)
    pre_ref[...] = pre
    act = gelu_parts(pre)[0].astype(BF16)
    query = jnp.dot(act, wout_ref[...], preferred_element_type=F32)
    core = coord(me, "core")
    streams = []
    for s in range(3):
        idx = block_index(me, ORDERS[s])
        for g in range(H_UNIT[s]):
            row = 8 * (H_FIRST[s] + g)
            h_ref[core * 512 + H_OFF[s] + idx * H_UNIT[s] + g] = query[row : row + 8, :].astype(BF16)
        streams.append((h_ref, core * 512 + H_OFF[s], H_UNIT[s], ORDERS[s]))
    tall_ref[core * TOK + block_index(me, ORDERS[2])] = tgt_ref[...]
    streams.append((tall_ref, core * TOK, 1, ORDERS[2]))
    for c in gather_streams(me, streams, [(h_ref, 512), (tall_ref, TOK)], send_sem, recv_sem):
        c.wait_send()


def stats_kernel(st_ref, out_ref, recv, cur, send_sem, recv_sem):
    me = lax.axis_index("dp")
    entry_barrier(me)
    sent = []
    pending = [None] * 3
    for phase in range(5):
        for s in range(3):
            g0, ng = H_FIRST[s], H_UNIT[s]
            if phase:
                for c in pending[s]:
                    c.wait_recv()
                base = 8 * (0, 3, 6, 9)[phase - 1]
                npart = len(pending[s])

                def merge(g, carry, phase=phase, base=base, npart=npart):
                    old = st_ref[g] if phase == 1 else cur[8 * (phase - 2) + g]
                    parts = [recv[base + 8 * k + g] for k in range(npart)]
                    top, z = old[0], old[2]
                    for p in parts:
                        top = jnp.maximum(top, p[0])
                        z = jnp.maximum(z, p[2])
                    total = old[1] * jnp.exp(old[0] - top)
                    for p in parts:
                        total = total + p[1] * jnp.exp(p[0] - top)
                    row = 8 * (phase - 1) + g
                    cur[row, 0] = top
                    cur[row, 1] = total
                    cur[row, 2] = z
                    return carry

                lax.fori_loop(g0, g0 + ng, merge, 0)
            if phase == 4:
                continue
            axis = (ORDERS[s] + ("core",))[phase]
            src = st_ref.at[pl.ds(g0, ng)] if phase == 0 else cur.at[pl.ds(8 * (phase - 1) + g0, ng)]
            base = 8 * (0, 3, 6, 9)[phase]
            pending[s] = []
            for k in range(1, COORD[axis][1]):
                n = s * NPEER + phase * 3 + k - 1
                c = remote(src, recv.at[pl.ds(base + 8 * (k - 1) + g0, ng)], send_sem.at[n], recv_sem.at[n], peer(me, axis, k))
                c.start()
                pending[s].append(c)
                sent.append(c)
    for g in range(8):
        m, t, z = cur[24 + g, 0], cur[24 + g, 1], cur[24 + g, 2]
        top = jnp.maximum(m, z)
        out_ref[0, 8 * g : 8 * g + 8, :] = top + jnp.log(t * jnp.exp(m - top) + jnp.exp(z - top))
        out_ref[1, 8 * g : 8 * g + 8, :] = z
    for c in sent:
        c.wait_send()


TILE = KILO


def score_kernel(h_ref, blk_ref, cand_ref, cid_ref, logq_ref, tgt_ref, e_ref, st_ref, pos_ref, row_ref, tok_ref, hc_ref, tc_ref, zd, cidb, logqb):
    step = pl.program_id(0)
    block_rows = blk_ref.shape[0]
    base = lax.axis_index("dp") * block_rows

    @pl.when(step == 0)
    def _():
        cidb[...] = jnp.broadcast_to(cid_ref[...], cidb.shape)
        logqb[...] = jnp.broadcast_to(logq_ref[...], logqb.shape)
        local = tgt_ref[...] - base
        own = (local >= 0) & (local < block_rows)
        own_f = jnp.where(own, 1.0, 0.0)
        own_b = own_f.astype(BF16)
        up = lax.broadcasted_iota(jnp.int32, (LANE, LANE), 0) < lax.broadcasted_iota(jnp.int32, (LANE, LANE), 1)
        prefix = jnp.dot(own_b, jnp.where(up, 1.0, 0.0).astype(BF16), preferred_element_type=F32)
        total = jnp.dot(own_b, jnp.ones((LANE, LANE), BF16), preferred_element_type=F32)
        low = lax.broadcasted_iota(jnp.int32, (TOK, TOK), 0) > lax.broadcasted_iota(jnp.int32, (TOK, TOK), 1)
        offset = jnp.dot(jnp.where(low, 1.0, 0.0).astype(BF16), total.astype(BF16), preferred_element_type=F32)
        pos_ref[...] = jnp.where(own, prefix + offset, -1.0)
        zd[...] = jnp.zeros_like(zd)
        chunks = (jnp.sum(own_f).astype(jnp.int32) + 127) // LANE
        slot0 = lax.broadcasted_iota(jnp.int32, (LANE, LANE), 0).astype(F32)
        lane = lax.broadcasted_iota(jnp.int32, (1, LANE), 1)

        def chunk(c, carry):
            slot = slot0 + (c * LANE).astype(F32)

            def collect(r, acc):
                hsum, code = acc
                hit = pos_ref[one(r), :] == slot
                local_row = tgt_ref[one(r), :] - base
                code = code + jnp.where(hit, local_row * ALL + (lane + r * LANE), 0)
                pick = jnp.where(hit, 1.0, 0.0).astype(BF16)
                return hsum + jnp.dot(pick, h_ref[pl.ds(r * LANE, LANE), :], preferred_element_type=F32), code

            hsum, code = lax.fori_loop(0, TOK, collect, (jnp.zeros((LANE, LANE), F32), jnp.zeros((LANE, LANE), jnp.int32)), unroll=4)
            row = jnp.sum((code // ALL).astype(F32), axis=1, keepdims=True)
            tok = jnp.sum((code % ALL).astype(F32), axis=1, keepdims=True)
            rowb = jnp.broadcast_to(row, (LANE, LANE))
            row_ref[one(c), :] = jnp.transpose(rowb)[0:1, :].astype(jnp.int32)
            tok_ref[one(c), :] = jnp.transpose(jnp.broadcast_to(tok, (LANE, LANE)))[0:1, :].astype(jnp.int32)

            def fetch(r, acc):
                hit = rowb == (lane + r * LANE).astype(F32)
                pick = jnp.where(hit, 1.0, 0.0).astype(BF16)
                return acc + jnp.dot(pick, blk_ref[pl.ds(r * LANE, LANE), :], preferred_element_type=F32)

            tsum = lax.fori_loop(0, block_rows // LANE, fetch, jnp.zeros((LANE, LANE), F32), unroll=4)
            hc_ref[pl.ds(c * LANE, LANE), :] = hsum.astype(BF16)
            tc_ref[pl.ds(c * LANE, LANE), :] = tsum.astype(BF16)
            z = jnp.broadcast_to(jnp.sum(hsum * tsum, axis=1, keepdims=True), (LANE, LANE))

            def spread(r, carry2):
                hit = pos_ref[one(r), :] == slot
                zd[one(r), :] += jnp.sum(jnp.where(hit, z, 0.0), axis=0, keepdims=True)
                return carry2

            lax.fori_loop(0, TOK, spread, 0, unroll=4)
            return carry

        lax.fori_loop(0, chunks, chunk, 0)

    for j in range(TILE // WIDE):
        col = pl.multiple_of(step * TILE + WIDE * j, WIDE)
        dots = nt_dot(cand_ref[...], h_ref[pl.ds(col, WIDE), :])
        for half in range(2):
            q = 2 * j + half
            cols = slice(LANE * q, LANE * q + LANE)
            tgt = tgt_ref[pl.ds(step * (TILE // LANE) + q, 1), :]
            s = dots[:, LANE * half : LANE * half + LANE] - logqb[...]
            s = jnp.where(cidb[...] == tgt, -1e9, s)
            m = jnp.max(s, axis=0, keepdims=True)
            e = jnp.exp(s - m)
            e_ref[:, cols] = e
            st_ref[0, 0, q : q + 1, :] = m
            st_ref[0, 1, q : q + 1, :] = jnp.sum(e, axis=0, keepdims=True)
    grp = pl.ds(pl.multiple_of(step * 8, 8), 8)
    st_ref[0, 2] = jnp.where(pos_ref[grp, :] >= 0.0, zd[grp, :], -jnp.inf)


def assemble_kernel(cidx_ref, row_ref, tok_ref, e_ref, st_ref, norm_ref, h_ref, cand_ref, pos_ref, hc_ref, tc_ref, dq_ref, de_ref, dcand, gh, gt, candt):
    step = pl.program_id(0)
    tokens = h_ref.shape[0]

    @pl.when(step == 0)
    def _():
        dcand[...] = jnp.zeros_like(dcand)
        candt[...] = jnp.transpose(cand_ref[...].astype(F32)).astype(BF16)

    for j in range(TILE // WIDE):
        probs = []
        for half in range(2):
            q = 2 * j + half
            cols = slice(LANE * q, LANE * q + LANE)
            scale = jnp.exp(st_ref[0, 0, q : q + 1, :] - norm_ref[0, pl.ds(step * 8 + q, 1), :]) / tokens
            probs.append((e_ref[:, cols] * scale).astype(BF16))
        p = jnp.concatenate(probs, axis=1)
        row = pl.multiple_of(step * TILE + WIDE * j, WIDE)
        dq_ref[pl.ds(row, WIDE), :] = jnp.transpose(jnp.dot(candt[...], p, preferred_element_type=F32))
        dcand[...] += jnp.dot(p, h_ref[pl.ds(row, WIDE), :], preferred_element_type=F32)

    @pl.when(step == pl.num_programs(0) - 1)
    def _():
        def clear(i, carry):
            de_ref[pl.ds(pl.multiple_of(i * TOK, TOK), TOK), :] = jnp.zeros((TOK, LANE), F32)
            return carry

        lax.fori_loop(0, de_ref.shape[0] // TOK, clear, 0)

        def place(i, carry):
            for u in range(8):
                de_ref[pl.ds(cidx_ref[i * 8 + u], 1), :] = dcand[pl.ds(i * 8 + u, 1), :]
            return carry

        lax.fori_loop(0, dcand.shape[0] // 8, place, 0)
        count = jnp.sum(jnp.where(pos_ref[...] >= 0.0, 1.0, 0.0)).astype(jnp.int32)
        slot0 = lax.broadcasted_iota(jnp.int32, (LANE, LANE), 0).astype(F32)

        def chunk(c, carry):
            slot = slot0 + (c * LANE).astype(F32)

            def collect(r, acc):
                hit = pos_ref[one(r), :] == slot
                g = (jnp.exp(norm_ref[1, one(r), :] - norm_ref[0, one(r), :]) - 1.0) / tokens
                return acc + jnp.where(hit, g, 0.0)

            g = jnp.sum(lax.fori_loop(0, TOK, collect, jnp.zeros((LANE, LANE), F32), unroll=4), axis=1, keepdims=True)
            gh[...] = g * hc_ref[pl.ds(c * LANE, LANE), :].astype(F32)
            gt[...] = g * tc_ref[pl.ds(c * LANE, LANE), :].astype(F32)

            def put(i, carry2):
                de_ref[pl.ds(row_ref[c, i], 1), :] += gh[one(i), :]
                dq_ref[pl.ds(tok_ref[c, i], 1), :] += gt[one(i), :]
                return carry2

            lax.fori_loop(0, jnp.minimum(count - c * LANE, LANE), put, 0)
            return carry

        lax.fori_loop(0, (count + 127) // LANE, chunk, 0)


def grad_kernel(dq_ref, x_ref, wout_ref, pre_ref, dwin_ref, dwout_ref, acc, recv, tiles, trecv, whole, send_sem, recv_sem):
    me = lax.axis_index("dp")
    entry_barrier(me)

    def fill(i, carry):
        acc[i] = dq_ref[i]
        return carry

    lax.fori_loop(0, KILO, fill, 0, unroll=8)
    streams = [(H_OFF[s], H_UNIT[s], ORDERS[s]) for s in range(3)]
    sent = scatter_streams(me, acc, 512, recv, streams, send_sem.at[0], recv_sem.at[0])
    core = coord(me, "core")
    rows = []
    for s in range(3):
        idx = block_index(me, ORDERS[s])
        for g in range(H_UNIT[s]):
            rows.append(acc[core * 512 + H_OFF[s] + idx * H_UNIT[s] + g])
    dh = jnp.concatenate(rows, axis=0).astype(BF16)
    act, slope = gelu_parts(pre_ref[...])
    d_pre = (slope * nt_dot(dh, wout_ref[...])).astype(BF16)
    dw_out = tn_dot(act.astype(BF16), dh)
    tiles[0:LANE] = dw_out.reshape(LANE, 8, LANE)
    dw_in = tn_dot(x_ref[...], d_pre)
    for j in range(8):
        tiles[LANE + 32 * j : 160 + 32 * j] = dw_in[:, LANE * j : LANE * j + LANE].reshape(32, 8, LANE)
    streams = [(TOK * s, 1, ORDERS[s]) for s in range(3)]
    sent2 = scatter_streams(me, tiles, 192, trecv, streams, send_sem.at[1], recv_sem.at[1])
    for c in sent + sent2:
        c.wait_send()
    streams = []
    for s in range(3):
        own = core * 192 + TOK * s + block_index(me, ORDERS[s])
        whole[own] = tiles[own]
        streams.append((whole, core * 192 + TOK * s, 1, ORDERS[s]))
    sent = gather_streams(me, streams, [(whole, 192)], send_sem.at[2], recv_sem.at[2])
    dwout_ref[...] = whole[0:LANE].reshape(KILO, LANE)
    for j in range(8):
        dwin_ref[:, LANE * j : LANE * j + LANE] = whole[LANE + 32 * j : 160 + 32 * j].reshape(WIDE, LANE)
    for c in sent:
        c.wait_send()


def vmem(n):
    return [pl.BlockSpec(memory_space=pltpu.VMEM)] * n


def params(cid):
    return pltpu.CompilerParams(collective_id=cid, has_side_effects=True, vmem_limit_bytes=48 * KILO * KILO)


def dma(*shape):
    return pltpu.SemaphoreType.DMA(shape)


def solution(mesh):
    num_dev = mesh.shape["dp"]

    def local_step(features, w_in, w_out, table_blk, cand_ids, log_q, targets):
        dev_index = lax.axis_index("dp")
        block_rows = table_blk.shape[0]
        cand_dev = cand_ids.shape[0] // num_dev
        tok_total = features.shape[0] * num_dev
        tgt_row = jnp.pad(targets[None, :], ((0, 0), (0, TOK)))
        h_all, tall, pre = pl.pallas_call(
            query_kernel,
            out_shape=[jax.ShapeDtypeStruct((KILO, 8, LANE), BF16), jax.ShapeDtypeStruct((LANE, 1, LANE), jnp.int32), jax.ShapeDtypeStruct((TOK, KILO), F32)],
            in_specs=vmem(4), out_specs=vmem(3),
            scratch_shapes=[dma(4 * NPEER), dma(4 * NPEER)],
            compiler_params=params(0), name="query_gather",
        )(features, w_in, w_out, tgt_row)
        query_all = h_all.reshape(ALL, LANE)
        t5 = tall[:, 0, :TOK].reshape(2, 4, 4, 4, TOK)
        tgt_all = jnp.concatenate([
            t5.transpose(0, 3, 1, 2, 4)[..., 0:24].reshape(2, -1),
            t5.transpose(0, 2, 3, 1, 4)[..., 24:48].reshape(2, -1),
            t5[..., 48:TOK].reshape(2, -1)], axis=1).reshape(TOK, LANE)
        own_cands = lax.dynamic_slice_in_dim(cand_ids, dev_index * cand_dev, cand_dev)
        own_logq = lax.dynamic_slice_in_dim(log_q, dev_index * cand_dev, cand_dev)
        cand_index = own_cands - dev_index * block_rows
        cand_rows = table_blk[cand_index]
        steps = tok_total // TILE
        whole = lambda *shape: pl.BlockSpec(shape, lambda i: (0,) * len(shape))
        smem = pl.BlockSpec(memory_space=pltpu.SMEM)
        e_spec = pl.BlockSpec((cand_dev, TILE), lambda i: (0, i))
        st_spec = pl.BlockSpec((1, 3, 8, LANE), lambda i: (i, 0, 0, 0))
        e, stats, pos, rows, toks, hc, tc = pl.pallas_call(
            score_kernel, grid=(steps,),
            out_shape=[
                jax.ShapeDtypeStruct((cand_dev, tok_total), F32), jax.ShapeDtypeStruct((steps, 3, 8, LANE), F32),
                jax.ShapeDtypeStruct((TOK, LANE), F32), jax.ShapeDtypeStruct((TOK, LANE), jnp.int32), jax.ShapeDtypeStruct((TOK, LANE), jnp.int32),
                jax.ShapeDtypeStruct((tok_total, LANE), BF16), jax.ShapeDtypeStruct((tok_total, LANE), BF16)],
            in_specs=[whole(tok_total, LANE), whole(block_rows, LANE), whole(cand_dev, LANE), whole(cand_dev, 1), whole(cand_dev, 1), whole(TOK, LANE)],
            out_specs=[e_spec, st_spec, whole(TOK, LANE), whole(TOK, LANE), whole(TOK, LANE), whole(tok_total, LANE), whole(tok_total, LANE)],
            scratch_shapes=[pltpu.VMEM((TOK, LANE), F32), pltpu.VMEM((cand_dev, LANE), jnp.int32), pltpu.VMEM((cand_dev, LANE), F32)],
            compiler_params=pltpu.CompilerParams(dimension_semantics=("arbitrary",), vmem_limit_bytes=48 * KILO * KILO), name="score",
        )(query_all, table_blk, cand_rows, own_cands[:, None], own_logq[:, None], tgt_all)
        norm = pl.pallas_call(
            stats_kernel,
            out_shape=jax.ShapeDtypeStruct((2, TOK, LANE), F32),
            in_specs=vmem(1), out_specs=vmem(1)[0],
            scratch_shapes=[pltpu.VMEM((80, 3, 8, LANE), F32), pltpu.VMEM((32, 3, 8, LANE), F32), dma(3 * NPEER), dma(3 * NPEER)],
            compiler_params=params(1), name="stats_reduce",
        )(stats)
        loss = jnp.sum(norm[0] - norm[1]) / tok_total
        dq_part, grad_blk = pl.pallas_call(
            assemble_kernel, grid=(steps,),
            out_shape=[jax.ShapeDtypeStruct((tok_total, LANE), F32), jax.ShapeDtypeStruct((block_rows, LANE), F32)],
            in_specs=[smem, smem, smem, e_spec, st_spec, whole(2, TOK, LANE), whole(tok_total, LANE), whole(cand_dev, LANE), whole(TOK, LANE), whole(tok_total, LANE), whole(tok_total, LANE)],
            out_specs=[whole(tok_total, LANE), whole(block_rows, LANE)],
            scratch_shapes=[pltpu.VMEM((cand_dev, LANE), F32), pltpu.VMEM((LANE, LANE), F32), pltpu.VMEM((LANE, LANE), F32), pltpu.VMEM((LANE, cand_dev), BF16)],
            compiler_params=pltpu.CompilerParams(dimension_semantics=("arbitrary",), vmem_limit_bytes=48 * KILO * KILO), name="assemble",
        )(cand_index, rows, toks, e, stats, norm, query_all, cand_rows, pos, hc, tc)
        grad_w_in, grad_w_out = pl.pallas_call(
            grad_kernel,
            out_shape=[jax.ShapeDtypeStruct((WIDE, KILO), F32), jax.ShapeDtypeStruct((KILO, LANE), F32)],
            in_specs=vmem(4), out_specs=vmem(2),
            scratch_shapes=[
                pltpu.VMEM((KILO, 8, LANE), F32), pltpu.VMEM((8 * 127 + 8, 8, LANE), F32),
                pltpu.VMEM((384, 8, LANE), F32), pltpu.VMEM((3 * 127, 8, LANE), F32), pltpu.VMEM((384, 8, LANE), F32),
                dma(3, 3 * NPEER), dma(3, 3 * NPEER)],
            compiler_params=params(2), name="grad_reduce",
        )(dq_part.reshape(KILO, 8, LANE), features, w_out, pre)
        return loss, grad_blk, grad_w_in, grad_w_out

    return jax.shard_map(local_step, mesh=mesh, in_specs=(P("dp", None), P(), P(), P("dp", None), P(), P(), P("dp")), out_specs=(P(), P("dp", None), P(), P()), check_vma=False)
```

```python
import functools
import jax
import jax.numpy as jnp
from jax import lax
from jax.experimental import pallas as pl
from jax.experimental.pallas import tpu as pltpu
from jax.sharding import PartitionSpec as P

MESH = pl.DeviceIdType.MESH
F32, BF16 = jnp.float32, jnp.bfloat16
COORD = {"core": (1, 2), "x": (2, 4), "y": (8, 4), "z": (32, 4)}
ORDERS = (("x", "y", "z"), ("y", "z", "x"), ("z", "x", "y"))
NDEV = 128
NPEER = 10
LANE, TOK, ALL, KILO, WIDE = 128, 64, 8192, 1024, 256


def one(i):
    return pl.ds(i, 1)


def coord(me, axis):
    stride, radix = COORD[axis]
    return (me // stride) % radix


def peer(me, axis, k):
    stride, radix = COORD[axis]
    c = coord(me, axis)
    return me + ((c + k) % radix - c) * stride


def block_index(me, order):
    idx, weight = 0, 1
    for axis in order:
        idx = idx + coord(me, axis) * weight
        weight *= COORD[axis][1]
    return idx


def entry_barrier(me):
    barrier = pltpu.get_barrier_semaphore()
    for axis in COORD:
        for k in range(1, COORD[axis][1]):
            pl.semaphore_signal(barrier, inc=1, device_id=(peer(me, axis, k),), device_id_type=MESH)
    pl.semaphore_wait(barrier, NPEER)


def remote(src, dst, send, recv, dev):
    return pltpu.make_async_remote_copy(src_ref=src, dst_ref=dst, send_sem=send, recv_sem=recv, device_id=(dev,), device_id_type=MESH)


def gather_streams(me, streams, bulk, send_sem, recv_sem):
    pending, sent = [None] * len(streams), []
    for phase in range(4):
        for s, (ref, off, unit, order) in enumerate(streams):
            if pending[s]:
                for c in pending[s]:
                    c.wait_recv()
            if phase == 3:
                continue
            span = 4 ** phase
            idx = block_index(me, order)
            where = ref.at[pl.ds(off + (idx - idx % span) * unit, span * unit)]
            pending[s] = []
            for k in range(1, 4):
                n = s * 9 + phase * 3 + k - 1
                c = remote(where, where, send_sem.at[n], recv_sem.at[n], peer(me, order[phase], k))
                c.start()
                pending[s].append(c)
                sent.append(c)
    last = []
    for i, (ref, count) in enumerate(bulk):
        n = len(streams) * 9 + i
        where = ref.at[pl.ds(coord(me, "core") * count, count)]
        c = remote(where, where, send_sem.at[n], recv_sem.at[n], peer(me, "core", 1))
        c.start()
        last.append(c)
    for c in last:
        c.wait_recv()
    return sent + last


def add_rows(ref, start, rref, base, count, parts):
    def add(i, carry):
        acc = ref[start + i]
        for k in range(parts):
            acc = acc + rref[base + k * count + i]
        ref[start + i] = acc
        return carry

    lax.fori_loop(0, count, add, 0, unroll=4)


def scatter_streams(me, ref, first, rref, rbase, streams, send_sem, recv_sem, between):
    sent = []
    pending = [None] * 3
    for step in range(4):
        for s, (off, unit, order) in enumerate(streams):
            idx = block_index(me, order)
            if pending[s]:
                for c in pending[s][0]:
                    c.wait_recv()
                add_rows(ref, pending[s][1], rref, pending[s][2], pending[s][3], 3)
            if step == 3:
                continue
            span = 4 ** (2 - step)
            axis = order[2 - step]
            start = first + off + (idx - idx % (4 * span)) * unit
            d = coord(me, axis)
            copies = []
            for k in range(1, 4):
                n = s * 9 + step * 3 + k - 1
                src = ref.at[pl.ds(start + (d + k) % 4 * span * unit, span * unit)]
                dst = rref.at[pl.ds(rbase + (k - 1) * span * unit, span * unit)]
                c = remote(src, dst, send_sem.at[n], recv_sem.at[n], peer(me, axis, k))
                c.start()
                copies.append(c)
            sent += copies
            pending[s] = (copies, start + d * span * unit, rbase, span * unit)
            rbase += 3 * span * unit
        if step == 0:
            between()
    return sent


def gelu_parts(a):
    c = 0.7978845608028654
    inner = jnp.tanh(c * (a + 0.044715 * (a * a * a)))
    half = 0.5 * (1.0 + inner)
    return a * half, half + 0.5 * a * (1.0 - inner * inner) * (c * (1.0 + 3.0 * 0.044715 * (a * a)))


def nt_dot(a, b):
    return lax.dot_general(a, b, (((1,), (1,)), ((), ())), preferred_element_type=F32)


def tn_dot(a, b):
    return lax.dot_general(a, b, (((0,), (0,)), ((), ())), preferred_element_type=F32)


H_OFF = (0, 192, 384)
H_UNIT = (3, 3, 2)
H_FIRST = (0, 3, 6)


def query_kernel(x_ref, win_ref, wout_ref, tgt_ref, h_ref, tall_ref, pre_ref, send_sem, recv_sem):
    me = lax.axis_index("dp")
    entry_barrier(me)
    pre = jnp.dot(x_ref[...], win_ref[...], preferred_element_type=F32)
    pre_ref[...] = pre
    act = gelu_parts(pre)[0].astype(BF16)
    query = jnp.dot(act, wout_ref[...], preferred_element_type=F32)
    core = coord(me, "core")
    streams = []
    for s in range(3):
        idx = block_index(me, ORDERS[s])
        for g in range(H_UNIT[s]):
            row = 8 * (H_FIRST[s] + g)
            h_ref[core * 512 + H_OFF[s] + idx * H_UNIT[s] + g] = query[row : row + 8, :].astype(BF16)
        streams.append((h_ref, core * 512 + H_OFF[s], H_UNIT[s], ORDERS[s]))
    tall_ref[core * TOK + block_index(me, ORDERS[2])] = tgt_ref[...]
    streams.append((tall_ref, core * TOK, 1, ORDERS[2]))
    for c in gather_streams(me, streams, [(h_ref, 512), (tall_ref, TOK)], send_sem, recv_sem):
        c.wait_send()


def reduce_stats(me, st_ref, recv, cur, send_sem, recv_sem):
    sent = []
    pending = [None] * 3
    for phase in range(5):
        for s in range(3):
            g0, ng = H_FIRST[s], H_UNIT[s]
            if phase:
                for c in pending[s]:
                    c.wait_recv()
                base = 8 * (0, 3, 6, 9)[phase - 1]
                npart = len(pending[s])

                def merge(g, carry, phase=phase, base=base, npart=npart):
                    old = st_ref[g] if phase == 1 else cur[8 * (phase - 2) + g]
                    parts = [recv[base + 8 * k + g] for k in range(npart)]
                    top, z = old[0], old[2]
                    for p in parts:
                        top = jnp.maximum(top, p[0])
                        z = jnp.maximum(z, p[2])
                    total = old[1] * jnp.exp(old[0] - top)
                    for p in parts:
                        total = total + p[1] * jnp.exp(p[0] - top)
                    row = 8 * (phase - 1) + g
                    cur[row, 0] = top
                    cur[row, 1] = total
                    cur[row, 2] = z
                    return carry

                lax.fori_loop(g0, g0 + ng, merge, 0)
            if phase == 4:
                continue
            axis = (ORDERS[s] + ("core",))[phase]
            src = st_ref.at[pl.ds(g0, ng)] if phase == 0 else cur.at[pl.ds(8 * (phase - 1) + g0, ng)]
            base = 8 * (0, 3, 6, 9)[phase]
            pending[s] = []
            for k in range(1, COORD[axis][1]):
                n = s * NPEER + phase * 3 + k - 1
                c = remote(src, recv.at[pl.ds(base + 8 * (k - 1) + g0, ng)], send_sem.at[n], recv_sem.at[n], peer(me, axis, k))
                c.start()
                pending[s].append(c)
                sent.append(c)
    return sent


TILE = KILO


def score_kernel(h_ref, blk_ref, cand_ref, cid_ref, logq_ref, tgt_ref, e_ref, mc_ref, st_ref, pos_ref, row_ref, hc_ref, te_ref, zd, cidb, logqb, part):
    step = pl.program_id(0)
    block_rows = blk_ref.shape[0]
    base = lax.axis_index("dp") * block_rows

    @pl.when(step == 0)
    def _():
        cidb[...] = jnp.broadcast_to(cid_ref[...], cidb.shape)
        logqb[...] = jnp.broadcast_to(logq_ref[...], logqb.shape)
        local = tgt_ref[...] - base
        own = (local >= 0) & (local < block_rows)
        own_f = jnp.where(own, 1.0, 0.0)
        own_b = own_f.astype(BF16)
        up = lax.broadcasted_iota(jnp.int32, (LANE, LANE), 0) < lax.broadcasted_iota(jnp.int32, (LANE, LANE), 1)
        prefix = jnp.dot(own_b, jnp.where(up, 1.0, 0.0).astype(BF16), preferred_element_type=F32)
        total = jnp.dot(own_b, jnp.ones((LANE, LANE), BF16), preferred_element_type=F32)
        low = lax.broadcasted_iota(jnp.int32, (TOK, TOK), 0) > lax.broadcasted_iota(jnp.int32, (TOK, TOK), 1)
        offset = jnp.dot(jnp.where(low, 1.0, 0.0).astype(BF16), total.astype(BF16), preferred_element_type=F32)
        pos_ref[...] = jnp.where(own, prefix + offset, -1.0)
        zd[...] = jnp.zeros_like(zd)
        te_ref[...] = jnp.zeros_like(te_ref)
        chunks = (jnp.sum(own_f).astype(jnp.int32) + 127) // LANE
        slot0 = lax.broadcasted_iota(jnp.int32, (LANE, LANE), 0).astype(F32)
        lane = lax.broadcasted_iota(jnp.int32, (1, LANE), 1)

        def chunk(c, carry):
            slot = slot0 + (c * LANE).astype(F32)

            def collect(i, acc):
                hsum, code = acc
                picks = []
                for u in range(8):
                    r = i * 8 + u
                    hit = pos_ref[one(r), :] == slot
                    code = code + jnp.where(hit, tgt_ref[one(r), :] - base, 0)
                    picks.append(jnp.where(hit, 1.0, 0.0).astype(BF16))
                pick = jnp.concatenate(picks, axis=1)
                tok = pl.ds(pl.multiple_of(i * KILO, KILO), KILO)
                return hsum + jnp.dot(pick, h_ref[tok, :], preferred_element_type=F32), code

            hsum, code = lax.fori_loop(0, 8, collect, (jnp.zeros((LANE, LANE), F32), jnp.zeros((LANE, LANE), jnp.int32)))
            rowb = jnp.broadcast_to(jnp.sum(code.astype(F32), axis=1, keepdims=True), (LANE, LANE))
            row_ref[one(c), :] = jnp.transpose(rowb)[0:1, :].astype(jnp.int32)

            def fetch(i, acc):
                picks = []
                for u in range(8):
                    hit = rowb == (lane + (i * 8 + u) * LANE).astype(F32)
                    picks.append(jnp.where(hit, 1.0, 0.0).astype(BF16))
                rows = pl.ds(pl.multiple_of(i * KILO, KILO), KILO)
                return acc + jnp.dot(jnp.concatenate(picks, axis=1), blk_ref[rows, :], preferred_element_type=F32)

            tsum = lax.fori_loop(0, block_rows // KILO, fetch, jnp.zeros((LANE, LANE), F32))
            hc_ref[pl.ds(c * LANE, LANE), :] = hsum.astype(BF16)
            z = jnp.transpose(jnp.broadcast_to(jnp.sum(hsum * tsum, axis=1, keepdims=True) / WIDE, (LANE, LANE)))[0:8, :]
            hi = z.astype(BF16).astype(F32)
            mid = (z - hi).astype(BF16).astype(F32)
            parts = jnp.concatenate([jnp.transpose(tsum), hi, mid, z - hi - mid], axis=0).astype(BF16)

            def spread(i, carry2):
                picks = []
                for u in range(4):
                    hit = pos_ref[one(i * 4 + u), :] == slot
                    picks.append(jnp.where(hit, 1.0, 0.0).astype(BF16))
                got = jnp.dot(parts, jnp.concatenate(picks, axis=1), preferred_element_type=F32)
                te_ref[i] = (te_ref[i].astype(F32) + got[0:LANE, :]).astype(BF16)
                zrow = (got[LANE : LANE + 1, :] + got[LANE + 8 : LANE + 9, :] + got[LANE + 16 : LANE + 17, :]) * WIDE
                for u in range(4):
                    zd[one(i * 4 + u), :] += zrow[:, LANE * u : LANE * u + LANE]
                return carry2

            lax.fori_loop(0, 16, spread, 0)
            return carry

        lax.fori_loop(0, chunks, chunk, 0)

    for j in range(4):
        col = pl.multiple_of(step * TILE + WIDE * j, WIDE)
        dots = nt_dot(cand_ref[...], h_ref[pl.ds(col, WIDE), :])
        for half in range(2):
            q = 2 * j + half
            cols = slice(LANE * (q % 4), LANE * (q % 4) + LANE)
            tgt = tgt_ref[one(step * 8 + q), :]
            for c in range(8):
                rows = slice(LANE * c, LANE * c + LANE)
                s = dots[rows, LANE * half : LANE * half + LANE] - logqb[rows, :]
                s = jnp.where(cidb[rows, :] == tgt, -1e9, s)
                m = jnp.max(s, axis=0, keepdims=True)
                e = jnp.exp(s - m)
                e_ref[q // 4, rows, cols] = e
                mc_ref[q, c : c + 1, :] = m
                part[q, c : c + 1, :] = jnp.sum(e, axis=0, keepdims=True)
            top = jnp.max(mc_ref[q], axis=0, keepdims=True)
            st_ref[0, 0, q : q + 1, :] = top
            st_ref[0, 1, q : q + 1, :] = jnp.sum(part[q] * jnp.exp(mc_ref[q] - top), axis=0, keepdims=True)
    grp = pl.ds(pl.multiple_of(step * 8, 8), 8)
    st_ref[0, 2] = jnp.where(pos_ref[grp, :] >= 0.0, zd[grp, :], -jnp.inf)


def table_kernel(cidx_ref, row_ref, g_ref, dcand_ref, pos_ref, hc_ref, de_ref, gh):
    def clear(i, carry):
        de_ref[pl.ds(pl.multiple_of(i * TOK, TOK), TOK), :] = jnp.zeros((TOK, LANE), F32)
        return carry

    lax.fori_loop(0, de_ref.shape[0] // TOK, clear, 0)

    def place(i, carry):
        for u in range(8):
            de_ref[one(cidx_ref[i * 8 + u]), :] = dcand_ref[one(i * 8 + u), :]
        return carry

    lax.fori_loop(0, dcand_ref.shape[0] // 8, place, 0)
    count = jnp.sum(jnp.where(pos_ref[...] >= 0.0, 1.0, 0.0)).astype(jnp.int32)
    slot0 = lax.broadcasted_iota(jnp.int32, (LANE, LANE), 0).astype(F32)

    def chunk(c, carry):
        slot = slot0 + (c * LANE).astype(F32)

        def collect(r, acc):
            return acc + jnp.where(pos_ref[one(r), :] == slot, g_ref[one(r), :], 0.0)

        g = jnp.sum(lax.fori_loop(0, 64, collect, jnp.zeros((LANE, LANE), F32), unroll=8), axis=1, keepdims=True)
        gh[...] = g * hc_ref[pl.ds(c * LANE, LANE), :].astype(F32)

        def put(i, carry2):
            de_ref[one(row_ref[c, i]), :] += gh[one(i), :]
            return carry2

        lax.fori_loop(0, jnp.minimum(count - c * LANE, LANE), put, 0)
        return carry

    lax.fori_loop(0, (count + 127) // LANE, chunk, 0)


LAST = 27
PART = 512


def core_exchange(me, ref, half, rref, send, recv):
    mine = coord(me, "core")
    c = remote(ref.at[pl.ds((1 - mine) * half, half)], rref.at[pl.ds(0, half)], send, recv, peer(me, "core", 1))
    c.start()
    c.wait_recv()
    add_rows(ref, mine * half, rref, 0, half, 1)
    return [c]


def grad_kernel(e_ref, mc_ref, st_ref, te_ref, h_ref, candt_ref, x_ref, wout_ref, pre_ref, dwin_ref, dwout_ref, g_ref, loss_ref, dcand_ref,
                ebuf, srecv, cur, norm, acc, recv, tiles, trecv, whole, e_sem, core_send, core_recv, send_sem, recv_sem):
    me = lax.axis_index("dp")
    core = coord(me, "core")
    entry_barrier(me)

    def load(i):
        return pltpu.make_async_copy(e_ref.at[i], ebuf.at[i], e_sem.at[i])

    def load_start(i, carry):
        load(i).start()
        return carry

    lax.fori_loop(0, 16, load_start, 0)
    sent = reduce_stats(me, st_ref, srecv, cur, send_sem.at[3], recv_sem.at[3])
    total = jnp.zeros((8, LANE), F32)
    for g in range(8):
        m, t, z = cur[24 + g, 0], cur[24 + g, 1], cur[24 + g, 2]
        top = jnp.maximum(m, z)
        log_norm = top + jnp.log(t * jnp.exp(m - top) + jnp.exp(z - top))
        total = total + (log_norm - z)
        norm[8 * g : 8 * g + 8, :] = log_norm
        g_ref[8 * g : 8 * g + 8, :] = (jnp.exp(z - log_norm) - 1.0) / ALL
    loss_ref[...] = jnp.broadcast_to(jnp.sum(total, keepdims=True) / ALL, loss_ref.shape)

    def probs(t):
        blocks = []
        for q in range(4):
            r = t * 4 + q
            scale = jnp.exp(mc_ref[r] - norm[one(r), :]) / ALL
            blocks.append(jnp.concatenate([
                (ebuf[t, LANE * c : LANE * c + LANE, LANE * q : LANE * q + LANE] * scale[c : c + 1, :]).astype(BF16) for c in range(8)], axis=0))
        return jnp.concatenate(blocks, axis=1)

    def query_grad(t):
        dqt = jnp.dot(candt_ref[...], probs(t), preferred_element_type=F32)
        grow = jnp.concatenate([g_ref[one(t * 4 + q), :] for q in range(4)], axis=1)
        dqt = dqt + grow * te_ref[t].astype(F32)
        return jnp.transpose(dqt).reshape(TOK, 8, LANE)

    def swap(i):
        return remote(acc.at[pl.ds(((1 - core) * 8 + i) * TOK, TOK)], recv.at[pl.ds(i * TOK, TOK)], core_send.at[i], core_recv.at[i], peer(me, "core", 1))

    def give(i, carry):
        t = (1 - core) * 8 + i
        load(t).wait()
        acc[pl.ds(t * TOK, TOK)] = query_grad(t)
        swap(i).start()
        return carry

    def keep(i, carry):
        t = core * 8 + i
        load(t).wait()
        val = query_grad(t)
        swap(i).wait_recv()
        acc[pl.ds(t * TOK, TOK)] = val + recv[pl.ds(i * TOK, TOK)]
        return carry

    lax.fori_loop(0, 8, give, 0)
    lax.fori_loop(0, 8, keep, 0)

    def cand_grad():
        dcand_ref[...] = jnp.zeros_like(dcand_ref)

        def accumulate(t, carry):
            dcand_ref[...] += jnp.dot(probs(t), h_ref[pl.ds(pl.multiple_of(t * PART, PART), PART), :], preferred_element_type=F32)
            return carry

        lax.fori_loop(0, 16, accumulate, 0)

    streams = [(H_OFF[s], H_UNIT[s], ORDERS[s]) for s in range(3)]
    sent += scatter_streams(me, acc, core * 512, recv, 512, streams, send_sem.at[0], recv_sem.at[0], cand_grad)
    rows = []
    for s in range(3):
        idx = block_index(me, ORDERS[s])
        for g in range(H_UNIT[s]):
            rows.append(acc[core * 512 + H_OFF[s] + idx * H_UNIT[s] + g])
    dh = jnp.concatenate(rows, axis=0).astype(BF16)
    act, slope = gelu_parts(pre_ref[...])
    d_pre = (slope * nt_dot(dh, wout_ref[...])).astype(BF16)
    dw_out = tn_dot(act.astype(BF16), dh)
    tiles[0:LANE] = dw_out.reshape(LANE, 8, LANE)
    dw_in = tn_dot(x_ref[...], d_pre)
    for j in range(8):
        tiles[LANE + 32 * j : 160 + 32 * j] = dw_in[:, LANE * j : LANE * j + LANE].reshape(32, 8, LANE)
    streams = [(TOK * s, 1, ORDERS[s]) for s in range(3)]
    half = core_exchange(me, tiles, 192, trecv, send_sem.at[1, LAST], recv_sem.at[1, LAST])
    sent += half + scatter_streams(me, tiles, core * 192, trecv, 192, streams, send_sem.at[1], recv_sem.at[1], lambda: None)
    streams = []
    for s in range(3):
        own = core * 192 + TOK * s + block_index(me, ORDERS[s])
        whole[own] = tiles[own]
        streams.append((whole, core * 192 + TOK * s, 1, ORDERS[s]))
    sent += gather_streams(me, streams, [(whole, 192)], send_sem.at[2], recv_sem.at[2])
    dwout_ref[...] = whole[0:LANE].reshape(KILO, LANE)
    for j in range(8):
        dwin_ref[:, LANE * j : LANE * j + LANE] = whole[LANE + 32 * j : 160 + 32 * j].reshape(WIDE, LANE)
    for c in sent:
        c.wait_send()

    def swap_done(i, carry):
        swap(i).wait_send()
        return carry

    lax.fori_loop(0, 8, swap_done, 0)


def vmem(n):
    return [pl.BlockSpec(memory_space=pltpu.VMEM)] * n


def params(cid):
    return pltpu.CompilerParams(collective_id=cid, has_side_effects=True, vmem_limit_bytes=63 * KILO * KILO)


def dma(*shape):
    return pltpu.SemaphoreType.DMA(shape)


def solution(mesh):
    num_dev = mesh.shape["dp"]

    def local_step(features, w_in, w_out, table_blk, cand_ids, log_q, targets):
        dev_index = lax.axis_index("dp")
        block_rows = table_blk.shape[0]
        cand_dev = cand_ids.shape[0] // num_dev
        tok_total = features.shape[0] * num_dev
        tgt_row = jnp.pad(targets[None, :], ((0, 0), (0, TOK)))
        h_all, tall, pre = pl.pallas_call(
            query_kernel,
            out_shape=[jax.ShapeDtypeStruct((KILO, 8, LANE), BF16), jax.ShapeDtypeStruct((LANE, 1, LANE), jnp.int32), jax.ShapeDtypeStruct((TOK, KILO), F32)],
            in_specs=vmem(4), out_specs=vmem(3),
            scratch_shapes=[dma(4 * NPEER), dma(4 * NPEER)],
            compiler_params=params(0), name="query_gather",
        )(features, w_in, w_out, tgt_row)
        query_all = h_all.reshape(ALL, LANE)
        t5 = tall[:, 0, :TOK].reshape(2, 4, 4, 4, TOK)
        tgt_all = jnp.concatenate([
            t5.transpose(0, 3, 1, 2, 4)[..., 0:24].reshape(2, -1),
            t5.transpose(0, 2, 3, 1, 4)[..., 24:48].reshape(2, -1),
            t5[..., 48:TOK].reshape(2, -1)], axis=1).reshape(TOK, LANE)
        own_cands = lax.dynamic_slice_in_dim(cand_ids, dev_index * cand_dev, cand_dev)
        own_logq = lax.dynamic_slice_in_dim(log_q, dev_index * cand_dev, cand_dev)
        cand_index = own_cands - dev_index * block_rows
        cand_rows = table_blk[cand_index]
        steps = tok_total // TILE
        whole = lambda *shape: pl.BlockSpec(shape, lambda i: (0,) * len(shape))
        smem = pl.BlockSpec(memory_space=pltpu.SMEM)
        e, mc, stats, pos, rows, hc, te = pl.pallas_call(
            score_kernel, grid=(steps,),
            out_shape=[
                jax.ShapeDtypeStruct((16, cand_dev, PART), F32), jax.ShapeDtypeStruct((TOK, 8, LANE), F32), jax.ShapeDtypeStruct((steps, 3, 8, LANE), F32),
                jax.ShapeDtypeStruct((TOK, LANE), F32), jax.ShapeDtypeStruct((TOK, LANE), jnp.int32),
                jax.ShapeDtypeStruct((tok_total, LANE), BF16), jax.ShapeDtypeStruct((16, LANE, PART), BF16)],
            in_specs=[whole(tok_total, LANE), whole(block_rows, LANE), whole(cand_dev, LANE), whole(cand_dev, 1), whole(cand_dev, 1), whole(TOK, LANE)],
            out_specs=[
                pl.BlockSpec((2, cand_dev, PART), lambda i: (i, 0, 0)), pl.BlockSpec((8, 8, LANE), lambda i: (i, 0, 0)),
                pl.BlockSpec((1, 3, 8, LANE), lambda i: (i, 0, 0, 0)), whole(TOK, LANE), whole(TOK, LANE), whole(tok_total, LANE), whole(16, LANE, PART)],
            scratch_shapes=[pltpu.VMEM((TOK, LANE), F32), pltpu.VMEM((cand_dev, LANE), jnp.int32), pltpu.VMEM((cand_dev, LANE), F32), pltpu.VMEM((8, 8, LANE), F32)],
            compiler_params=pltpu.CompilerParams(dimension_semantics=("arbitrary",), vmem_limit_bytes=48 * KILO * KILO), name="score",
        )(query_all, table_blk, cand_rows, own_cands[:, None], own_logq[:, None], tgt_all)
        grad_w_in, grad_w_out, grad_tgt, loss, dcand = pl.pallas_call(
            grad_kernel,
            out_shape=[
                jax.ShapeDtypeStruct((WIDE, KILO), F32), jax.ShapeDtypeStruct((KILO, LANE), F32), jax.ShapeDtypeStruct((TOK, LANE), F32),
                jax.ShapeDtypeStruct((8, LANE), F32), jax.ShapeDtypeStruct((cand_dev, LANE), F32)],
            in_specs=[pl.BlockSpec(memory_space=pl.ANY)] + vmem(8), out_specs=vmem(5),
            scratch_shapes=[
                pltpu.VMEM((16, cand_dev, PART), F32), pltpu.VMEM((80, 3, 8, LANE), F32), pltpu.VMEM((32, 3, 8, LANE), F32), pltpu.VMEM((TOK, LANE), F32),
                pltpu.VMEM((KILO, 8, LANE), F32), pltpu.VMEM((KILO, 8, LANE), F32),
                pltpu.VMEM((384, 8, LANE), F32), pltpu.VMEM((384, 8, LANE), F32), pltpu.VMEM((384, 8, LANE), F32),
                dma(16), dma(8), dma(8), dma(4, 3 * NPEER), dma(4, 3 * NPEER)],
            compiler_params=params(1), name="grad_reduce",
        )(e, mc, stats, te, query_all, cand_rows.T, features, w_out, pre)
        grad_blk = pl.pallas_call(
            table_kernel,
            out_shape=jax.ShapeDtypeStruct((block_rows, LANE), F32),
            in_specs=[smem, smem] + vmem(4), out_specs=vmem(1)[0],
            scratch_shapes=[pltpu.VMEM((LANE, LANE), F32)],
            compiler_params=pltpu.CompilerParams(vmem_limit_bytes=48 * KILO * KILO), name="table_grad",
        )(cand_index, rows, grad_tgt, dcand, pos, hc)
        loss = loss[0, 0]
        return loss, grad_blk, grad_w_in, grad_w_out

    return jax.shard_map(local_step, mesh=mesh, in_specs=(P("dp", None), P(), P(), P("dp", None), P(), P(), P("dp")), out_specs=(P(), P("dp", None), P(), P()), check_vma=False)
```

```python
import functools
import jax
import jax.numpy as jnp
from jax import lax
from jax.experimental import pallas as pl
from jax.experimental.pallas import tpu as pltpu
from jax.sharding import PartitionSpec as P

MESH = pl.DeviceIdType.MESH
F32, BF16 = jnp.float32, jnp.bfloat16
COORD = {"core": (1, 2), "x": (2, 4), "y": (8, 4), "z": (32, 4)}
ORDERS = (("x", "y", "z"), ("y", "z", "x"), ("z", "x", "y"))
NDEV = 128
NPEER = 10
LANE, TOK, ALL, KILO, WIDE = 128, 64, 8192, 1024, 256


def one(i):
    return pl.ds(i, 1)


def flag(mask):
    return jnp.where(mask, 1.0, 0.0)


def iota(shape, dim):
    return lax.broadcasted_iota(jnp.int32, shape, dim)


def coord(me, axis):
    stride, radix = COORD[axis]
    return (me // stride) % radix


def peer(me, axis, k):
    stride, radix = COORD[axis]
    c = coord(me, axis)
    return me + ((c + k) % radix - c) * stride


def block_index(me, order):
    idx, weight = 0, 1
    for axis in order:
        idx = idx + coord(me, axis) * weight
        weight *= COORD[axis][1]
    return idx


def entry_barrier(me):
    barrier = pltpu.get_barrier_semaphore()
    for axis in COORD:
        for k in range(1, COORD[axis][1]):
            pl.semaphore_signal(barrier, inc=1, device_id=(peer(me, axis, k),), device_id_type=MESH)
    pl.semaphore_wait(barrier, NPEER)


def remote(src, dst, send, recv, dev):
    return pltpu.make_async_remote_copy(src_ref=src, dst_ref=dst, send_sem=send, recv_sem=recv, device_id=(dev,), device_id_type=MESH)


def gather_streams(me, streams, bulk, send_sem, recv_sem, between=None):
    pending, sent = [None] * len(streams), []
    for phase in range(4):
        for s, (ref, off, unit, order) in enumerate(streams):
            if pending[s]:
                for c in pending[s]:
                    c.wait_recv()
            if phase == 3:
                continue
            span = 4 ** phase
            idx = block_index(me, order)
            where = ref.at[pl.ds(off + (idx - idx % span) * unit, span * unit)]
            pending[s] = []
            for k in range(1, 4):
                n = s * 9 + phase * 3 + k - 1
                c = remote(where, where, send_sem.at[n], recv_sem.at[n], peer(me, order[phase], k))
                c.start()
                pending[s].append(c)
                sent.append(c)
        if between and phase < 3:
            between(phase)
    last = []
    for i, (ref, count) in enumerate(bulk):
        n = len(streams) * 9 + i
        where = ref.at[pl.ds(coord(me, "core") * count, count)]
        c = remote(where, where, send_sem.at[n], recv_sem.at[n], peer(me, "core", 1))
        c.start()
        last.append(c)
    for c in last:
        c.wait_recv()
    return sent + last


def add_rows(ref, start, rref, base, count, parts):
    def add(i, carry):
        acc = ref[start + i]
        for k in range(parts):
            acc = acc + rref[base + k * count + i]
        ref[start + i] = acc
        return carry

    lax.fori_loop(0, count, add, 0, unroll=4)


def scatter_streams(me, ref, first, rref, rbase, streams, send_sem, recv_sem, between):
    sent = []
    pending = [None] * 3
    for step in range(4):
        for s, (off, unit, order) in enumerate(streams):
            idx = block_index(me, order)
            if pending[s]:
                for c in pending[s][0]:
                    c.wait_recv()
                add_rows(ref, pending[s][1], rref, pending[s][2], pending[s][3], 3)
            if step == 3:
                continue
            span = 4 ** (2 - step)
            axis = order[2 - step]
            start = first + off + (idx - idx % (4 * span)) * unit
            d = coord(me, axis)
            copies = []
            for k in range(1, 4):
                n = s * 9 + step * 3 + k - 1
                src = ref.at[pl.ds(start + (d + k) % 4 * span * unit, span * unit)]
                dst = rref.at[pl.ds(rbase + (k - 1) * span * unit, span * unit)]
                c = remote(src, dst, send_sem.at[n], recv_sem.at[n], peer(me, axis, k))
                c.start()
                copies.append(c)
            sent += copies
            pending[s] = (copies, start + d * span * unit, rbase, span * unit)
            rbase += 3 * span * unit
        if step == 0:
            between()
    return sent


def gelu_parts(a):
    c = 0.7978845608028654
    inner = jnp.tanh(c * (a + 0.044715 * (a * a * a)))
    half = 0.5 * (1.0 + inner)
    return a * half, half + 0.5 * a * (1.0 - inner * inner) * (c * (1.0 + 3.0 * 0.044715 * (a * a)))


def nt_dot(a, b):
    return lax.dot_general(a, b, (((1,), (1,)), ((), ())), preferred_element_type=F32)


def tn_dot(a, b):
    return lax.dot_general(a, b, (((0,), (0,)), ((), ())), preferred_element_type=F32)


H_OFF = (0, 192, 384)
H_UNIT = (3, 3, 2)
H_FIRST = (0, 3, 6)


def column(row):
    return jnp.transpose(jnp.broadcast_to(row, (LANE, LANE)))


def query_kernel(x_ref, win_ref, wout_ref, tgt_ref, blk_ref, cid_ref, logq_ref, h_ref, tall_ref, pre_ref, cand_ref, candt_ref, cidb_ref, logqb_ref,
                 blk, ids, lqs, rows, load_sem, send_sem, recv_sem):
    me = lax.axis_index("dp")
    mine = pl.ds(pl.multiple_of(me * 8, 8), 8)
    loads = [
        pltpu.make_async_copy(cid_ref.at[mine], ids, load_sem.at[0]), pltpu.make_async_copy(logq_ref.at[mine], lqs, load_sem.at[1]),
        pltpu.make_async_copy(blk_ref, blk, load_sem.at[2])]
    for c in loads:
        c.start()
    entry_barrier(me)
    pre = jnp.dot(x_ref[...], win_ref[...], preferred_element_type=F32)
    pre_ref[...] = pre
    act = gelu_parts(pre)[0].astype(BF16)
    query = jnp.dot(act, wout_ref[...], preferred_element_type=F32)
    core = coord(me, "core")
    streams = []
    for s in range(3):
        idx = block_index(me, ORDERS[s])
        for g in range(H_UNIT[s]):
            row = 8 * (H_FIRST[s] + g)
            h_ref[core * 512 + H_OFF[s] + idx * H_UNIT[s] + g] = query[row : row + 8, :].astype(BF16)
        streams.append((h_ref, core * 512 + H_OFF[s], H_UNIT[s], ORDERS[s]))
    tall_ref[core * TOK + block_index(me, ORDERS[2])] = tgt_ref[...]
    streams.append((tall_ref, core * TOK, 1, ORDERS[2]))
    lane = iota((1, LANE), 1)

    def pick(n, carry):
        part = pl.ds(pl.multiple_of(n // 8 * WIDE, WIDE), WIDE)
        first = n % 8 * KILO
        want = cidb_ref[part, :]
        picks = [flag(want == (lane + (first + u * LANE)).astype(F32)).astype(BF16) for u in range(8)]
        rows[part, :] += jnp.dot(jnp.concatenate(picks, axis=1), blk[pl.ds(pl.multiple_of(first, KILO), KILO), :], preferred_element_type=F32)
        return carry

    def fill(phase):
        if phase == 0:
            for c in loads:
                c.wait()
            for c in range(8):
                at = slice(c * LANE, c * LANE + LANE)
                cidb_ref[at, :] = column((ids[c : c + 1, :] - me * ALL).astype(F32))
                logqb_ref[at, :] = column(lqs[c : c + 1, :])
            rows[...] = jnp.zeros_like(rows)
        bounds = (0, 8, 17, 32)
        lax.fori_loop(bounds[phase], bounds[phase + 1], pick, 0)
        if phase == 2:
            cand_ref[...] = rows[...].astype(BF16)
            candt_ref[...] = jnp.transpose(rows[...]).astype(BF16)

    for c in gather_streams(me, streams, [(h_ref, 512), (tall_ref, TOK)], send_sem, recv_sem, fill):
        c.wait_send()


def reduce_stats(me, st_ref, recv, cur, send_sem, recv_sem):
    sent = []
    pending = [None] * 3
    for phase in range(5):
        for s in range(3):
            g0, ng = H_FIRST[s], H_UNIT[s]
            if phase:
                for c in pending[s]:
                    c.wait_recv()
                base = 8 * (0, 3, 6, 9)[phase - 1]
                npart = len(pending[s])

                def merge(g, carry, phase=phase, base=base, npart=npart):
                    old = st_ref[g] if phase == 1 else cur[8 * (phase - 2) + g]
                    parts = [recv[base + 8 * k + g] for k in range(npart)]
                    top, z = old[0], old[2]
                    for p in parts:
                        top = jnp.maximum(top, p[0])
                        z = jnp.maximum(z, p[2])
                    total = old[1] * jnp.exp(old[0] - top)
                    for p in parts:
                        total = total + p[1] * jnp.exp(p[0] - top)
                    row = 8 * (phase - 1) + g
                    cur[row, 0] = top
                    cur[row, 1] = total
                    cur[row, 2] = z
                    return carry

                lax.fori_loop(g0, g0 + ng, merge, 0)
            if phase == 4:
                continue
            axis = (ORDERS[s] + ("core",))[phase]
            src = st_ref.at[pl.ds(g0, ng)] if phase == 0 else cur.at[pl.ds(8 * (phase - 1) + g0, ng)]
            base = 8 * (0, 3, 6, 9)[phase]
            pending[s] = []
            for k in range(1, COORD[axis][1]):
                n = s * NPEER + phase * 3 + k - 1
                c = remote(src, recv.at[pl.ds(base + 8 * (k - 1) + g0, ng)], send_sem.at[n], recv_sem.at[n], peer(me, axis, k))
                c.start()
                pending[s].append(c)
                sent.append(c)
    return sent


TILE = KILO


def score_kernel(h_ref, blk_ref, cand_ref, cidb, logqb, tgt_ref, e_ref, mc_ref, st_ref, pos_ref, code_ref, hc_ref, te_ref, zd, part, local, hs, es, codes, sem):
    step = pl.program_id(0)
    block_rows = blk_ref.shape[0]

    @pl.when(step == 0)
    def _():
        rel = tgt_ref[...] - lax.axis_index("dp") * block_rows
        own = (rel >= 0) & (rel < block_rows)
        local[...] = rel.astype(F32)
        own_f = flag(own)
        own_b = own_f.astype(BF16)
        up = iota((LANE, LANE), 0) < iota((LANE, LANE), 1)
        prefix = jnp.dot(own_b, flag(up).astype(BF16), preferred_element_type=F32)
        total = jnp.dot(own_b, jnp.ones((LANE, LANE), BF16), preferred_element_type=F32)
        low = iota((TOK, TOK), 0) > iota((TOK, TOK), 1)
        offset = jnp.dot(flag(low).astype(BF16), total.astype(BF16), preferred_element_type=F32)
        pos_ref[...] = jnp.where(own, prefix + offset, -1.0)
        zd[...] = jnp.zeros_like(zd)

        def clear(i, carry):
            te_ref[pl.ds(pl.multiple_of(i * LANE, LANE), LANE), :] = jnp.zeros((LANE, LANE), F32)
            return carry

        lax.fori_loop(0, TOK, clear, 0)
        count = jnp.sum(own_f).astype(jnp.int32)
        slot0 = iota((LANE, LANE), 0).astype(F32)
        lane = iota((1, LANE), 1)
        sub = iota((16, LANE), 0)

        def one_row(ref, i):
            tile = ref[pl.ds(pl.multiple_of(i // 16 * 16, 16), 16), :].astype(F32)
            return jnp.sum(jnp.where(sub == i % 16, tile, 0.0), axis=0, keepdims=True)

        def chunk(c, carry):
            slot = slot0 + (c * LANE).astype(F32)

            def collect(r, code):
                mark = (tgt_ref[one(r), :] % block_rows) * ALL + (lane + r * LANE)
                return code + jnp.where(pos_ref[one(r), :] == slot, mark, 0)

            code = lax.fori_loop(0, TOK, collect, jnp.zeros((LANE, LANE), jnp.int32), unroll=8)
            row = jnp.sum((code // ALL).astype(F32), axis=1, keepdims=True)
            tok = jnp.sum((code % ALL).astype(F32), axis=1, keepdims=True)
            both = row.astype(jnp.int32) * ALL + tok.astype(jnp.int32)
            code_ref[one(c), :] = jnp.transpose(jnp.broadcast_to(both, (LANE, LANE)))[0:1, :]
            copy = pltpu.make_async_copy(code_ref.at[one(c)], codes, sem)
            copy.start()
            copy.wait()
            left = count - c * LANE

            def fetch(i, carry2):
                for u in range(8):
                    n = i * 8 + u
                    v = codes[0, n]
                    hs[one(n), :] = one_row(h_ref, v % ALL)
                    row = one_row(blk_ref, v // ALL)
                    es[one(n), :] = row
                    te_ref[one(jnp.where(n < left, v % ALL, ALL)), :] = row
                return carry2

            lax.fori_loop(0, (jnp.minimum(left, LANE) + 7) // 8, fetch, 0)
            hc_ref[pl.ds(c * LANE, LANE), :] = hs[...]
            z = jnp.broadcast_to(jnp.sum(hs[...] * es[...], axis=1, keepdims=True), (LANE, LANE))

            def spread(r, carry2):
                hit = pos_ref[one(r), :] == slot
                zd[one(r), :] += jnp.sum(jnp.where(hit, z, 0.0), axis=0, keepdims=True)
                return carry2

            lax.fori_loop(0, TOK, spread, 0, unroll=8)
            return carry

        lax.fori_loop(0, (count + 127) // LANE, chunk, 0)

    for j in range(4):
        col = pl.multiple_of(step * TILE + WIDE * j, WIDE)
        dots = nt_dot(cand_ref[...], h_ref[pl.ds(col, WIDE), :])
        for half in range(2):
            q = 2 * j + half
            cols = slice(LANE * (q % 4), LANE * (q % 4) + LANE)
            tgt = local[one(step * 8 + q), :]
            for c in range(8):
                rows = slice(LANE * c, LANE * c + LANE)
                s = dots[rows, LANE * half : LANE * half + LANE] - logqb[rows, :]
                s = jnp.where(cidb[rows, :] == tgt, -1e9, s)
                m = jnp.max(s, axis=0, keepdims=True)
                e = jnp.exp(s - m)
                e_ref[q // 4, rows, cols] = e
                mc_ref[q, c : c + 1, :] = m
                part[q, c : c + 1, :] = jnp.sum(e, axis=0, keepdims=True)
            top = jnp.max(mc_ref[q], axis=0, keepdims=True)
            st_ref[0, 0, q : q + 1, :] = top
            st_ref[0, 1, q : q + 1, :] = jnp.sum(part[q] * jnp.exp(mc_ref[q] - top), axis=0, keepdims=True)
    grp = pl.ds(pl.multiple_of(step * 8, 8), 8)
    st_ref[0, 2] = jnp.where(pos_ref[grp, :] >= 0.0, zd[grp, :], -jnp.inf)


def table_kernel(cidx_ref, code_ref, g_ref, pos_ref, lossrow_ref, dcand_hbm, tiles_hbm, hc_ref, de_ref, dwin_ref, dwout_ref, loss_ref, dcand, whole, hc, gh, sem):
    loads = [pltpu.make_async_copy(dcand_hbm, dcand, sem.at[0]), pltpu.make_async_copy(tiles_hbm, whole, sem.at[1])]
    for c in loads:
        c.start()
    loss_ref[0, 0] = jnp.max(lossrow_ref[...])

    def clear(i, carry):
        de_ref[pl.ds(pl.multiple_of(i * LANE, LANE), LANE), :] = jnp.zeros((LANE, LANE), F32)
        return carry

    lax.fori_loop(0, de_ref.shape[0] // LANE, clear, 0)
    for c in loads:
        c.wait()

    base = lax.axis_index("dp") * ALL

    def place(i, carry):
        for u in range(8):
            n = i * 8 + u
            de_ref[one(cidx_ref[0, n] - base), :] = dcand[one(n), :]
        return carry

    lax.fori_loop(0, dcand.shape[0] // 8, place, 0)
    count = jnp.sum(flag(pos_ref[...] >= 0.0)).astype(jnp.int32)
    slot0 = iota((LANE, LANE), 0).astype(F32)

    def chunk(c, carry):
        slot = slot0 + (c * LANE).astype(F32)
        copy = pltpu.make_async_copy(hc_ref.at[pl.ds(pl.multiple_of(c * LANE, LANE), LANE)], hc, sem.at[2])
        copy.start()

        def collect(r, acc):
            return acc + jnp.where(pos_ref[one(r), :] == slot, g_ref[one(r), :], 0.0)

        g = jnp.sum(lax.fori_loop(0, TOK, collect, jnp.zeros((LANE, LANE), F32), unroll=8), axis=1, keepdims=True)
        copy.wait()
        gh[...] = g * hc[...]

        def put(i, carry2):
            de_ref[one(code_ref[c, i] // ALL), :] += gh[one(i), :]
            return carry2

        lax.fori_loop(0, jnp.minimum(count - c * LANE, LANE), put, 0)
        return carry

    lax.fori_loop(0, (count + 127) // LANE, chunk, 0)
    dwout_ref[...] = whole[0:LANE].reshape(KILO, LANE)
    for j in range(8):
        dwin_ref[:, LANE * j : LANE * j + LANE] = whole[LANE + 32 * j : 160 + 32 * j].reshape(WIDE, LANE)


LAST = 27
PART = 512


def core_exchange(me, ref, half, rref, send, recv):
    mine = coord(me, "core")
    c = remote(ref.at[pl.ds((1 - mine) * half, half)], rref.at[pl.ds(0, half)], send, recv, peer(me, "core", 1))
    c.start()
    c.wait_recv()
    add_rows(ref, mine * half, rref, 0, half, 1)
    return [c]


def grad_kernel(e_ref, mc_ref, st_ref, te_hbm, h_hbm, candt_hbm, x_hbm, wout_hbm, pre_hbm, whole, g_ref, loss_ref, dcand_ref,
                ebuf, srecv, cur, norm, acc, recv, tiles, trecv, te_ref, h_ref, candt_ref, x_ref, wout_ref, pre_ref,
                load_sem, e_sem, core_send, core_recv, send_sem, recv_sem):
    me = lax.axis_index("dp")
    core = coord(me, "core")
    loads = [
        pltpu.make_async_copy(a, b, load_sem.at[i]) for i, (a, b) in enumerate([
            (candt_hbm, candt_ref), (te_hbm.at[pl.ds(0, ALL)], te_ref), (h_hbm, h_ref), (x_hbm, x_ref), (wout_hbm, wout_ref), (pre_hbm, pre_ref)])]
    for c in loads:
        c.start()
    entry_barrier(me)

    def load(i):
        return pltpu.make_async_copy(e_ref.at[i], ebuf.at[i], e_sem.at[i])

    def load_start(i, carry):
        load(i).start()
        return carry

    lax.fori_loop(0, 16, load_start, 0)
    sent = reduce_stats(me, st_ref, srecv, cur, send_sem.at[3], recv_sem.at[3])
    total = jnp.zeros((8, LANE), F32)
    for g in range(8):
        m, t, z = cur[24 + g, 0], cur[24 + g, 1], cur[24 + g, 2]
        top = jnp.maximum(m, z)
        log_norm = top + jnp.log(t * jnp.exp(m - top) + jnp.exp(z - top))
        total = total + (log_norm - z)
        norm[8 * g : 8 * g + 8, :] = log_norm
        g_ref[8 * g : 8 * g + 8, :] = (jnp.exp(z - log_norm) - 1.0) / ALL
    loss_ref[...] = jnp.broadcast_to(jnp.sum(total, keepdims=True) / ALL, loss_ref.shape)

    def probs(t):
        blocks = []
        for q in range(4):
            r = t * 4 + q
            scale = jnp.exp(mc_ref[r] - norm[one(r), :]) / ALL
            blocks.append(jnp.concatenate([
                (ebuf[t, LANE * c : LANE * c + LANE, LANE * q : LANE * q + LANE] * scale[c : c + 1, :]).astype(BF16) for c in range(8)], axis=0))
        return jnp.concatenate(blocks, axis=1)

    for c in loads:
        c.wait()

    def query_grad(t):
        dqt = jnp.dot(candt_ref[...], probs(t), preferred_element_type=F32)
        gcol = jnp.concatenate([column(g_ref[one(t * 4 + q), :]) for q in range(4)], axis=0)
        dq = jnp.transpose(dqt) + gcol * te_ref[pl.ds(pl.multiple_of(t * PART, PART), PART), :]
        return dq.reshape(TOK, 8, LANE)

    def swap(i):
        return remote(acc.at[pl.ds(((1 - core) * 8 + i) * TOK, TOK)], recv.at[pl.ds(i * TOK, TOK)], core_send.at[i], core_recv.at[i], peer(me, "core", 1))

    def give(i, carry):
        t = (1 - core) * 8 + i
        load(t).wait()
        acc[pl.ds(t * TOK, TOK)] = query_grad(t)
        swap(i).start()
        return carry

    def keep(i, carry):
        t = core * 8 + i
        load(t).wait()
        val = query_grad(t)
        swap(i).wait_recv()
        acc[pl.ds(t * TOK, TOK)] = val + recv[pl.ds(i * TOK, TOK)]
        return carry

    lax.fori_loop(0, 8, give, 0)
    lax.fori_loop(0, 8, keep, 0)

    def cand_grad():
        dcand_ref[...] = jnp.zeros_like(dcand_ref)

        def accumulate(t, carry):
            dcand_ref[...] += jnp.dot(probs(t), h_ref[pl.ds(pl.multiple_of(t * PART, PART), PART), :], preferred_element_type=F32)
            return carry

        lax.fori_loop(0, 16, accumulate, 0)

    streams = [(H_OFF[s], H_UNIT[s], ORDERS[s]) for s in range(3)]
    sent += scatter_streams(me, acc, core * 512, recv, 512, streams, send_sem.at[0], recv_sem.at[0], cand_grad)
    rows = []
    for s in range(3):
        idx = block_index(me, ORDERS[s])
        for g in range(H_UNIT[s]):
            rows.append(acc[core * 512 + H_OFF[s] + idx * H_UNIT[s] + g])
    dh = jnp.concatenate(rows, axis=0).astype(BF16)
    act, slope = gelu_parts(pre_ref[...])
    d_pre = (slope * nt_dot(dh, wout_ref[...])).astype(BF16)
    dw_out = tn_dot(act.astype(BF16), dh)
    tiles[0:LANE] = dw_out.reshape(LANE, 8, LANE)
    dw_in = tn_dot(x_ref[...], d_pre)
    for j in range(8):
        tiles[LANE + 32 * j : 160 + 32 * j] = dw_in[:, LANE * j : LANE * j + LANE].reshape(32, 8, LANE)
    streams = [(TOK * s, 1, ORDERS[s]) for s in range(3)]
    half = core_exchange(me, tiles, 192, trecv, send_sem.at[1, LAST], recv_sem.at[1, LAST])
    sent += half + scatter_streams(me, tiles, core * 192, trecv, 192, streams, send_sem.at[1], recv_sem.at[1], lambda: None)
    streams = []
    for s in range(3):
        own = core * 192 + TOK * s + block_index(me, ORDERS[s])
        whole[own] = tiles[own]
        streams.append((whole, core * 192 + TOK * s, 1, ORDERS[s]))
    sent += gather_streams(me, streams, [(whole, 192)], send_sem.at[2], recv_sem.at[2])
    for c in sent:
        c.wait_send()

    def swap_done(i, carry):
        swap(i).wait_send()
        return carry

    lax.fori_loop(0, 8, swap_done, 0)


def vmem(n):
    return [pl.BlockSpec(memory_space=pltpu.VMEM)] * n


def params(cid):
    return pltpu.CompilerParams(collective_id=cid, has_side_effects=True, vmem_limit_bytes=63 * KILO * KILO)


def dma(*shape):
    return pltpu.SemaphoreType.DMA(shape)


def solution(mesh):
    num_dev = mesh.shape["dp"]

    def local_step(features, w_in, w_out, table_blk, cand_ids, log_q, targets):
        dev_index = lax.axis_index("dp")
        block_rows = table_blk.shape[0]
        cand_dev = cand_ids.shape[0] // num_dev
        tok_total = features.shape[0] * num_dev
        anyspec = pl.BlockSpec(memory_space=pl.ANY)
        cid_rows, logq_rows = cand_ids.reshape(KILO, LANE), log_q.reshape(KILO, LANE)
        h_all, tall, pre, cand_rows, cand_t, cidb, logqb = pl.pallas_call(
            query_kernel,
            out_shape=[
                jax.ShapeDtypeStruct((KILO, 8, LANE), BF16), jax.ShapeDtypeStruct((LANE, 1, TOK), jnp.int32), jax.ShapeDtypeStruct((TOK, KILO), F32),
                jax.ShapeDtypeStruct((cand_dev, LANE), BF16), jax.ShapeDtypeStruct((LANE, cand_dev), BF16),
                jax.ShapeDtypeStruct((cand_dev, LANE), F32), jax.ShapeDtypeStruct((cand_dev, LANE), F32)],
            in_specs=vmem(4) + [anyspec] * 3, out_specs=vmem(7),
            scratch_shapes=[
                pltpu.VMEM((block_rows, LANE), BF16), pltpu.VMEM((8, LANE), jnp.int32), pltpu.VMEM((8, LANE), F32), pltpu.VMEM((cand_dev, LANE), F32),
                dma(3), dma(4 * NPEER), dma(4 * NPEER)],
            compiler_params=params(0), name="query_gather",
        )(features, w_in, w_out, targets[None, :], table_blk, cid_rows, logq_rows)
        query_all = h_all.reshape(ALL, LANE)
        t5 = tall.reshape(2, 4, 4, 4, TOK)
        tgt_all = jnp.concatenate([
            t5.transpose(0, 3, 1, 2, 4)[..., 0:24].reshape(2, -1),
            t5.transpose(0, 2, 3, 1, 4)[..., 24:48].reshape(2, -1),
            t5[..., 48:TOK].reshape(2, -1)], axis=1).reshape(TOK, LANE)
        steps = tok_total // TILE
        whole = lambda *shape: pl.BlockSpec(shape, lambda i: (0,) * len(shape))
        smem = pl.BlockSpec(memory_space=pltpu.SMEM)
        e, mc, stats, pos, codes, hc, te = pl.pallas_call(
            score_kernel, grid=(steps,),
            out_shape=[
                jax.ShapeDtypeStruct((16, cand_dev, PART), F32), jax.ShapeDtypeStruct((TOK, 8, LANE), F32), jax.ShapeDtypeStruct((steps, 3, 8, LANE), F32),
                jax.ShapeDtypeStruct((TOK, LANE), F32), jax.ShapeDtypeStruct((TOK, LANE), jnp.int32),
                jax.ShapeDtypeStruct((tok_total, LANE), F32), jax.ShapeDtypeStruct((tok_total + 8, LANE), F32)],
            in_specs=[whole(tok_total, LANE), whole(block_rows, LANE)] + [whole(cand_dev, LANE)] * 3 + [whole(TOK, LANE)],
            out_specs=[
                pl.BlockSpec((2, cand_dev, PART), lambda i: (i, 0, 0)), pl.BlockSpec((8, 8, LANE), lambda i: (i, 0, 0)),
                pl.BlockSpec((1, 3, 8, LANE), lambda i: (i, 0, 0, 0)), whole(TOK, LANE), whole(TOK, LANE), whole(tok_total, LANE), whole(tok_total + 8, LANE)],
            scratch_shapes=[
                pltpu.VMEM((TOK, LANE), F32), pltpu.VMEM((8, 8, LANE), F32), pltpu.VMEM((TOK, LANE), F32), pltpu.VMEM((LANE, LANE), F32), pltpu.VMEM((LANE, LANE), F32),
                pltpu.SMEM((1, LANE), jnp.int32), pltpu.SemaphoreType.DMA],
            compiler_params=pltpu.CompilerParams(dimension_semantics=("arbitrary",), vmem_limit_bytes=48 * KILO * KILO), name="score",
        )(query_all, table_blk, cand_rows, cidb, logqb, tgt_all)
        tiles, grad_tgt, loss_row, dcand = pl.pallas_call(
            grad_kernel,
            out_shape=[
                jax.ShapeDtypeStruct((384, 8, LANE), F32), jax.ShapeDtypeStruct((TOK, LANE), F32),
                jax.ShapeDtypeStruct((8, LANE), F32), jax.ShapeDtypeStruct((cand_dev, LANE), F32)],
            in_specs=[anyspec] + vmem(2) + [anyspec] * 6, out_specs=vmem(4),
            scratch_shapes=[
                pltpu.VMEM((16, cand_dev, PART), F32), pltpu.VMEM((80, 3, 8, LANE), F32), pltpu.VMEM((32, 3, 8, LANE), F32), pltpu.VMEM((TOK, LANE), F32),
                pltpu.VMEM((KILO, 8, LANE), F32), pltpu.VMEM((KILO, 8, LANE), F32),
                pltpu.VMEM((384, 8, LANE), F32), pltpu.VMEM((384, 8, LANE), F32),
                pltpu.VMEM((tok_total, LANE), F32), pltpu.VMEM((tok_total, LANE), BF16), pltpu.VMEM((LANE, cand_dev), BF16),
                pltpu.VMEM(features.shape, BF16), pltpu.VMEM(w_out.shape, BF16), pltpu.VMEM(pre.shape, F32),
                dma(6), dma(16), dma(8), dma(8), dma(4, 3 * NPEER), dma(4, 3 * NPEER)],
            compiler_params=params(1), name="grad_reduce",
        )(e, mc, stats, te, query_all, cand_t, features, w_out, pre)
        grad_blk, grad_w_in, grad_w_out, loss = pl.pallas_call(
            table_kernel,
            out_shape=[
                jax.ShapeDtypeStruct((block_rows, LANE), F32), jax.ShapeDtypeStruct(w_in.shape, F32), jax.ShapeDtypeStruct(w_out.shape, F32),
                jax.ShapeDtypeStruct((1, 1), F32)],
            in_specs=[smem, smem] + vmem(3) + [anyspec] * 3,
            out_specs=vmem(3) + [smem],
            scratch_shapes=[pltpu.VMEM((cand_dev, LANE), F32), pltpu.VMEM((384, 8, LANE), F32), pltpu.VMEM((LANE, LANE), F32), pltpu.VMEM((LANE, LANE), F32), dma(3)],
            compiler_params=pltpu.CompilerParams(vmem_limit_bytes=48 * KILO * KILO), name="table_grad",
        )(lax.dynamic_slice_in_dim(cand_ids, dev_index * cand_dev, cand_dev)[None, :], codes, grad_tgt, pos, loss_row, dcand, tiles, hc)
        loss = loss.reshape(())
        return loss, grad_blk, grad_w_in, grad_w_out

    return jax.shard_map(local_step, mesh=mesh, in_specs=(P("dp", None), P(), P(), P("dp", None), P(), P(), P("dp")), out_specs=(P(), P("dp", None), P(), P()), check_vma=False)
```

```python
import functools
import jax
import jax.numpy as jnp
from jax import lax
from jax.experimental import pallas as pl
from jax.experimental.pallas import tpu as pltpu
from jax.sharding import PartitionSpec as P

MESH = pl.DeviceIdType.MESH
F32, BF16 = jnp.float32, jnp.bfloat16
COORD = {"core": (1, 2), "x": (2, 4), "y": (8, 4), "z": (32, 4)}
ORDERS = (("x", "y", "z"), ("y", "z", "x"), ("z", "x", "y"))
NDEV = 128
NPEER = 10
LANE, TOK, ALL, KILO, WIDE = 128, 64, 8192, 1024, 256


def one(i):
    return pl.ds(i, 1)


def down(v):
    return jnp.sum(v, axis=0, keepdims=True)


def across(v):
    return jnp.sum(v, axis=1, keepdims=True)


def peak(v):
    return jnp.max(v, axis=0, keepdims=True)


def flag(mask):
    return jnp.where(mask, 1.0, 0.0)


def iota(shape, dim):
    return lax.broadcasted_iota(jnp.int32, shape, dim)


def coord(me, axis):
    stride, radix = COORD[axis]
    return (me // stride) % radix


def peer(me, axis, k):
    stride, radix = COORD[axis]
    c = coord(me, axis)
    return me + ((c + k) % radix - c) * stride


def block_index(me, order):
    idx, weight = 0, 1
    for axis in order:
        idx = idx + coord(me, axis) * weight
        weight *= COORD[axis][1]
    return idx


def greet(me):
    barrier = pltpu.get_barrier_semaphore()
    for axis in COORD:
        for k in range(1, COORD[axis][1]):
            pl.semaphore_signal(barrier, inc=1, device_id=(peer(me, axis, k),), device_id_type=MESH)
    return barrier


def remote(src, dst, send, recv, dev):
    return pltpu.make_async_remote_copy(src_ref=src, dst_ref=dst, send_sem=send, recv_sem=recv, device_id=(dev,), device_id_type=MESH)


def gather_streams(me, streams, bulk, send_sem, recv_sem, between=None):
    pending, sent = [None] * len(streams), []
    for phase in range(4):
        for s, (ref, off, unit, order) in enumerate(streams):
            if pending[s]:
                for c in pending[s]:
                    c.wait_recv()
            if phase == 3:
                continue
            span = 4 ** phase
            idx = block_index(me, order)
            where = ref.at[pl.ds(off + (idx - idx % span) * unit, span * unit)]
            pending[s] = []
            for k in range(1, 4):
                n = s * 9 + phase * 3 + k - 1
                c = remote(where, where, send_sem.at[n], recv_sem.at[n], peer(me, order[phase], k))
                c.start()
                pending[s].append(c)
                sent.append(c)
        if between and phase < 3:
            between(phase)
    last = []
    for i, (ref, count) in enumerate(bulk):
        n = len(streams) * 9 + i
        where = ref.at[pl.ds(coord(me, "core") * count, count)]
        c = remote(where, where, send_sem.at[n], recv_sem.at[n], peer(me, "core", 1))
        c.start()
        last.append(c)
    if between:
        between(3)
    for c in last:
        c.wait_recv()
    return sent + last


def add_rows(ref, start, rref, base, count, parts):
    def add(i, carry):
        acc = ref[start + i]
        for k in range(parts):
            acc = acc + rref[base + k * count + i]
        ref[start + i] = acc
        return carry

    lax.fori_loop(0, count, add, 0, unroll=4)


def scatter_streams(me, ref, first, rref, rbase, streams, send_sem, recv_sem, prepare=None, between=None):
    sent = []
    pending = [None] * 3
    for step in range(4):
        for s, (off, unit, order) in enumerate(streams):
            idx = block_index(me, order)
            if pending[s]:
                for c in pending[s][0]:
                    c.wait_recv()
                add_rows(ref, pending[s][1], rref, pending[s][2], pending[s][3], 3)
            if step == 3:
                continue
            if step == 0 and prepare:
                prepare(s)
            span = 4 ** (2 - step)
            axis = order[2 - step]
            start = first + off + (idx - idx % (4 * span)) * unit
            d = coord(me, axis)
            copies = []
            for k in range(1, 4):
                n = s * 9 + step * 3 + k - 1
                src = ref.at[pl.ds(start + (d + k) % 4 * span * unit, span * unit)]
                dst = rref.at[pl.ds(rbase + (k - 1) * span * unit, span * unit)]
                c = remote(src, dst, send_sem.at[n], recv_sem.at[n], peer(me, axis, k))
                c.start()
                copies.append(c)
            sent += copies
            pending[s] = (copies, start + d * span * unit, rbase, span * unit)
            rbase += 3 * span * unit
        if step == 0 and between:
            between()
    return sent


def gelu_parts(a):
    c = 0.7978845608028654
    inner = jnp.tanh(c * (a + 0.044715 * (a * a * a)))
    half = 0.5 * (1.0 + inner)
    return a * half, half + 0.5 * a * (1.0 - inner * inner) * (c * (1.0 + 3.0 * 0.044715 * (a * a)))


def nt_dot(a, b):
    return lax.dot_general(a, b, (((1,), (1,)), ((), ())), preferred_element_type=F32)


def tn_dot(a, b):
    return lax.dot_general(a, b, (((0,), (0,)), ((), ())), preferred_element_type=F32)


H_OFF = (0, 192, 384)
H_UNIT = (3, 3, 2)
H_FIRST = (0, 3, 6)


def column(row):
    return jnp.transpose(jnp.broadcast_to(row, (LANE, LANE)))


def query_kernel(x_ref, win_ref, wout_ref, tgt_ref, blk_ref, cid_ref, logq_ref, tall_ref, h_out, pre_out, cand_out, candt_out, cidb_out, logqb_out,
                 blk, ids, lqs, rows, h_ref, pre_ref, cand_ref, candt_ref, cidb_ref, logqb_ref, load_sem, out_sem, send_sem, recv_sem):
    me = lax.axis_index("dp")
    mine = pl.ds(pl.multiple_of(me * 8, 8), 8)
    loads = [
        pltpu.make_async_copy(cid_ref.at[mine], ids, load_sem.at[0]), pltpu.make_async_copy(logq_ref.at[mine], lqs, load_sem.at[1]),
        pltpu.make_async_copy(blk_ref, blk, load_sem.at[2])]
    for c in loads:
        c.start()
    pl.semaphore_wait(greet(me), NPEER)
    pre = jnp.dot(x_ref[...], win_ref[...], preferred_element_type=F32)
    pre_ref[...] = pre
    act = gelu_parts(pre)[0].astype(BF16)
    query = jnp.dot(act, wout_ref[...], preferred_element_type=F32)
    core = coord(me, "core")
    streams = []
    for s in range(3):
        idx = block_index(me, ORDERS[s])
        for g in range(H_UNIT[s]):
            row = 8 * (H_FIRST[s] + g)
            h_ref[core * 512 + H_OFF[s] + idx * H_UNIT[s] + g] = query[row : row + 8, :].astype(BF16)
        streams.append((h_ref, core * 512 + H_OFF[s], H_UNIT[s], ORDERS[s]))
    tall_ref[core * TOK + block_index(me, ORDERS[2])] = tgt_ref[...]
    streams.append((tall_ref, core * TOK, 1, ORDERS[2]))
    lane = iota((1, LANE), 1)

    def pick(n, carry):
        part = pl.ds(pl.multiple_of(n // 8 * WIDE, WIDE), WIDE)
        first = n % 8 * KILO
        want = cidb_ref[part, :]
        picks = [flag(want == (lane + (first + u * LANE)).astype(F32)).astype(BF16) for u in range(8)]
        rows[part, :] += jnp.dot(jnp.concatenate(picks, axis=1), blk[pl.ds(pl.multiple_of(first, KILO), KILO), :], preferred_element_type=F32)
        return carry

    def fill(phase):
        if phase == 0:
            for c in loads:
                c.wait()
            for c in range(8):
                at = slice(c * LANE, c * LANE + LANE)
                cidb_ref[at, :] = column((ids[c : c + 1, :] - me * ALL).astype(F32))
                logqb_ref[at, :] = column(lqs[c : c + 1, :])
            rows[...] = jnp.zeros_like(rows)
        bounds = (0, 8, 17, 32, 32)
        lax.fori_loop(bounds[phase], bounds[phase + 1], pick, 0)
        if phase == 2:
            cand_ref[...] = rows[...].astype(BF16)
            candt_ref[...] = jnp.transpose(rows[...]).astype(BF16)
            for c in outs:
                c.start()
        if phase == 3:
            half(core).start()

    outs = [
        pltpu.make_async_copy(a, b, out_sem.at[i]) for i, (a, b) in enumerate([
            (pre_ref, pre_out), (cand_ref, cand_out), (candt_ref, candt_out), (cidb_ref, cidb_out), (logqb_ref, logqb_out)])]

    def half(c):
        where = pl.ds(c * 512, 512)
        return pltpu.make_async_copy(h_ref.at[where], h_out.at[where], out_sem.at[5 + c])

    sent = gather_streams(me, streams, [(h_ref, 512), (tall_ref, TOK)], send_sem, recv_sem, fill)
    half(1 - core).start()
    for c in outs:
        c.wait()
    for c in sent:
        c.wait_send()
    half(core).wait()
    half(1 - core).wait()


def reduce_stats(me, st_ref, recv, cur, send_sem, recv_sem):
    sent = []
    pending = [None] * 3
    for phase in range(5):
        for s in range(3):
            g0, ng = H_FIRST[s], H_UNIT[s]
            if phase:
                for c in pending[s]:
                    c.wait_recv()
                base = 8 * (0, 3, 6, 9)[phase - 1]
                npart = len(pending[s])

                def merge(g, carry, phase=phase, base=base, npart=npart):
                    old = st_ref[g] if phase == 1 else cur[8 * (phase - 2) + g]
                    parts = [recv[base + 8 * k + g] for k in range(npart)]
                    top, z = old[0], old[2]
                    for p in parts:
                        top = jnp.maximum(top, p[0])
                        z = jnp.maximum(z, p[2])
                    total = old[1] * jnp.exp(old[0] - top)
                    for p in parts:
                        total = total + p[1] * jnp.exp(p[0] - top)
                    row = 8 * (phase - 1) + g
                    cur[row, 0] = top
                    cur[row, 1] = total
                    cur[row, 2] = z
                    return carry

                lax.fori_loop(g0, g0 + ng, merge, 0)
            if phase == 4:
                continue
            axis = (ORDERS[s] + ("core",))[phase]
            src = st_ref.at[pl.ds(g0, ng)] if phase == 0 else cur.at[pl.ds(8 * (phase - 1) + g0, ng)]
            base = 8 * (0, 3, 6, 9)[phase]
            pending[s] = []
            for k in range(1, COORD[axis][1]):
                n = s * NPEER + phase * 3 + k - 1
                c = remote(src, recv.at[pl.ds(base + 8 * (k - 1) + g0, ng)], send_sem.at[n], recv_sem.at[n], peer(me, axis, k))
                c.start()
                pending[s].append(c)
                sent.append(c)
    return sent


TILE = KILO


def target_kernel(tgt_ref, h_hbm, blk_hbm, zst_ref, pos_ref, code_ref, hc_ref, te_out, h_ref, blk_ref, te_ref, zd, hs, es, codes, load_sem, sem):
    block_rows = blk_ref.shape[0]
    loads = [pltpu.make_async_copy(h_hbm, h_ref, load_sem.at[0]), pltpu.make_async_copy(blk_hbm, blk_ref, load_sem.at[1])]
    for c in loads:
        c.start()
    rel = tgt_ref[...] - lax.axis_index("dp") * block_rows
    own = (rel >= 0) & (rel < block_rows)
    own_f = flag(own)
    own_b = own_f.astype(BF16)
    up = iota((LANE, LANE), 0) < iota((LANE, LANE), 1)
    prefix = jnp.dot(own_b, flag(up).astype(BF16), preferred_element_type=F32)
    total = jnp.dot(own_b, jnp.ones((LANE, LANE), BF16), preferred_element_type=F32)
    low = iota((TOK, TOK), 0) > iota((TOK, TOK), 1)
    offset = jnp.dot(flag(low).astype(BF16), total.astype(BF16), preferred_element_type=F32)
    pos_ref[...] = jnp.where(own, prefix + offset, -1.0)
    zd[...] = jnp.zeros_like(zd)

    def clear(i, carry):
        te_ref[pl.ds(pl.multiple_of(i * LANE, LANE), LANE), :] = jnp.zeros((LANE, LANE), F32)
        return carry

    lax.fori_loop(0, TOK, clear, 0)
    count = jnp.sum(own_f).astype(jnp.int32)
    for c in loads:
        c.wait()
    slot0 = iota((LANE, LANE), 0).astype(F32)
    lane = iota((1, LANE), 1)
    sub = iota((16, LANE), 0)

    def one_row(ref, i):
        tile = ref[pl.ds(pl.multiple_of(i // 16 * 16, 16), 16), :].astype(F32)
        return down(jnp.where(sub == i % 16, tile, 0.0))

    def chunk(c, carry):
        slot = slot0 + (c * LANE).astype(F32)

        def collect(r, code):
            mark = (tgt_ref[one(r), :] % block_rows) * ALL + (lane + r * LANE)
            return code + jnp.where(pos_ref[one(r), :] == slot, mark, 0)

        code = lax.fori_loop(0, TOK, collect, jnp.zeros((LANE, LANE), jnp.int32), unroll=8)
        row = across((code // ALL).astype(F32))
        tok = across((code % ALL).astype(F32))
        both = row.astype(jnp.int32) * ALL + tok.astype(jnp.int32)
        code_ref[one(c), :] = jnp.transpose(jnp.broadcast_to(both, (LANE, LANE)))[0:1, :]
        copy = pltpu.make_async_copy(code_ref.at[one(c)], codes, sem)
        copy.start()
        copy.wait()
        left = count - c * LANE

        def fetch(i, carry2):
            for u in range(8):
                n = i * 8 + u
                v = codes[0, n]
                hs[one(n), :] = one_row(h_ref, v % ALL)
                row = one_row(blk_ref, v // ALL)
                es[one(n), :] = row
                te_ref[one(jnp.where(n < left, v % ALL, ALL)), :] = row
            return carry2

        lax.fori_loop(0, (jnp.minimum(left, LANE) + 7) // 8, fetch, 0)
        keep = pltpu.make_async_copy(hs, hc_ref.at[pl.ds(pl.multiple_of(c * LANE, LANE), LANE)], load_sem.at[3])
        keep.start()
        z = jnp.broadcast_to(across(hs[...] * es[...]), (LANE, LANE))

        def spread(r, carry2):
            hit = pos_ref[one(r), :] == slot
            zd[one(r), :] += down(jnp.where(hit, z, 0.0))
            return carry2

        lax.fori_loop(0, TOK, spread, 0, unroll=8)
        keep.wait()
        return carry

    lax.fori_loop(0, (count + 127) // LANE, chunk, 0)
    copy = pltpu.make_async_copy(te_ref.at[pl.ds(0, ALL)], te_out, load_sem.at[2])
    copy.start()
    zst_ref[...] = jnp.where(pos_ref[...] >= 0.0, zd[...], -jnp.inf)
    copy.wait()


def table_kernel(code_ref, g_ref, pos_ref, lossrow_ref, cid_hbm, dcand_hbm, tiles_hbm, hc_ref, de_ref, dwin_ref, dwout_ref, loss_ref, cidx, dcand, whole, hc, gh, sem):
    me = lax.axis_index("dp")
    loads = [pltpu.make_async_copy(cid_hbm.at[pl.ds(pl.multiple_of(me * 8, 8), 8)], cidx, sem.at[3]), pltpu.make_async_copy(dcand_hbm, dcand, sem.at[0]), pltpu.make_async_copy(tiles_hbm, whole, sem.at[1])]
    for c in loads:
        c.start()
    loss_ref[0, 0] = jnp.max(lossrow_ref[...])

    def clear(i, carry):
        de_ref[pl.ds(pl.multiple_of(i * LANE, LANE), LANE), :] = jnp.zeros((LANE, LANE), F32)
        return carry

    lax.fori_loop(0, de_ref.shape[0] // LANE, clear, 0)
    for c in loads:
        c.wait()

    base = me * ALL

    def place(i, carry):
        for u in range(8):
            n = i * 8 + u
            de_ref[one(cidx[i // 16, i % 16 * 8 + u] - base), :] = dcand[one(n), :]
        return carry

    lax.fori_loop(0, dcand.shape[0] // 8, place, 0)
    count = jnp.sum(flag(pos_ref[...] >= 0.0)).astype(jnp.int32)
    slot0 = iota((LANE, LANE), 0).astype(F32)

    def chunk(c, carry):
        slot = slot0 + (c * LANE).astype(F32)
        copy = pltpu.make_async_copy(hc_ref.at[pl.ds(pl.multiple_of(c * LANE, LANE), LANE)], hc, sem.at[2])
        copy.start()

        def collect(r, acc):
            return acc + jnp.where(pos_ref[one(r), :] == slot, g_ref[one(r), :], 0.0)

        g = jnp.sum(lax.fori_loop(0, TOK, collect, jnp.zeros((LANE, LANE), F32), unroll=8), axis=1, keepdims=True)
        copy.wait()
        gh[...] = g * hc[...]

        def put(i, carry2):
            de_ref[one(code_ref[c, i] // ALL), :] += gh[one(i), :]
            return carry2

        lax.fori_loop(0, jnp.minimum(count - c * LANE, LANE), put, 0)
        return carry

    lax.fori_loop(0, (count + 127) // LANE, chunk, 0)
    dwout_ref[...] = whole[0:LANE].reshape(KILO, LANE)
    for j in range(8):
        dwin_ref[:, LANE * j : LANE * j + LANE] = whole[LANE + 32 * j : 160 + 32 * j].reshape(WIDE, LANE)


LAST = 27
PART = 512


def core_exchange(me, ref, half, rref, send, recv):
    mine = coord(me, "core")
    c = remote(ref.at[pl.ds((1 - mine) * half, half)], rref.at[pl.ds(0, half)], send, recv, peer(me, "core", 1))
    c.start()
    c.wait_recv()
    add_rows(ref, mine * half, rref, 0, half, 1)
    return [c]


def grad_kernel(tgt_ref, zst_ref, h_hbm, cand_hbm, cidb_hbm, logqb_hbm, candt_hbm, te_hbm, x_hbm, wout_hbm, pre_hbm, g_ref, loss_ref, tiles_out, dcand_out,
                ebuf, mc_ref, st_ref, part, local, srecv, cur, norm, acc, recv, tiles, trecv, whole, dcand_ref,
                h_ref, cand_ref, cidb, logqb, candt_ref, te_ref, x_ref, wout_ref, pre_ref,
                load_sem, core_send, core_recv, send_sem, recv_sem):
    me = lax.axis_index("dp")
    core = coord(me, "core")
    loads = [
        pltpu.make_async_copy(a, b, load_sem.at[i]) for i, (a, b) in enumerate([
            (cand_hbm, cand_ref), (cidb_hbm, cidb), (logqb_hbm, logqb), (h_hbm, h_ref),
            (candt_hbm, candt_ref), (te_hbm, te_ref), (x_hbm, x_ref), (wout_hbm, wout_ref), (pre_hbm, pre_ref)])]
    for c in loads:
        c.start()
    barrier = greet(me)
    local[...] = (tgt_ref[...] - me * ALL).astype(F32)
    for g in range(8):
        st_ref[g, 2] = zst_ref[8 * g : 8 * g + 8, :]
    for c in loads[:4]:
        c.wait()

    def score(t, carry):
        for j in range(2):
            dots = nt_dot(cand_ref[...], h_ref[pl.ds(pl.multiple_of(t * PART + WIDE * j, WIDE), WIDE), :])
            for half in range(2):
                q = 2 * j + half
                r = t * 4 + q
                tgt = local[one(r), :]
                for c in range(8):
                    rows = slice(LANE * c, LANE * c + LANE)
                    s = dots[rows, LANE * half : LANE * half + LANE] - logqb[rows, :]
                    s = jnp.where(cidb[rows, :] == tgt, -1e9, s)
                    m = peak(s)
                    e = jnp.exp(s - m)
                    ebuf[t, rows, LANE * q : LANE * q + LANE] = e
                    mc_ref[r, c : c + 1, :] = m
                    part[q, c : c + 1, :] = down(e)
                most = mc_ref[r]
                top = peak(most)
                row = one(t % 2 * 4 + q)
                st_ref[t // 2, 0, row, :] = top
                st_ref[t // 2, 1, row, :] = down(part[q] * jnp.exp(most - top))
        return carry

    lax.fori_loop(0, 16, score, 0)
    pl.semaphore_wait(barrier, NPEER)
    sent = reduce_stats(me, st_ref, srecv, cur, send_sem.at[3], recv_sem.at[3])
    total = jnp.zeros((8, LANE), F32)
    for g in range(8):
        m, t, z = cur[24 + g, 0], cur[24 + g, 1], cur[24 + g, 2]
        top = jnp.maximum(m, z)
        log_norm = top + jnp.log(t * jnp.exp(m - top) + jnp.exp(z - top))
        total = total + (log_norm - z)
        norm[8 * g : 8 * g + 8, :] = log_norm
        g_ref[8 * g : 8 * g + 8, :] = (jnp.exp(z - log_norm) - 1.0) / ALL
    loss_ref[...] = jnp.broadcast_to(jnp.sum(total, keepdims=True) / ALL, loss_ref.shape)

    def probs(t):
        blocks = []
        for q in range(4):
            r = t * 4 + q
            scale = jnp.exp(mc_ref[r] - norm[one(r), :]) / ALL
            blocks.append(jnp.concatenate([
                (ebuf[t, LANE * c : LANE * c + LANE, LANE * q : LANE * q + LANE] * scale[c : c + 1, :]).astype(BF16) for c in range(8)], axis=0))
        return jnp.concatenate(blocks, axis=1)

    for c in loads[4:]:
        c.wait()

    def query_grad(t):
        dqt = jnp.dot(candt_ref[...], probs(t), preferred_element_type=F32)
        gcol = jnp.concatenate([column(g_ref[one(t * 4 + q), :]) for q in range(4)], axis=0)
        dq = jnp.transpose(dqt) + gcol * te_ref[pl.ds(pl.multiple_of(t * PART, PART), PART), :]
        return dq.reshape(TOK, 8, LANE)

    def swap(i):
        return remote(acc.at[pl.ds(((1 - core) * 8 + i) * TOK, TOK)], recv.at[pl.ds(i * TOK, TOK)], core_send.at[i], core_recv.at[i], peer(me, "core", 1))

    def give(i, carry):
        t = (1 - core) * 8 + i
        acc[pl.ds(t * TOK, TOK)] = query_grad(t)
        swap(i).start()
        return carry

    def keep(i, carry):
        t = core * 8 + i
        val = query_grad(t)
        swap(i).wait_recv()
        acc[pl.ds(t * TOK, TOK)] = val + recv[pl.ds(i * TOK, TOK)]
        return carry

    lax.fori_loop(0, 8, give, 0)

    def prepare(s):
        lax.fori_loop(H_FIRST[s], H_FIRST[s] + H_UNIT[s], keep, 0)

    def cand_grad():
        dcand_ref[...] = jnp.zeros_like(dcand_ref)

        def accumulate(t, carry):
            dcand_ref[...] += jnp.dot(probs(t), h_ref[pl.ds(pl.multiple_of(t * PART, PART), PART), :], preferred_element_type=F32)
            return carry

        lax.fori_loop(0, 16, accumulate, 0)
        dcand_copy.start()

    dcand_copy = pltpu.make_async_copy(dcand_ref, dcand_out, load_sem.at[9])
    streams = [(H_OFF[s], H_UNIT[s], ORDERS[s]) for s in range(3)]
    sent += scatter_streams(me, acc, core * 512, recv, 512, streams, send_sem.at[0], recv_sem.at[0], prepare, cand_grad)
    rows = []
    for s in range(3):
        idx = block_index(me, ORDERS[s])
        for g in range(H_UNIT[s]):
            rows.append(acc[core * 512 + H_OFF[s] + idx * H_UNIT[s] + g])
    dh = jnp.concatenate(rows, axis=0).astype(BF16)
    act, slope = gelu_parts(pre_ref[...])
    d_pre = (slope * nt_dot(dh, wout_ref[...])).astype(BF16)
    dw_out = tn_dot(act.astype(BF16), dh)
    tiles[0:LANE] = dw_out.reshape(LANE, 8, LANE)
    dw_in = tn_dot(x_ref[...], d_pre)
    for j in range(8):
        tiles[LANE + 32 * j : 160 + 32 * j] = dw_in[:, LANE * j : LANE * j + LANE].reshape(32, 8, LANE)
    streams = [(TOK * s, 1, ORDERS[s]) for s in range(3)]
    half = core_exchange(me, tiles, 192, trecv, send_sem.at[1, LAST], recv_sem.at[1, LAST])
    sent += half + scatter_streams(me, tiles, core * 192, trecv, 192, streams, send_sem.at[1], recv_sem.at[1])
    streams = []
    for s in range(3):
        own = core * 192 + TOK * s + block_index(me, ORDERS[s])
        whole[own] = tiles[own]
        streams.append((whole, core * 192 + TOK * s, 1, ORDERS[s]))
    sent += gather_streams(me, streams, [(whole, 192)], send_sem.at[2], recv_sem.at[2])
    tiles_copy = pltpu.make_async_copy(whole, tiles_out, load_sem.at[10])
    tiles_copy.start()
    dcand_copy.wait()
    for c in sent:
        c.wait_send()

    def swap_done(i, carry):
        swap(i).wait_send()
        return carry

    lax.fori_loop(0, 8, swap_done, 0)
    tiles_copy.wait()


def vmem(n):
    return [pl.BlockSpec(memory_space=pltpu.VMEM)] * n


def params(cid):
    return pltpu.CompilerParams(collective_id=cid, has_side_effects=True, vmem_limit_bytes=63 * KILO * KILO)


def dma(*shape):
    return pltpu.SemaphoreType.DMA(shape)


def solution(mesh):
    num_dev = mesh.shape["dp"]

    def local_step(features, w_in, w_out, table_blk, cand_ids, log_q, targets):
        dev_index = lax.axis_index("dp")
        block_rows = table_blk.shape[0]
        cand_dev = cand_ids.shape[0] // num_dev
        tok_total = features.shape[0] * num_dev
        anyspec = pl.BlockSpec(memory_space=pl.ANY)
        cid_rows, logq_rows = cand_ids.reshape(KILO, LANE), log_q.reshape(KILO, LANE)
        tall, h_all, pre, cand_rows, cand_t, cidb, logqb = pl.pallas_call(
            query_kernel,
            out_shape=[
                jax.ShapeDtypeStruct((LANE, 1, TOK), jnp.int32), jax.ShapeDtypeStruct((KILO, 8, LANE), BF16), jax.ShapeDtypeStruct((TOK, KILO), F32),
                jax.ShapeDtypeStruct((cand_dev, LANE), BF16), jax.ShapeDtypeStruct((LANE, cand_dev), BF16),
                jax.ShapeDtypeStruct((cand_dev, LANE), F32), jax.ShapeDtypeStruct((cand_dev, LANE), F32)],
            in_specs=vmem(4) + [anyspec] * 3, out_specs=vmem(1) + [anyspec] * 6,
            scratch_shapes=[
                pltpu.VMEM((block_rows, LANE), BF16), pltpu.VMEM((8, LANE), jnp.int32), pltpu.VMEM((8, LANE), F32), pltpu.VMEM((cand_dev, LANE), F32),
                pltpu.VMEM((KILO, 8, LANE), BF16), pltpu.VMEM((TOK, KILO), F32), pltpu.VMEM((cand_dev, LANE), BF16), pltpu.VMEM((LANE, cand_dev), BF16),
                pltpu.VMEM((cand_dev, LANE), F32), pltpu.VMEM((cand_dev, LANE), F32),
                dma(3), dma(7), dma(4 * NPEER), dma(4 * NPEER)],
            compiler_params=params(0), name="query_gather",
        )(features, w_in, w_out, targets[None, :], table_blk, cid_rows, logq_rows)
        query_all = h_all.reshape(ALL, LANE)
        t5 = tall.reshape(2, 4, 4, 4, TOK)
        tgt_all = jnp.concatenate([
            t5.transpose(0, 3, 1, 2, 4)[..., 0:24].reshape(2, -1),
            t5.transpose(0, 2, 3, 1, 4)[..., 24:48].reshape(2, -1),
            t5[..., 48:TOK].reshape(2, -1)], axis=1).reshape(TOK, LANE)
        smem = pl.BlockSpec(memory_space=pltpu.SMEM)
        square = pltpu.VMEM((LANE, LANE), F32)
        big = pltpu.CompilerParams(vmem_limit_bytes=48 * KILO * KILO)
        zst, pos, codes, hc, te = pl.pallas_call(
            target_kernel,
            out_shape=[
                jax.ShapeDtypeStruct((TOK, LANE), F32), jax.ShapeDtypeStruct((TOK, LANE), F32), jax.ShapeDtypeStruct((TOK, LANE), jnp.int32),
                jax.ShapeDtypeStruct((tok_total, LANE), F32), jax.ShapeDtypeStruct((tok_total, LANE), F32)],
            in_specs=vmem(1) + [anyspec] * 2, out_specs=vmem(3) + [anyspec] * 2,
            scratch_shapes=[
                pltpu.VMEM((tok_total, LANE), BF16), pltpu.VMEM((block_rows, LANE), BF16), pltpu.VMEM((tok_total + 8, LANE), F32), pltpu.VMEM((TOK, LANE), F32),
                square, square, pltpu.SMEM((1, LANE), jnp.int32), dma(4), pltpu.SemaphoreType.DMA],
            compiler_params=big, name="target_rows",
        )(tgt_all, query_all, table_blk)
        grad_tgt, loss_row, tiles, dcand = pl.pallas_call(
            grad_kernel,
            out_shape=[
                jax.ShapeDtypeStruct((TOK, LANE), F32), jax.ShapeDtypeStruct((8, LANE), F32),
                jax.ShapeDtypeStruct((384, 8, LANE), F32), jax.ShapeDtypeStruct((cand_dev, LANE), F32)],
            in_specs=vmem(2) + [anyspec] * 9, out_specs=vmem(2) + [anyspec] * 2,
            scratch_shapes=[
                pltpu.VMEM((16, cand_dev, PART), F32), pltpu.VMEM((TOK, 8, LANE), F32), pltpu.VMEM((8, 3, 8, LANE), F32), pltpu.VMEM((4, 8, LANE), F32), pltpu.VMEM((TOK, LANE), F32),
                pltpu.VMEM((80, 3, 8, LANE), F32), pltpu.VMEM((32, 3, 8, LANE), F32), pltpu.VMEM((TOK, LANE), F32),
                pltpu.VMEM((KILO, 8, LANE), F32), pltpu.VMEM((KILO, 8, LANE), F32),
                pltpu.VMEM((384, 8, LANE), F32), pltpu.VMEM((384, 8, LANE), F32), pltpu.VMEM((384, 8, LANE), F32), pltpu.VMEM((cand_dev, LANE), F32),
                pltpu.VMEM((tok_total, LANE), BF16), pltpu.VMEM((cand_dev, LANE), BF16), pltpu.VMEM((cand_dev, LANE), F32), pltpu.VMEM((cand_dev, LANE), F32),
                pltpu.VMEM((LANE, cand_dev), BF16), pltpu.VMEM((tok_total, LANE), F32),
                pltpu.VMEM(features.shape, BF16), pltpu.VMEM(w_out.shape, BF16), pltpu.VMEM(pre.shape, F32),
                dma(11), dma(8), dma(8), dma(4, 3 * NPEER), dma(4, 3 * NPEER)],
            compiler_params=params(1), name="grad_reduce",
        )(tgt_all, zst, query_all, cand_rows, cidb, logqb, cand_t, te, features, w_out, pre)
        grad_blk, grad_w_in, grad_w_out, loss = pl.pallas_call(
            table_kernel,
            out_shape=[
                jax.ShapeDtypeStruct((block_rows, LANE), F32), jax.ShapeDtypeStruct(w_in.shape, F32), jax.ShapeDtypeStruct(w_out.shape, F32),
                jax.ShapeDtypeStruct((1, 1), F32)],
            in_specs=[smem] + vmem(3) + [anyspec] * 4, out_specs=vmem(3) + [smem],
            scratch_shapes=[pltpu.SMEM((8, LANE), jnp.int32), pltpu.VMEM((cand_dev, LANE), F32), pltpu.VMEM((384, 8, LANE), F32), square, square, dma(4)],
            compiler_params=big, name="table_grad",
        )(codes, grad_tgt, pos, loss_row, cid_rows, dcand, tiles, hc)
        loss = loss.reshape(())
        return loss, grad_blk, grad_w_in, grad_w_out

    return jax.shard_map(local_step, mesh=mesh, in_specs=(P("dp", None), P(), P(), P("dp", None), P(), P(), P("dp")), out_specs=(P(), P("dp", None), P(), P()), check_vma=False)
```

```python
import functools
import jax
import jax.numpy as jnp
from jax import lax
from jax.experimental import pallas as pl
from jax.experimental.pallas import tpu as pltpu
from jax.sharding import PartitionSpec as P

MESH = pl.DeviceIdType.MESH
F32, BF16 = jnp.float32, jnp.bfloat16
COORD = {"core": (1, 2), "x": (2, 4), "y": (8, 4), "z": (32, 4)}
ORDERS = (("x", "y", "z"), ("y", "z", "x"), ("z", "x", "y"))
NDEV = 128
NPEER = 10
LANE, TOK, ALL, KILO, WIDE = 128, 64, 8192, 1024, 256


def one(i):
    return pl.ds(i, 1)


def down(v):
    return jnp.sum(v, axis=0, keepdims=True)


def across(v):
    return jnp.sum(v, axis=1, keepdims=True)


def peak(v):
    return jnp.max(v, axis=0, keepdims=True)


def flag(mask):
    return jnp.where(mask, 1.0, 0.0)


def iota(shape, dim):
    return lax.broadcasted_iota(jnp.int32, shape, dim)


def coord(me, axis):
    stride, radix = COORD[axis]
    return (me // stride) % radix


def peer(me, axis, k):
    stride, radix = COORD[axis]
    c = coord(me, axis)
    return me + ((c + k) % radix - c) * stride


def block_index(me, order):
    idx, weight = 0, 1
    for axis in order:
        idx = idx + coord(me, axis) * weight
        weight *= COORD[axis][1]
    return idx


def greet(me):
    barrier = pltpu.get_barrier_semaphore()
    for axis in COORD:
        for k in range(1, COORD[axis][1]):
            pl.semaphore_signal(barrier, inc=1, device_id=(peer(me, axis, k),), device_id_type=MESH)
    return barrier


def remote(src, dst, send, recv, dev):
    return pltpu.make_async_remote_copy(src_ref=src, dst_ref=dst, send_sem=send, recv_sem=recv, device_id=(dev,), device_id_type=MESH)


def gather_streams(me, streams, bulk, send_sem, recv_sem, between=None):
    pending, sent = [None] * len(streams), []
    for phase in range(4):
        for s, (ref, off, unit, order) in enumerate(streams):
            if pending[s]:
                for c in pending[s]:
                    c.wait_recv()
            if phase == 3:
                continue
            span = 4 ** phase
            idx = block_index(me, order)
            where = ref.at[pl.ds(off + (idx - idx % span) * unit, span * unit)]
            pending[s] = []
            for k in range(1, 4):
                n = s * 9 + phase * 3 + k - 1
                c = remote(where, where, send_sem.at[n], recv_sem.at[n], peer(me, order[phase], k))
                c.start()
                pending[s].append(c)
                sent.append(c)
        if between and phase < 3:
            between(phase)
    last = []
    for i, (ref, count) in enumerate(bulk):
        n = len(streams) * 9 + i
        where = ref.at[pl.ds(coord(me, "core") * count, count)]
        c = remote(where, where, send_sem.at[n], recv_sem.at[n], peer(me, "core", 1))
        c.start()
        last.append(c)
    if between:
        between(3)
    for c in last:
        c.wait_recv()
    return sent + last


def add_rows(ref, start, rref, base, count, parts):
    def add(i, carry):
        acc = ref[start + i]
        for k in range(parts):
            acc = acc + rref[base + k * count + i]
        ref[start + i] = acc
        return carry

    lax.fori_loop(0, count, add, 0, unroll=4)


class Scatter:
    def __init__(self, me, ref, first, rref, rbase, streams, send_sem, recv_sem):
        self.me, self.ref, self.first, self.rref, self.rbase = me, ref, first, rref, rbase
        self.streams, self.sems = streams, (send_sem, recv_sem)
        self.step, self.pending, self.sent = [0] * 3, [None] * 3, []

    def send(self, s):
        off, unit, order = self.streams[s]
        step, me = self.step[s], self.me
        span = 4 ** (2 - step)
        axis = order[2 - step]
        idx = block_index(me, order)
        start = self.first + off + (idx - idx % (4 * span)) * unit
        d = coord(me, axis)
        copies = []
        for k in range(1, 4):
            n = s * 9 + step * 3 + k - 1
            src = self.ref.at[pl.ds(start + (d + k) % 4 * span * unit, span * unit)]
            dst = self.rref.at[pl.ds(self.rbase + (k - 1) * span * unit, span * unit)]
            c = remote(src, dst, self.sems[0].at[n], self.sems[1].at[n], peer(me, axis, k))
            c.start()
            copies.append(c)
        self.sent += copies
        self.pending[s] = (copies, start + d * span * unit, self.rbase, span * unit)
        self.rbase += 3 * span * unit
        self.step[s] += 1

    def receive(self, s):
        copies, start, base, count = self.pending[s]
        for c in copies:
            c.wait_recv()
        add_rows(self.ref, start, self.rref, base, count, 3)

    def rest(self):
        for step in range(3):
            for s in range(3):
                self.receive(s)
                if step < 2:
                    self.send(s)


def gelu_parts(a):
    c = 0.7978845608028654
    inner = jnp.tanh(c * (a + 0.044715 * (a * a * a)))
    half = 0.5 * (1.0 + inner)
    return a * half, half + 0.5 * a * (1.0 - inner * inner) * (c * (1.0 + 3.0 * 0.044715 * (a * a)))


def nt_dot(a, b):
    return lax.dot_general(a, b, (((1,), (1,)), ((), ())), preferred_element_type=F32)


def tn_dot(a, b):
    return lax.dot_general(a, b, (((0,), (0,)), ((), ())), preferred_element_type=F32)


H_OFF = (0, 192, 384)
H_UNIT = (3, 3, 2)
H_FIRST = (0, 3, 6)


def column(row):
    return jnp.transpose(jnp.broadcast_to(row, (LANE, LANE)))


def query_kernel(x_ref, win_ref, wout_ref, tgt_ref, blk_ref, cid_ref, logq_ref, tall_ref, h_out, pre_out, cand_out, candt_out, cidb_out, logqb_out,
                 blk, ids, lqs, rows, h_ref, pre_ref, cand_ref, candt_ref, cidb_ref, logqb_ref, load_sem, out_sem, send_sem, recv_sem):
    me = lax.axis_index("dp")
    mine = pl.ds(pl.multiple_of(me * 8, 8), 8)
    loads = [
        pltpu.make_async_copy(cid_ref.at[mine], ids, load_sem.at[0]), pltpu.make_async_copy(logq_ref.at[mine], lqs, load_sem.at[1]),
        pltpu.make_async_copy(blk_ref, blk, load_sem.at[2])]
    for c in loads:
        c.start()
    pl.semaphore_wait(greet(me), NPEER)
    pre = jnp.dot(x_ref[...], win_ref[...], preferred_element_type=F32)
    pre_ref[...] = pre
    act = gelu_parts(pre)[0].astype(BF16)
    query = jnp.dot(act, wout_ref[...], preferred_element_type=F32)
    core = coord(me, "core")
    streams = []
    for s in range(3):
        idx = block_index(me, ORDERS[s])
        for g in range(H_UNIT[s]):
            row = 8 * (H_FIRST[s] + g)
            h_ref[core * 512 + H_OFF[s] + idx * H_UNIT[s] + g] = query[row : row + 8, :].astype(BF16)
        streams.append((h_ref, core * 512 + H_OFF[s], H_UNIT[s], ORDERS[s]))
    tall_ref[core * TOK + block_index(me, ORDERS[2])] = tgt_ref[...]
    streams.append((tall_ref, core * TOK, 1, ORDERS[2]))
    lane = iota((1, LANE), 1)

    def pick(n, carry):
        part = pl.ds(pl.multiple_of(n // 8 * WIDE, WIDE), WIDE)
        first = n % 8 * KILO
        want = cidb_ref[part, :]
        picks = [flag(want == (lane + (first + u * LANE)).astype(F32)).astype(BF16) for u in range(8)]
        rows[part, :] += jnp.dot(jnp.concatenate(picks, axis=1), blk[pl.ds(pl.multiple_of(first, KILO), KILO), :], preferred_element_type=F32)
        return carry

    def fill(phase):
        if phase == 0:
            for c in loads:
                c.wait()
            for c in range(8):
                at = slice(c * LANE, c * LANE + LANE)
                cidb_ref[at, :] = column((ids[c : c + 1, :] - me * ALL).astype(F32))
                logqb_ref[at, :] = column(lqs[c : c + 1, :])
            rows[...] = jnp.zeros_like(rows)
        bounds = (0, 8, 17, 32, 32)
        lax.fori_loop(bounds[phase], bounds[phase + 1], pick, 0)
        if phase == 2:
            cand_ref[...] = rows[...].astype(BF16)
            candt_ref[...] = jnp.transpose(rows[...]).astype(BF16)
            for c in outs:
                c.start()
        if phase == 3:
            half(core).start()

    outs = [
        pltpu.make_async_copy(a, b, out_sem.at[i]) for i, (a, b) in enumerate([
            (pre_ref, pre_out), (cand_ref, cand_out), (candt_ref, candt_out), (cidb_ref, cidb_out), (logqb_ref, logqb_out)])]

    def half(c):
        where = pl.ds(c * 512, 512)
        return pltpu.make_async_copy(h_ref.at[where], h_out.at[where], out_sem.at[5 + c])

    sent = gather_streams(me, streams, [(h_ref, 512), (tall_ref, TOK)], send_sem, recv_sem, fill)
    half(1 - core).start()
    for c in outs:
        c.wait()
    for c in sent:
        c.wait_send()
    half(core).wait()
    half(1 - core).wait()


class Stats:
    def __init__(self, me, recv, cur, send_sem, recv_sem):
        self.me, self.recv, self.cur, self.sems = me, recv, cur, (send_sem, recv_sem)
        self.phase, self.pending, self.sent = [0] * 3, [None] * 3, []

    def send(self, s):
        phase, g0, ng = self.phase[s], H_FIRST[s], H_UNIT[s]
        axis = (ORDERS[s] + ("core",))[phase]
        src = self.cur.at[pl.ds(8 * phase + g0, ng)]
        self.pending[s] = []
        for k in range(1, COORD[axis][1]):
            n = s * NPEER + phase * 3 + k - 1
            dst = self.recv.at[pl.ds(8 * (3 * phase + k - 1) + g0, ng)]
            c = remote(src, dst, self.sems[0].at[n], self.sems[1].at[n], peer(self.me, axis, k))
            c.start()
            self.pending[s].append(c)
        self.sent += self.pending[s]

    def receive(self, s):
        phase, cur, recv, npart = self.phase[s], self.cur, self.recv, len(self.pending[s])
        for c in self.pending[s]:
            c.wait_recv()

        def merge(g, carry):
            old = cur[8 * phase + g]
            parts = [recv[8 * (3 * phase + k) + g] for k in range(npart)]
            top, z = old[0], old[2]
            for p in parts:
                top = jnp.maximum(top, p[0])
                z = jnp.maximum(z, p[2])
            total = old[1] * jnp.exp(old[0] - top)
            for p in parts:
                total = total + p[1] * jnp.exp(p[0] - top)
            row = 8 * (phase + 1) + g
            cur[row, 0] = top
            cur[row, 1] = total
            cur[row, 2] = z
            return carry

        lax.fori_loop(H_FIRST[s], H_FIRST[s] + H_UNIT[s], merge, 0)
        self.phase[s] += 1

    def advance(self, s):
        self.receive(s)
        self.send(s)


def target_kernel(tgt_ref, h_hbm, blk_hbm, zst_ref, pos_ref, code_ref, hc_ref, te_out, h_ref, blk_ref, te_ref, zd, hs, es, codes, load_sem, sem):
    block_rows = blk_ref.shape[0]
    loads = [pltpu.make_async_copy(h_hbm, h_ref, load_sem.at[0]), pltpu.make_async_copy(blk_hbm, blk_ref, load_sem.at[1])]
    for c in loads:
        c.start()
    rel = tgt_ref[...] - lax.axis_index("dp") * block_rows
    own = (rel >= 0) & (rel < block_rows)
    own_f = flag(own)
    own_b = own_f.astype(BF16)
    up = iota((LANE, LANE), 0) < iota((LANE, LANE), 1)
    prefix = jnp.dot(own_b, flag(up).astype(BF16), preferred_element_type=F32)
    total = jnp.dot(own_b, jnp.ones((LANE, LANE), BF16), preferred_element_type=F32)
    low = iota((TOK, TOK), 0) > iota((TOK, TOK), 1)
    offset = jnp.dot(flag(low).astype(BF16), total.astype(BF16), preferred_element_type=F32)
    pos_ref[...] = jnp.where(own, prefix + offset, -1.0)
    zd[...] = jnp.zeros_like(zd)

    def clear(i, carry):
        te_ref[pl.ds(pl.multiple_of(i * LANE, LANE), LANE), :] = jnp.zeros((LANE, LANE), F32)
        return carry

    lax.fori_loop(0, TOK, clear, 0)
    count = jnp.sum(own_f).astype(jnp.int32)
    for c in loads:
        c.wait()
    slot0 = iota((LANE, LANE), 0).astype(F32)
    lane = iota((1, LANE), 1)
    sub = iota((16, LANE), 0)

    def one_row(ref, i):
        tile = ref[pl.ds(pl.multiple_of(i & -16, 16), 16), :].astype(F32)
        return down(jnp.where(sub == (i & 15), tile, 0.0))

    def chunk(c, carry):
        slot = slot0 + (c * LANE).astype(F32)

        def collect(r, code):
            mark = (tgt_ref[one(r), :] % block_rows) * ALL + (lane + r * LANE)
            return code + jnp.where(pos_ref[one(r), :] == slot, mark, 0)

        code = lax.fori_loop(0, TOK, collect, jnp.zeros((LANE, LANE), jnp.int32), unroll=8)
        row = across((code // ALL).astype(F32))
        tok = across((code % ALL).astype(F32))
        both = row.astype(jnp.int32) * ALL + tok.astype(jnp.int32)
        code_ref[one(c), :] = jnp.transpose(jnp.broadcast_to(both, (LANE, LANE)))[0:1, :]
        copy = pltpu.make_async_copy(code_ref.at[one(c)], codes, sem)
        copy.start()
        copy.wait()
        left = count - c * LANE

        def fetch(i, carry2):
            for u in range(8):
                n = i * 8 + u
                v = codes[0, n]
                tok, at = v & (ALL - 1), lax.shift_right_logical(v, 13)
                hs[one(n), :] = one_row(h_ref, tok)
                row = one_row(blk_ref, at)
                es[one(n), :] = row
                te_ref[one(jnp.where(n < left, tok, ALL)), :] = row
            return carry2

        lax.fori_loop(0, (jnp.minimum(left, LANE) + 7) // 8, fetch, 0)
        keep = pltpu.make_async_copy(hs, hc_ref.at[pl.ds(pl.multiple_of(c * LANE, LANE), LANE)], load_sem.at[3])
        keep.start()
        z = jnp.broadcast_to(across(hs[...] * es[...]), (LANE, LANE))

        def spread(r, carry2):
            hit = pos_ref[one(r), :] == slot
            zd[one(r), :] += down(jnp.where(hit, z, 0.0))
            return carry2

        lax.fori_loop(0, TOK, spread, 0, unroll=8)
        keep.wait()
        return carry

    lax.fori_loop(0, (count + 127) // LANE, chunk, 0)
    copy = pltpu.make_async_copy(te_ref.at[pl.ds(0, ALL)], te_out, load_sem.at[2])
    copy.start()
    zst_ref[...] = jnp.where(pos_ref[...] >= 0.0, zd[...], -jnp.inf)
    copy.wait()


def table_kernel(code_ref, g_ref, pos_ref, lossrow_ref, cid_hbm, dcand_hbm, tiles_hbm, hc_ref, de_ref, dwin_ref, dwout_ref, loss_ref, cidx, dcand, whole, hc, gh, sem):
    me = lax.axis_index("dp")
    loads = [pltpu.make_async_copy(cid_hbm.at[pl.ds(pl.multiple_of(me * 8, 8), 8)], cidx, sem.at[3]), pltpu.make_async_copy(dcand_hbm, dcand, sem.at[0]), pltpu.make_async_copy(tiles_hbm, whole, sem.at[1])]
    for c in loads:
        c.start()
    loss_ref[0, 0] = jnp.max(lossrow_ref[...])

    def clear(i, carry):
        de_ref[pl.ds(pl.multiple_of(i * LANE, LANE), LANE), :] = jnp.zeros((LANE, LANE), F32)
        return carry

    lax.fori_loop(0, de_ref.shape[0] // LANE, clear, 0)
    for c in loads:
        c.wait()

    base = me * ALL

    def place(i, carry):
        for u in range(32):
            de_ref[one(cidx[lax.shift_right_logical(i, 2), (i & 3) * 32 + u] - base), :] = dcand[one(i * 32 + u), :]
        return carry

    lax.fori_loop(0, 32, place, 0)
    count = jnp.sum(flag(pos_ref[...] >= 0.0)).astype(jnp.int32)
    slot0 = iota((LANE, LANE), 0).astype(F32)

    def chunk(c, carry):
        slot = slot0 + (c * LANE).astype(F32)
        copy = pltpu.make_async_copy(hc_ref.at[pl.ds(pl.multiple_of(c * LANE, LANE), LANE)], hc, sem.at[2])
        copy.start()

        def collect(r, acc):
            return acc + jnp.where(pos_ref[one(r), :] == slot, g_ref[one(r), :], 0.0)

        g = jnp.sum(lax.fori_loop(0, TOK, collect, jnp.zeros((LANE, LANE), F32), unroll=8), axis=1, keepdims=True)
        copy.wait()
        gh[...] = g * hc[...]

        def put(i, carry2):
            de_ref[one(lax.shift_right_logical(code_ref[c, i], 13)), :] += gh[one(i), :]
            return carry2

        lax.fori_loop(0, jnp.minimum(count - c * LANE, LANE), put, 0)
        return carry

    lax.fori_loop(0, (count + 127) // LANE, chunk, 0)
    dwout_ref[...] = whole[0:LANE].reshape(KILO, LANE)
    for j in range(8):
        dwin_ref[:, LANE * j : LANE * j + LANE] = whole[LANE + 32 * j : 160 + 32 * j].reshape(WIDE, LANE)


LAST = 27
PART = 512


def core_exchange(me, ref, half, rref, send, recv):
    mine = coord(me, "core")
    c = remote(ref.at[pl.ds((1 - mine) * half, half)], rref.at[pl.ds(0, half)], send, recv, peer(me, "core", 1))
    c.start()
    c.wait_recv()
    add_rows(ref, mine * half, rref, 0, half, 1)
    return [c]


def grad_kernel(tgt_ref, zst_ref, h_hbm, cand_hbm, cidb_hbm, logqb_hbm, candt_hbm, te_hbm, x_hbm, wout_hbm, pre_hbm, g_ref, loss_ref, tiles_out, dcand_out,
                ebuf, mc_ref, part, local, total, srecv, cur, norm, acc, recv, tiles, trecv, whole, dcand_ref,
                h_ref, cand_ref, cidb, logqb, candt_ref, te_ref, x_ref, wout_ref, pre_ref,
                load_sem, core_send, core_recv, send_sem, recv_sem):
    me = lax.axis_index("dp")
    core = coord(me, "core")
    loads = [
        pltpu.make_async_copy(a, b, load_sem.at[i]) for i, (a, b) in enumerate([
            (cand_hbm, cand_ref), (cidb_hbm, cidb), (logqb_hbm, logqb), (h_hbm, h_ref),
            (candt_hbm, candt_ref), (te_hbm, te_ref), (x_hbm, x_ref), (wout_hbm, wout_ref), (pre_hbm, pre_ref)])]
    for c in loads:
        c.start()
    barrier = greet(me)
    local[...] = (tgt_ref[...] - me * ALL).astype(F32)
    for g in range(8):
        for half in range(2):
            cur[g, 2, 4 * half : 4 * half + 4, :] = zst_ref[32 * half + 4 * g : 32 * half + 4 * g + 4, :]
    for c in loads[:4]:
        c.wait()

    def score(t, carry):
        for j in range(2):
            dots = nt_dot(cand_ref[...], h_ref[pl.ds(pl.multiple_of(t * PART + WIDE * j, WIDE), WIDE), :])
            for half in range(2):
                q = 2 * j + half
                r = t * 4 + q
                tgt = local[one(r), :]
                for c in range(8):
                    rows = slice(LANE * c, LANE * c + LANE)
                    s = dots[rows, LANE * half : LANE * half + LANE] - logqb[rows, :]
                    s = jnp.where(cidb[rows, :] == tgt, -1e9, s)
                    m = peak(s)
                    e = jnp.exp(s - m)
                    ebuf[t, rows, LANE * q : LANE * q + LANE] = e
                    mc_ref[r, c : c + 1, :] = m
                    part[q, c : c + 1, :] = down(e)
                most = mc_ref[r]
                top = peak(most)
                row = one(t // 8 * 4 + q)
                cur[t % 8, 0, row, :] = top
                cur[t % 8, 1, row, :] = down(part[q] * jnp.exp(most - top))
        return carry

    def part_loop(s, base, body):
        lax.fori_loop(base + H_FIRST[s], base + H_FIRST[s] + H_UNIT[s], body, 0)

    def score_part(s):
        part_loop(s, 0, score)
        part_loop(s, 8, score)

    def finish(s):
        stats.receive(s)

        def norms(g, carry):
            m, t, z = cur[32 + g, 0], cur[32 + g, 1], cur[32 + g, 2]
            top = jnp.maximum(m, z)
            log_norm = top + jnp.log(t * jnp.exp(m - top) + jnp.exp(z - top))
            grad = (jnp.exp(z - log_norm) - 1.0) / ALL
            total[...] += log_norm - z
            for half in range(2):
                rows = pl.ds(32 * half + 4 * g, 4)
                norm[rows, :] = log_norm[4 * half : 4 * half + 4, :]
                g_ref[rows, :] = grad[4 * half : 4 * half + 4, :]
            return carry

        part_loop(s, 0, norms)

    total[...] = jnp.zeros_like(total)

    def probs(t):
        blocks = []
        for q in range(4):
            r = t * 4 + q
            scale = jnp.exp(mc_ref[r] - norm[one(r), :]) / ALL
            blocks.append(jnp.concatenate([
                (ebuf[t, LANE * c : LANE * c + LANE, LANE * q : LANE * q + LANE] * scale[c : c + 1, :]).astype(BF16) for c in range(8)], axis=0))
        return jnp.concatenate(blocks, axis=1)

    def query_grad(t):
        dqt = jnp.dot(candt_ref[...], probs(t), preferred_element_type=F32)
        gcol = jnp.concatenate([column(g_ref[one(t * 4 + q), :]) for q in range(4)], axis=0)
        dq = jnp.transpose(dqt) + gcol * te_ref[pl.ds(pl.multiple_of(t * PART, PART), PART), :]
        return dq.reshape(TOK, 8, LANE)

    def swap(i):
        return remote(acc.at[pl.ds(((1 - core) * 8 + i) * TOK, TOK)], recv.at[pl.ds(i * TOK, TOK)], core_send.at[i], core_recv.at[i], peer(me, "core", 1))

    def give(i, carry):
        t = (1 - core) * 8 + i
        acc[pl.ds(t * TOK, TOK)] = query_grad(t)
        swap(i).start()
        return carry

    def keep(i, carry):
        t = core * 8 + i
        val = query_grad(t)
        swap(i).wait_recv()
        acc[pl.ds(t * TOK, TOK)] = val + recv[pl.ds(i * TOK, TOK)]
        return carry

    def cand_grad():
        dcand_ref[...] = jnp.zeros_like(dcand_ref)

        def accumulate(t, carry):
            dcand_ref[...] += jnp.dot(probs(t), h_ref[pl.ds(pl.multiple_of(t * PART, PART), PART), :], preferred_element_type=F32)
            return carry

        lax.fori_loop(0, 16, accumulate, 0)
        dcand_copy.start()

    dcand_copy = pltpu.make_async_copy(dcand_ref, dcand_out, load_sem.at[9])
    streams = [(H_OFF[s], H_UNIT[s], ORDERS[s]) for s in range(3)]
    scatter = Scatter(me, acc, core * 512, recv, 512, streams, send_sem.at[0], recv_sem.at[0])
    stats = Stats(me, srecv, cur, send_sem.at[3], recv_sem.at[3])
    a, b, c = range(3)

    def keep_part(s):
        part_loop(s, 0, keep)
        scatter.send(s)

    score_part(a)
    pl.semaphore_wait(barrier, NPEER)
    stats.send(a)
    score_part(b)
    stats.advance(a)
    stats.send(b)
    score_part(c)
    stats.advance(a)
    stats.advance(b)
    stats.send(c)
    for s in (a, b, c):
        stats.advance(s)
    finish(a)
    for load in loads[4:]:
        load.wait()
    part_loop(a, 0, give)
    stats.advance(b)
    stats.advance(c)
    keep_part(a)
    finish(b)
    part_loop(b, 0, give)
    stats.advance(c)
    keep_part(b)
    finish(c)
    part_loop(c, 0, give)
    keep_part(c)
    loss_ref[...] = jnp.broadcast_to(jnp.sum(total[...], keepdims=True) / ALL, loss_ref.shape)
    cand_grad()
    scatter.rest()
    sent = stats.sent + scatter.sent
    rows = []
    for s in range(3):
        idx = block_index(me, ORDERS[s])
        for g in range(H_UNIT[s]):
            rows.append(acc[core * 512 + H_OFF[s] + idx * H_UNIT[s] + g])
    dh = jnp.concatenate(rows, axis=0).astype(BF16)
    act, slope = gelu_parts(pre_ref[...])
    d_pre = (slope * nt_dot(dh, wout_ref[...])).astype(BF16)
    dw_out = tn_dot(act.astype(BF16), dh)
    tiles[0:LANE] = dw_out.reshape(LANE, 8, LANE)
    dw_in = tn_dot(x_ref[...], d_pre)
    for j in range(8):
        tiles[LANE + 32 * j : 160 + 32 * j] = dw_in[:, LANE * j : LANE * j + LANE].reshape(32, 8, LANE)
    streams = [(TOK * s, 1, ORDERS[s]) for s in range(3)]
    half = core_exchange(me, tiles, 192, trecv, send_sem.at[1, LAST], recv_sem.at[1, LAST])
    scatter = Scatter(me, tiles, core * 192, trecv, 192, streams, send_sem.at[1], recv_sem.at[1])
    for s in range(3):
        scatter.send(s)
    scatter.rest()
    sent += half + scatter.sent
    streams = []
    for s in range(3):
        own = core * 192 + TOK * s + block_index(me, ORDERS[s])
        whole[own] = tiles[own]
        streams.append((whole, core * 192 + TOK * s, 1, ORDERS[s]))
    sent += gather_streams(me, streams, [(whole, 192)], send_sem.at[2], recv_sem.at[2])
    tiles_copy = pltpu.make_async_copy(whole, tiles_out, load_sem.at[10])
    tiles_copy.start()
    dcand_copy.wait()
    for c in sent:
        c.wait_send()

    def swap_done(i, carry):
        swap(i).wait_send()
        return carry

    lax.fori_loop(0, 8, swap_done, 0)
    tiles_copy.wait()


def vmem(n):
    return [pl.BlockSpec(memory_space=pltpu.VMEM)] * n


def params(cid):
    return pltpu.CompilerParams(collective_id=cid, has_side_effects=True, vmem_limit_bytes=63 * KILO * KILO)


def dma(*shape):
    return pltpu.SemaphoreType.DMA(shape)


def solution(mesh):
    num_dev = mesh.shape["dp"]

    def local_step(features, w_in, w_out, table_blk, cand_ids, log_q, targets):
        dev_index = lax.axis_index("dp")
        block_rows = table_blk.shape[0]
        cand_dev = cand_ids.shape[0] // num_dev
        tok_total = features.shape[0] * num_dev
        anyspec = pl.BlockSpec(memory_space=pl.ANY)
        cid_rows, logq_rows = cand_ids.reshape(KILO, LANE), log_q.reshape(KILO, LANE)
        tall, h_all, pre, cand_rows, cand_t, cidb, logqb = pl.pallas_call(
            query_kernel,
            out_shape=[
                jax.ShapeDtypeStruct((LANE, 1, TOK), jnp.int32), jax.ShapeDtypeStruct((KILO, 8, LANE), BF16), jax.ShapeDtypeStruct((TOK, KILO), F32),
                jax.ShapeDtypeStruct((cand_dev, LANE), BF16), jax.ShapeDtypeStruct((LANE, cand_dev), BF16),
                jax.ShapeDtypeStruct((cand_dev, LANE), F32), jax.ShapeDtypeStruct((cand_dev, LANE), F32)],
            in_specs=vmem(4) + [anyspec] * 3, out_specs=vmem(1) + [anyspec] * 6,
            scratch_shapes=[
                pltpu.VMEM((block_rows, LANE), BF16), pltpu.VMEM((8, LANE), jnp.int32), pltpu.VMEM((8, LANE), F32), pltpu.VMEM((cand_dev, LANE), F32),
                pltpu.VMEM((KILO, 8, LANE), BF16), pltpu.VMEM((TOK, KILO), F32), pltpu.VMEM((cand_dev, LANE), BF16), pltpu.VMEM((LANE, cand_dev), BF16),
                pltpu.VMEM((cand_dev, LANE), F32), pltpu.VMEM((cand_dev, LANE), F32),
                dma(3), dma(7), dma(4 * NPEER), dma(4 * NPEER)],
            compiler_params=params(0), name="query_gather",
        )(features, w_in, w_out, targets[None, :], table_blk, cid_rows, logq_rows)
        query_all = h_all.reshape(ALL, LANE)
        t5 = tall.reshape(2, 4, 4, 4, TOK)
        tgt_all = jnp.concatenate([
            t5.transpose(0, 3, 1, 2, 4)[..., 0:24].reshape(2, -1),
            t5.transpose(0, 2, 3, 1, 4)[..., 24:48].reshape(2, -1),
            t5[..., 48:TOK].reshape(2, -1)], axis=1).reshape(TOK, LANE)
        smem = pl.BlockSpec(memory_space=pltpu.SMEM)
        square = pltpu.VMEM((LANE, LANE), F32)
        big = pltpu.CompilerParams(vmem_limit_bytes=63 * KILO * KILO)
        zst, pos, codes, hc, te = pl.pallas_call(
            target_kernel,
            out_shape=[
                jax.ShapeDtypeStruct((TOK, LANE), F32), jax.ShapeDtypeStruct((TOK, LANE), F32), jax.ShapeDtypeStruct((TOK, LANE), jnp.int32),
                jax.ShapeDtypeStruct((tok_total, LANE), F32), jax.ShapeDtypeStruct((tok_total, LANE), F32)],
            in_specs=vmem(1) + [anyspec] * 2, out_specs=vmem(3) + [anyspec] * 2,
            scratch_shapes=[
                pltpu.VMEM((tok_total, LANE), BF16), pltpu.VMEM((block_rows, LANE), BF16), pltpu.VMEM((tok_total + 8, LANE), F32), pltpu.VMEM((TOK, LANE), F32),
                square, square, pltpu.SMEM((1, LANE), jnp.int32), dma(4), pltpu.SemaphoreType.DMA],
            compiler_params=big, name="target_rows",
        )(tgt_all, query_all, table_blk)
        grad_tgt, loss_row, tiles, dcand = pl.pallas_call(
            grad_kernel,
            out_shape=[
                jax.ShapeDtypeStruct((TOK, LANE), F32), jax.ShapeDtypeStruct((8, LANE), F32),
                jax.ShapeDtypeStruct((384, 8, LANE), F32), jax.ShapeDtypeStruct((cand_dev, LANE), F32)],
            in_specs=vmem(2) + [anyspec] * 9, out_specs=vmem(2) + [anyspec] * 2,
            scratch_shapes=[
                pltpu.VMEM((16, cand_dev, PART), F32), pltpu.VMEM((TOK, 8, LANE), F32), pltpu.VMEM((4, 8, LANE), F32), pltpu.VMEM((TOK, LANE), F32), pltpu.VMEM((8, LANE), F32),
                pltpu.VMEM((80, 3, 8, LANE), F32), pltpu.VMEM((40, 3, 8, LANE), F32), pltpu.VMEM((TOK, LANE), F32),
                pltpu.VMEM((KILO, 8, LANE), F32), pltpu.VMEM((KILO, 8, LANE), F32),
                pltpu.VMEM((384, 8, LANE), F32), pltpu.VMEM((384, 8, LANE), F32), pltpu.VMEM((384, 8, LANE), F32), pltpu.VMEM((cand_dev, LANE), F32),
                pltpu.VMEM((tok_total, LANE), BF16), pltpu.VMEM((cand_dev, LANE), BF16), pltpu.VMEM((cand_dev, LANE), F32), pltpu.VMEM((cand_dev, LANE), F32),
                pltpu.VMEM((LANE, cand_dev), BF16), pltpu.VMEM((tok_total, LANE), F32),
                pltpu.VMEM(features.shape, BF16), pltpu.VMEM(w_out.shape, BF16), pltpu.VMEM(pre.shape, F32),
                dma(11), dma(8), dma(8), dma(4, 3 * NPEER), dma(4, 3 * NPEER)],
            compiler_params=params(1), name="grad_reduce",
        )(tgt_all, zst, query_all, cand_rows, cidb, logqb, cand_t, te, features, w_out, pre)
        grad_blk, grad_w_in, grad_w_out, loss = pl.pallas_call(
            table_kernel,
            out_shape=[
                jax.ShapeDtypeStruct((block_rows, LANE), F32), jax.ShapeDtypeStruct(w_in.shape, F32), jax.ShapeDtypeStruct(w_out.shape, F32),
                jax.ShapeDtypeStruct((1, 1), F32)],
            in_specs=[smem] + vmem(3) + [anyspec] * 4, out_specs=vmem(3) + [smem],
            scratch_shapes=[pltpu.SMEM((8, LANE), jnp.int32), pltpu.VMEM((cand_dev, LANE), F32), pltpu.VMEM((384, 8, LANE), F32), square, square, dma(4)],
            compiler_params=big, name="table_grad",
        )(codes, grad_tgt, pos, loss_row, cid_rows, dcand, tiles, hc)
        loss = loss.reshape(())
        return loss, grad_blk, grad_w_in, grad_w_out

    return jax.shard_map(local_step, mesh=mesh, in_specs=(P("dp", None), P(), P(), P("dp", None), P(), P(), P("dp")), out_specs=(P(), P("dp", None), P(), P()), check_vma=False)
```

```python
import functools
import jax
import jax.numpy as jnp
from jax import lax
from jax.experimental import pallas as pl
from jax.experimental.pallas import tpu as pltpu
from jax.sharding import PartitionSpec as P

MESH = pl.DeviceIdType.MESH
F32, BF16 = jnp.float32, jnp.bfloat16
COORD = {"core": (1, 2), "x": (2, 4), "y": (8, 4), "z": (32, 4)}
ORDERS = (("x", "y", "z"), ("y", "z", "x"), ("z", "x", "y"))
NDEV = 128
NPEER = 10
LANE, TOK, ALL, KILO, WIDE = 128, 64, 8192, 1024, 256


def one(i):
    return pl.ds(i, 1)


def repeat(n, body, unroll=1):
    lax.fori_loop(0, n, body, 0, unroll=unroll)


def down(v):
    return jnp.sum(v, axis=0, keepdims=True)


def across(v):
    return jnp.sum(v, axis=1, keepdims=True)


def peak(v):
    return jnp.max(v, axis=0, keepdims=True)


def flag(mask):
    return jnp.where(mask, 1.0, 0.0)


def iota(shape, dim):
    return lax.broadcasted_iota(jnp.int32, shape, dim)


def coord(me, axis):
    stride, radix = COORD[axis]
    return (me // stride) % radix


def peer(me, axis, k):
    stride, radix = COORD[axis]
    c = coord(me, axis)
    return me + ((c + k) % radix - c) * stride


def block_index(me, order):
    idx, weight = 0, 1
    for axis in order:
        idx = idx + coord(me, axis) * weight
        weight *= COORD[axis][1]
    return idx


def greet(me):
    barrier = pltpu.get_barrier_semaphore()
    for axis in COORD:
        for k in range(1, COORD[axis][1]):
            pl.semaphore_signal(barrier, inc=1, device_id=(peer(me, axis, k),), device_id_type=MESH)
    return barrier


def remote(src, dst, send, recv, dev):
    return pltpu.make_async_remote_copy(src_ref=src, dst_ref=dst, send_sem=send, recv_sem=recv, device_id=(dev,), device_id_type=MESH)


def gather_streams(me, streams, bulk, send_sem, recv_sem, between=None):
    pending, sent = [None] * len(streams), []
    for phase in range(4):
        for s, (ref, off, unit, order) in enumerate(streams):
            if pending[s]:
                for c in pending[s]:
                    c.wait_recv()
            if phase == 3:
                continue
            span = 4 ** phase
            idx = block_index(me, order)
            where = ref.at[pl.ds(off + (idx - idx % span) * unit, span * unit)]
            pending[s] = []
            for k in range(1, 4):
                n = s * 9 + phase * 3 + k - 1
                c = remote(where, where, send_sem.at[n], recv_sem.at[n], peer(me, order[phase], k))
                c.start()
                pending[s].append(c)
                sent.append(c)
        if between and phase < 3:
            between(phase)
    last = []
    for i, (ref, count) in enumerate(bulk):
        n = len(streams) * 9 + i
        where = ref.at[pl.ds(coord(me, "core") * count, count)]
        c = remote(where, where, send_sem.at[n], recv_sem.at[n], peer(me, "core", 1))
        c.start()
        last.append(c)
    if between:
        between(3)
    for c in last:
        c.wait_recv()
    return sent + last


def add_rows(ref, start, rref, base, count, parts):
    def add(i, carry):
        acc = ref[start + i]
        for k in range(parts):
            acc = acc + rref[base + k * count + i]
        ref[start + i] = acc
        return carry

    lax.fori_loop(0, count, add, 0, unroll=4)


class Scatter:
    def __init__(self, me, ref, first, rref, rbase, streams, send_sem, recv_sem):
        self.me, self.ref, self.first, self.rref, self.rbase = me, ref, first, rref, rbase
        self.streams, self.sems = streams, (send_sem, recv_sem)
        self.step, self.pending, self.sent = [0] * 3, [None] * 3, []

    def send(self, s):
        off, unit, order = self.streams[s]
        step, me = self.step[s], self.me
        span = 4 ** (2 - step)
        axis = order[2 - step]
        idx = block_index(me, order)
        start = self.first + off + (idx - idx % (4 * span)) * unit
        d = coord(me, axis)
        copies = []
        for k in range(1, 4):
            n = s * 9 + step * 3 + k - 1
            src = self.ref.at[pl.ds(start + (d + k) % 4 * span * unit, span * unit)]
            dst = self.rref.at[pl.ds(self.rbase + (k - 1) * span * unit, span * unit)]
            c = remote(src, dst, self.sems[0].at[n], self.sems[1].at[n], peer(me, axis, k))
            c.start()
            copies.append(c)
        self.sent += copies
        self.pending[s] = (copies, start + d * span * unit, self.rbase, span * unit)
        self.rbase += 3 * span * unit
        self.step[s] += 1

    def receive(self, s):
        copies, start, base, count = self.pending[s]
        for c in copies:
            c.wait_recv()
        add_rows(self.ref, start, self.rref, base, count, 3)

    def rest(self):
        for step in range(3):
            for s in range(3):
                self.receive(s)
                if step < 2:
                    self.send(s)


def gelu_parts(a):
    c = 0.7978845608028654
    inner = jnp.tanh(c * (a + 0.044715 * (a * a * a)))
    half = 0.5 * (1.0 + inner)
    return a * half, half + 0.5 * a * (1.0 - inner * inner) * (c * (1.0 + 3.0 * 0.044715 * (a * a)))


def nt_dot(a, b):
    return lax.dot_general(a, b, (((1,), (1,)), ((), ())), preferred_element_type=F32)


def tn_dot(a, b):
    return lax.dot_general(a, b, (((0,), (0,)), ((), ())), preferred_element_type=F32)


H_OFF = (0, 192, 384)
H_UNIT = (3, 3, 2)
H_FIRST = (0, 3, 6)


def column(row):
    return jnp.transpose(jnp.broadcast_to(row, (LANE, LANE)))


def query_kernel(x_ref, win_ref, wout_ref, tgt_ref, blk_ref, cid_ref, logq_ref, tall_ref, h_out, pre_out, cand_out, candt_out, cidb_out, logqb_out,
                 blk, ids, lqs, rows, h_ref, pre_ref, cand_ref, candt_ref, cidb_ref, logqb_ref, load_sem, out_sem, send_sem, recv_sem):
    me = lax.axis_index("dp")
    mine = pl.ds(pl.multiple_of(me * 8, 8), 8)
    loads = [
        pltpu.make_async_copy(cid_ref.at[mine], ids, load_sem.at[0]), pltpu.make_async_copy(logq_ref.at[mine], lqs, load_sem.at[1]),
        pltpu.make_async_copy(blk_ref, blk, load_sem.at[2])]
    for c in loads:
        c.start()
    barrier = greet(me)
    pre = jnp.dot(x_ref[...], win_ref[...], preferred_element_type=F32)
    pre_ref[...] = pre
    act = gelu_parts(pre)[0].astype(BF16)
    query = jnp.dot(act, wout_ref[...], preferred_element_type=F32)
    core = coord(me, "core")
    streams = []
    for s in range(3):
        idx = block_index(me, ORDERS[s])
        for g in range(H_UNIT[s]):
            row = 8 * (H_FIRST[s] + g)
            h_ref[core * 512 + H_OFF[s] + idx * H_UNIT[s] + g] = query[row : row + 8, :].astype(BF16)
        streams.append((h_ref, core * 512 + H_OFF[s], H_UNIT[s], ORDERS[s]))
    tall_ref[core * TOK + block_index(me, ORDERS[2])] = tgt_ref[...]
    streams.append((tall_ref, core * TOK, 1, ORDERS[2]))
    lane = iota((1, LANE), 1)
    pl.semaphore_wait(barrier, NPEER)

    def pick(n, carry):
        part = pl.ds(pl.multiple_of(n // 8 * WIDE, WIDE), WIDE)
        first = n % 8 * KILO
        want = cidb_ref[part, :]
        picks = [flag(want == (lane + (first + u * LANE)).astype(F32)).astype(BF16) for u in range(8)]
        rows[part, :] += jnp.dot(jnp.concatenate(picks, axis=1), blk[pl.ds(pl.multiple_of(first, KILO), KILO), :], preferred_element_type=F32)
        return carry

    def fill(phase):
        if phase == 0:
            for c in loads:
                c.wait()
            for c in range(8):
                at = slice(c * LANE, c * LANE + LANE)
                cidb_ref[at, :] = column((ids[c : c + 1, :] - me * ALL).astype(F32))
                logqb_ref[at, :] = column(lqs[c : c + 1, :])
            rows[...] = jnp.zeros_like(rows)
        bounds = (0, 8, 17, 32, 32)
        lax.fori_loop(bounds[phase], bounds[phase + 1], pick, 0)
        if phase == 2:
            cand_ref[...] = rows[...].astype(BF16)
            candt_ref[...] = jnp.transpose(rows[...]).astype(BF16)
            for c in outs:
                c.start()
        if phase == 3:
            half(core).start()

    outs = [
        pltpu.make_async_copy(a, b, out_sem.at[i]) for i, (a, b) in enumerate([
            (pre_ref, pre_out), (cand_ref, cand_out), (candt_ref, candt_out), (cidb_ref, cidb_out), (logqb_ref, logqb_out)])]

    def half(c):
        where = pl.ds(c * 512, 512)
        return pltpu.make_async_copy(h_ref.at[where], h_out.at[where], out_sem.at[5 + c])

    sent = gather_streams(me, streams, [(h_ref, 512), (tall_ref, TOK)], send_sem, recv_sem, fill)
    half(1 - core).start()
    for c in outs:
        c.wait()
    for c in sent:
        c.wait_send()
    half(core).wait()
    half(1 - core).wait()


class Stats:
    def __init__(self, me, recv, cur, send_sem, recv_sem):
        self.me, self.recv, self.cur, self.sems = me, recv, cur, (send_sem, recv_sem)
        self.phase, self.pending, self.sent = [0] * 3, [None] * 3, []

    def send(self, s):
        phase, g0, ng = self.phase[s], H_FIRST[s], H_UNIT[s]
        axis = (ORDERS[s] + ("core",))[phase]
        src = self.cur.at[pl.ds(8 * phase + g0, ng)]
        self.pending[s] = []
        for k in range(1, COORD[axis][1]):
            n = s * NPEER + phase * 3 + k - 1
            dst = self.recv.at[pl.ds(8 * (3 * phase + k - 1) + g0, ng)]
            c = remote(src, dst, self.sems[0].at[n], self.sems[1].at[n], peer(self.me, axis, k))
            c.start()
            self.pending[s].append(c)
        self.sent += self.pending[s]

    def receive(self, s):
        phase, cur, recv, npart = self.phase[s], self.cur, self.recv, len(self.pending[s])
        for c in self.pending[s]:
            c.wait_recv()

        def merge(g, carry):
            old = cur[8 * phase + g]
            parts = [recv[8 * (3 * phase + k) + g] for k in range(npart)]
            top, z = old[0], old[2]
            for p in parts:
                top = jnp.maximum(top, p[0])
                z = jnp.maximum(z, p[2])
            total = old[1] * jnp.exp(old[0] - top)
            for p in parts:
                total = total + p[1] * jnp.exp(p[0] - top)
            row = 8 * (phase + 1) + g
            cur[row, 0] = top
            cur[row, 1] = total
            cur[row, 2] = z
            return carry

        lax.fori_loop(H_FIRST[s], H_FIRST[s] + H_UNIT[s], merge, 0)
        self.phase[s] += 1

    def advance(self, s):
        self.receive(s)
        self.send(s)


def arrange(tall_ref, square, tok_ref):
    def row(b, carry):
        square[one(b), :] = tall_ref[b]
        return carry

    repeat(LANE, row)
    ids = square[...]
    pieces = jnp.concatenate([lax.shift_right_logical(ids, 14), lax.shift_right_logical(ids, 7) & 127, ids & 127], axis=0).astype(F32).astype(BF16)
    b = iota((LANE, 1), 0)
    bt = iota((1, LANE), 1)

    def place(v, s):
        c = [lax.shift_right_logical(v, n) & 3 for n in (0, 2, 4)]
        z, x, y = c
        first, second, third = ((x, y, z), (y, z, x), (z, x, y))[s]
        return (v & TOK) + first + 4 * second + 16 * third

    for s in range(3):
        width, per = 8 * H_UNIT[s], (16, 16, 8)[s]
        span = width * per
        pick = iota((TOK, span), 0) == iota((TOK, span), 1) % width + 8 * H_FIRST[s]
        lanes = jnp.dot(pieces, flag(pick).astype(BF16), preferred_element_type=F32)
        mask = place(b, s) % per == iota((LANE, span), 1) // width
        group = flag(place(bt, s) // per == iota((LANE // per, LANE), 0)).astype(BF16)
        got = [
            jnp.dot(group, jnp.where(mask, lanes[LANE * p : LANE * p + LANE, :], 0.0).astype(BF16), preferred_element_type=F32).astype(jnp.int32)
            for p in range(3)]
        full = (got[0] * LANE + got[1]) * LANE + got[2]
        rows = span // LANE
        for a in range(LANE // per):
            half, rest = divmod(a, TOK // per)
            for r in range(rows):
                at = 32 * half + H_OFF[s] // 16 + rest * rows + r
                tok_ref[at : at + 1, :] = full[a : a + 1, LANE * r : LANE * r + LANE]


def target_kernel(tall_ref, h_hbm, blk_hbm, zst_ref, pos_ref, code_ref, local_ref, hc_ref, te_out, h_ref, blk_ref, te_ref, zd, hs, es, square, tgt_ref, codes, load_sem, sem):
    block_rows = blk_ref.shape[0]
    loads = [pltpu.make_async_copy(h_hbm, h_ref, load_sem.at[0]), pltpu.make_async_copy(blk_hbm, blk_ref, load_sem.at[1])]
    for c in loads:
        c.start()
    arrange(tall_ref, square, tgt_ref)
    rel = tgt_ref[...] - lax.axis_index("dp") * block_rows
    local_ref[...] = rel.astype(F32)
    own = (rel >= 0) & (rel < block_rows)
    own_f = flag(own)
    own_b = own_f.astype(BF16)
    up = iota((LANE, LANE), 0) < iota((LANE, LANE), 1)
    prefix = jnp.dot(own_b, flag(up).astype(BF16), preferred_element_type=F32)
    total = jnp.dot(own_b, jnp.ones((LANE, LANE), BF16), preferred_element_type=F32)
    low = iota((TOK, TOK), 0) > iota((TOK, TOK), 1)
    offset = jnp.dot(flag(low).astype(BF16), total.astype(BF16), preferred_element_type=F32)
    pos_ref[...] = jnp.where(own, prefix + offset, -1.0)
    zd[...] = jnp.zeros_like(zd)

    def clear(i, carry):
        te_ref[pl.ds(pl.multiple_of(i * LANE, LANE), LANE), :] = jnp.zeros((LANE, LANE), F32)
        return carry

    repeat(TOK, clear)
    count = jnp.sum(own_f).astype(jnp.int32)
    slot0 = iota((LANE, LANE), 0).astype(F32)
    lane = iota((1, LANE), 1)
    sub = iota((16, LANE), 0)

    def one_row(ref, i):
        tile = ref[pl.ds(pl.multiple_of(i & -16, 16), 16), :].astype(F32)
        return down(jnp.where(sub == (i & 15), tile, 0.0))

    def compact(c, carry):
        slot = slot0 + (c * LANE).astype(F32)

        def collect(r, code):
            mark = (tgt_ref[one(r), :] % block_rows) * ALL + (lane + r * LANE)
            return code + jnp.where(pos_ref[one(r), :] == slot, mark, 0)

        code = lax.fori_loop(0, TOK, collect, jnp.zeros((LANE, LANE), jnp.int32), unroll=8)
        row = across((code // ALL).astype(F32))
        tok = across((code % ALL).astype(F32))
        both = row.astype(jnp.int32) * ALL + tok.astype(jnp.int32)
        code_ref[one(c), :] = jnp.transpose(jnp.broadcast_to(both, (LANE, LANE)))[0:1, :]
        return carry

    chunks = (count + 127) // LANE
    repeat(chunks, compact)
    copy = pltpu.make_async_copy(code_ref, codes, sem)
    copy.start()
    for c in loads:
        c.wait()
    copy.wait()

    def chunk(c, carry):
        slot = slot0 + (c * LANE).astype(F32)
        left = count - c * LANE

        def fetch(i, carry2):
            for u in range(8):
                n = i * 8 + u
                v = codes[c, n]
                tok, at = v & (ALL - 1), lax.shift_right_logical(v, 13)
                hs[one(n), :] = one_row(h_ref, tok)
                row = one_row(blk_ref, at)
                es[one(n), :] = row
                te_ref[one(jnp.where(n < left, tok, ALL)), :] = row
            return carry2

        repeat((jnp.minimum(left, LANE) + 7) // 8, fetch)
        keep = pltpu.make_async_copy(hs, hc_ref.at[pl.ds(pl.multiple_of(c * LANE, LANE), LANE)], load_sem.at[3])
        keep.start()
        z = jnp.broadcast_to(across(hs[...] * es[...]), (LANE, LANE))

        def spread(r, carry2):
            hit = pos_ref[one(r), :] == slot
            zd[one(r), :] += down(jnp.where(hit, z, 0.0))
            return carry2

        repeat(TOK, spread, 8)
        keep.wait()
        return carry

    repeat(chunks, chunk)
    copy = pltpu.make_async_copy(te_ref.at[pl.ds(0, ALL)], te_out, load_sem.at[2])
    copy.start()
    zst_ref[...] = jnp.where(pos_ref[...] >= 0.0, zd[...], -jnp.inf)
    copy.wait()


def table_kernel(code_ref, g_ref, pos_ref, lossrow_ref, cid_hbm, dcand_hbm, tiles_hbm, hc_ref, de_ref, dwin_ref, dwout_ref, loss_ref, cidx, dcand, whole, hc, gh, sem):
    me = lax.axis_index("dp")
    loads = [pltpu.make_async_copy(cid_hbm.at[pl.ds(pl.multiple_of(me * 8, 8), 8)], cidx, sem.at[3]), pltpu.make_async_copy(dcand_hbm, dcand, sem.at[0]), pltpu.make_async_copy(tiles_hbm, whole, sem.at[1])]
    for c in loads:
        c.start()
    loss_ref[0, 0] = jnp.max(lossrow_ref[...])

    def clear(i, carry):
        de_ref[pl.ds(pl.multiple_of(i * LANE, LANE), LANE), :] = jnp.zeros((LANE, LANE), F32)
        return carry

    repeat(de_ref.shape[0] // LANE, clear)
    for c in loads:
        c.wait()

    base = me * ALL

    def place(i, carry):
        for u in range(32):
            de_ref[one(cidx[lax.shift_right_logical(i, 2), (i & 3) * 32 + u] - base), :] = dcand[one(i * 32 + u), :]
        return carry

    repeat(32, place)
    count = jnp.sum(flag(pos_ref[...] >= 0.0)).astype(jnp.int32)
    slot0 = iota((LANE, LANE), 0).astype(F32)

    def chunk(c, carry):
        slot = slot0 + (c * LANE).astype(F32)
        copy = pltpu.make_async_copy(hc_ref.at[pl.ds(pl.multiple_of(c * LANE, LANE), LANE)], hc, sem.at[2])
        copy.start()

        def collect(r, acc):
            return acc + jnp.where(pos_ref[one(r), :] == slot, g_ref[one(r), :], 0.0)

        g = jnp.sum(lax.fori_loop(0, TOK, collect, jnp.zeros((LANE, LANE), F32), unroll=8), axis=1, keepdims=True)
        copy.wait()
        gh[...] = g * hc[...]

        def put(i, carry2):
            de_ref[one(lax.shift_right_logical(code_ref[c, i], 13)), :] += gh[one(i), :]
            return carry2

        repeat(jnp.minimum(count - c * LANE, LANE), put)
        return carry

    repeat((count + 127) // LANE, chunk)
    dwout_ref[...] = whole[0:LANE].reshape(KILO, LANE)
    for j in range(8):
        dwin_ref[:, LANE * j : LANE * j + LANE] = whole[LANE + 32 * j : 160 + 32 * j].reshape(WIDE, LANE)


LAST = 27
PART = 512


def core_exchange(me, ref, half, rref, send, recv):
    mine = coord(me, "core")
    c = remote(ref.at[pl.ds((1 - mine) * half, half)], rref.at[pl.ds(0, half)], send, recv, peer(me, "core", 1))
    c.start()
    c.wait_recv()
    add_rows(ref, mine * half, rref, 0, half, 1)
    return [c]


def grad_kernel(local, zst_ref, h_hbm, cand_hbm, cidb_hbm, logqb_hbm, candt_hbm, te_hbm, x_hbm, wout_hbm, pre_hbm, g_ref, loss_ref, tiles_out, dcand_out,
                ebuf, mc_ref, part, total, srecv, cur, norm, acc, recv, tiles, trecv, whole, dcand_ref,
                h_ref, cand_ref, cidb, logqb, candt_ref, te_ref, x_ref, wout_ref, pre_ref,
                load_sem, core_send, core_recv, send_sem, recv_sem):
    me = lax.axis_index("dp")
    core = coord(me, "core")
    loads = [
        pltpu.make_async_copy(a, b, load_sem.at[i]) for i, (a, b) in enumerate([
            (cand_hbm, cand_ref), (cidb_hbm, cidb), (logqb_hbm, logqb), (h_hbm, h_ref),
            (candt_hbm, candt_ref), (te_hbm, te_ref), (x_hbm, x_ref), (wout_hbm, wout_ref), (pre_hbm, pre_ref)])]
    for c in loads:
        c.start()
    barrier = greet(me)
    for g in range(8):
        for half in range(2):
            cur[g, 2, 4 * half : 4 * half + 4, :] = zst_ref[32 * half + 4 * g : 32 * half + 4 * g + 4, :]
    for c in loads[:4]:
        c.wait()

    def score(t, carry):
        for j in range(2):
            dots = nt_dot(cand_ref[...], h_ref[pl.ds(pl.multiple_of(t * PART + WIDE * j, WIDE), WIDE), :])
            for half in range(2):
                q = 2 * j + half
                r = t * 4 + q
                tgt = local[one(r), :]
                for c in range(8):
                    rows = slice(LANE * c, LANE * c + LANE)
                    s = dots[rows, LANE * half : LANE * half + LANE] - logqb[rows, :]
                    s = jnp.where(cidb[rows, :] == tgt, -1e9, s)
                    m = peak(s)
                    e = jnp.exp(s - m)
                    ebuf[t, rows, LANE * q : LANE * q + LANE] = e
                    mc_ref[r, c : c + 1, :] = m
                    part[q, c : c + 1, :] = down(e)
                most = mc_ref[r]
                top = peak(most)
                row = one(t // 8 * 4 + q)
                cur[t % 8, 0, row, :] = top
                cur[t % 8, 1, row, :] = down(part[q] * jnp.exp(most - top))
        return carry

    def part_loop(s, base, body):
        lax.fori_loop(base + H_FIRST[s], base + H_FIRST[s] + H_UNIT[s], body, 0)

    def score_part(s):
        part_loop(s, 0, score)
        part_loop(s, 8, score)

    def finish(s):
        stats.receive(s)

        def norms(g, carry):
            m, t, z = cur[32 + g, 0], cur[32 + g, 1], cur[32 + g, 2]
            top = jnp.maximum(m, z)
            log_norm = top + jnp.log(t * jnp.exp(m - top) + jnp.exp(z - top))
            grad = (jnp.exp(z - log_norm) - 1.0) / ALL
            total[...] += log_norm - z
            for half in range(2):
                rows = pl.ds(32 * half + 4 * g, 4)
                norm[rows, :] = log_norm[4 * half : 4 * half + 4, :]
                g_ref[rows, :] = grad[4 * half : 4 * half + 4, :]
            return carry

        part_loop(s, 0, norms)

    total[...] = jnp.zeros_like(total)

    def probs(t):
        blocks = []
        for q in range(4):
            r = t * 4 + q
            scale = jnp.exp(mc_ref[r] - norm[one(r), :]) / ALL
            blocks.append(jnp.concatenate([
                (ebuf[t, LANE * c : LANE * c + LANE, LANE * q : LANE * q + LANE] * scale[c : c + 1, :]).astype(BF16) for c in range(8)], axis=0))
        return jnp.concatenate(blocks, axis=1)

    def query_grad(t):
        dqt = jnp.dot(candt_ref[...], probs(t), preferred_element_type=F32)
        gcol = jnp.concatenate([column(g_ref[one(t * 4 + q), :]) for q in range(4)], axis=0)
        dq = jnp.transpose(dqt) + gcol * te_ref[pl.ds(pl.multiple_of(t * PART, PART), PART), :]
        return dq.reshape(TOK, 8, LANE)

    def swap(i):
        return remote(acc.at[pl.ds(((1 - core) * 8 + i) * TOK, TOK)], recv.at[pl.ds(i * TOK, TOK)], core_send.at[i], core_recv.at[i], peer(me, "core", 1))

    def give(i, carry):
        t = (1 - core) * 8 + i
        acc[pl.ds(t * TOK, TOK)] = query_grad(t)
        swap(i).start()
        return carry

    def keep(i, carry):
        t = core * 8 + i
        val = query_grad(t)
        swap(i).wait_recv()
        acc[pl.ds(t * TOK, TOK)] = val + recv[pl.ds(i * TOK, TOK)]
        return carry

    def cand_grad():
        dcand_ref[...] = jnp.zeros_like(dcand_ref)

        def accumulate(t, carry):
            dcand_ref[...] += jnp.dot(probs(t), h_ref[pl.ds(pl.multiple_of(t * PART, PART), PART), :], preferred_element_type=F32)
            return carry

        repeat(16, accumulate)
        dcand_copy.start()

    dcand_copy = pltpu.make_async_copy(dcand_ref, dcand_out, load_sem.at[9])
    streams = [(H_OFF[s], H_UNIT[s], ORDERS[s]) for s in range(3)]
    scatter = Scatter(me, acc, core * 512, recv, 512, streams, send_sem.at[0], recv_sem.at[0])
    stats = Stats(me, srecv, cur, send_sem.at[3], recv_sem.at[3])
    a, b, c = range(3)

    def keep_part(s):
        part_loop(s, 0, keep)
        scatter.send(s)

    score_part(a)
    pl.semaphore_wait(barrier, NPEER)
    stats.send(a)
    score_part(b)
    stats.advance(a)
    stats.send(b)
    score_part(c)
    stats.advance(a)
    stats.advance(b)
    stats.send(c)
    for s in (a, b, c):
        stats.advance(s)
    finish(a)
    for load in loads[4:]:
        load.wait()
    part_loop(a, 0, give)
    stats.advance(b)
    stats.advance(c)
    keep_part(a)
    finish(b)
    part_loop(b, 0, give)
    stats.advance(c)
    keep_part(b)
    finish(c)
    part_loop(c, 0, give)
    keep_part(c)
    loss_ref[...] = jnp.broadcast_to(jnp.sum(total[...], keepdims=True) / ALL, loss_ref.shape)
    cand_grad()
    scatter.rest()
    sent = stats.sent + scatter.sent
    rows = []
    for s in range(3):
        idx = block_index(me, ORDERS[s])
        for g in range(H_UNIT[s]):
            rows.append(acc[core * 512 + H_OFF[s] + idx * H_UNIT[s] + g])
    dh = jnp.concatenate(rows, axis=0).astype(BF16)
    act, slope = gelu_parts(pre_ref[...])
    d_pre = (slope * nt_dot(dh, wout_ref[...])).astype(BF16)
    dw_out = tn_dot(act.astype(BF16), dh)
    tiles[0:LANE] = dw_out.reshape(LANE, 8, LANE)
    dw_in = tn_dot(x_ref[...], d_pre)
    for j in range(8):
        tiles[LANE + 32 * j : 160 + 32 * j] = dw_in[:, LANE * j : LANE * j + LANE].reshape(32, 8, LANE)
    streams = [(TOK * s, 1, ORDERS[s]) for s in range(3)]
    half = core_exchange(me, tiles, 192, trecv, send_sem.at[1, LAST], recv_sem.at[1, LAST])
    scatter = Scatter(me, tiles, core * 192, trecv, 192, streams, send_sem.at[1], recv_sem.at[1])
    for s in range(3):
        scatter.send(s)
    scatter.rest()
    sent += half + scatter.sent
    streams = []
    for s in range(3):
        own = core * 192 + TOK * s + block_index(me, ORDERS[s])
        whole[own] = tiles[own]
        streams.append((whole, core * 192 + TOK * s, 1, ORDERS[s]))
    sent += gather_streams(me, streams, [(whole, 192)], send_sem.at[2], recv_sem.at[2])
    tiles_copy = pltpu.make_async_copy(whole, tiles_out, load_sem.at[10])
    tiles_copy.start()
    dcand_copy.wait()
    for c in sent:
        c.wait_send()

    def swap_done(i, carry):
        swap(i).wait_send()
        return carry

    repeat(8, swap_done)
    tiles_copy.wait()


def vmem(n):
    return [pl.BlockSpec(memory_space=pltpu.VMEM)] * n


def params(cid):
    return pltpu.CompilerParams(collective_id=cid, has_side_effects=True, vmem_limit_bytes=63 * KILO * KILO)


def dma(*shape):
    return pltpu.SemaphoreType.DMA(shape)


def solution(mesh):
    num_dev = mesh.shape["dp"]

    def local_step(features, w_in, w_out, table_blk, cand_ids, log_q, targets):
        dev_index = lax.axis_index("dp")
        block_rows = table_blk.shape[0]
        cand_dev = cand_ids.shape[0] // num_dev
        tok_total = features.shape[0] * num_dev
        anyspec = pl.BlockSpec(memory_space=pl.ANY)
        cid_rows, logq_rows = cand_ids.reshape(KILO, LANE), log_q.reshape(KILO, LANE)
        tall, h_all, pre, cand_rows, cand_t, cidb, logqb = pl.pallas_call(
            query_kernel,
            out_shape=[
                jax.ShapeDtypeStruct((LANE, 1, TOK), jnp.int32), jax.ShapeDtypeStruct((KILO, 8, LANE), BF16), jax.ShapeDtypeStruct((TOK, KILO), F32),
                jax.ShapeDtypeStruct((cand_dev, LANE), BF16), jax.ShapeDtypeStruct((LANE, cand_dev), BF16),
                jax.ShapeDtypeStruct((cand_dev, LANE), F32), jax.ShapeDtypeStruct((cand_dev, LANE), F32)],
            in_specs=vmem(4) + [anyspec] * 3, out_specs=vmem(1) + [anyspec] * 6,
            scratch_shapes=[
                pltpu.VMEM((block_rows, LANE), BF16), pltpu.VMEM((8, LANE), jnp.int32), pltpu.VMEM((8, LANE), F32), pltpu.VMEM((cand_dev, LANE), F32),
                pltpu.VMEM((KILO, 8, LANE), BF16), pltpu.VMEM((TOK, KILO), F32), pltpu.VMEM((cand_dev, LANE), BF16), pltpu.VMEM((LANE, cand_dev), BF16),
                pltpu.VMEM((cand_dev, LANE), F32), pltpu.VMEM((cand_dev, LANE), F32),
                dma(3), dma(7), dma(4 * NPEER), dma(4 * NPEER)],
            compiler_params=params(0), name="query_gather",
        )(features, w_in, w_out, targets[None, :], table_blk, cid_rows, logq_rows)
        query_all = h_all.reshape(ALL, LANE)
        smem = pl.BlockSpec(memory_space=pltpu.SMEM)
        square = pltpu.VMEM((LANE, LANE), F32)
        big = pltpu.CompilerParams(vmem_limit_bytes=63 * KILO * KILO)
        zst, pos, codes, local, hc, te = pl.pallas_call(
            target_kernel,
            out_shape=[
                jax.ShapeDtypeStruct((TOK, LANE), F32), jax.ShapeDtypeStruct((TOK, LANE), F32), jax.ShapeDtypeStruct((TOK, LANE), jnp.int32), jax.ShapeDtypeStruct((TOK, LANE), F32),
                jax.ShapeDtypeStruct((tok_total, LANE), F32), jax.ShapeDtypeStruct((tok_total, LANE), F32)],
            in_specs=vmem(1) + [anyspec] * 2, out_specs=vmem(4) + [anyspec] * 2,
            scratch_shapes=[
                pltpu.VMEM((tok_total, LANE), BF16), pltpu.VMEM((block_rows, LANE), BF16), pltpu.VMEM((tok_total + 8, LANE), F32), pltpu.VMEM((TOK, LANE), F32),
                square, square, pltpu.VMEM((LANE, TOK), jnp.int32), pltpu.VMEM((TOK, LANE), jnp.int32), pltpu.SMEM((TOK, LANE), jnp.int32), dma(4), pltpu.SemaphoreType.DMA],
            compiler_params=big, name="target_rows",
        )(tall, query_all, table_blk)
        grad_tgt, loss_row, tiles, dcand = pl.pallas_call(
            grad_kernel,
            out_shape=[
                jax.ShapeDtypeStruct((TOK, LANE), F32), jax.ShapeDtypeStruct((8, LANE), F32),
                jax.ShapeDtypeStruct((384, 8, LANE), F32), jax.ShapeDtypeStruct((cand_dev, LANE), F32)],
            in_specs=vmem(2) + [anyspec] * 9, out_specs=vmem(2) + [anyspec] * 2,
            scratch_shapes=[
                pltpu.VMEM((16, cand_dev, PART), F32), pltpu.VMEM((TOK, 8, LANE), F32), pltpu.VMEM((4, 8, LANE), F32), pltpu.VMEM((8, LANE), F32),
                pltpu.VMEM((80, 3, 8, LANE), F32), pltpu.VMEM((40, 3, 8, LANE), F32), pltpu.VMEM((TOK, LANE), F32),
                pltpu.VMEM((KILO, 8, LANE), F32), pltpu.VMEM((KILO, 8, LANE), F32),
                pltpu.VMEM((384, 8, LANE), F32), pltpu.VMEM((384, 8, LANE), F32), pltpu.VMEM((384, 8, LANE), F32), pltpu.VMEM((cand_dev, LANE), F32),
                pltpu.VMEM((tok_total, LANE), BF16), pltpu.VMEM((cand_dev, LANE), BF16), pltpu.VMEM((cand_dev, LANE), F32), pltpu.VMEM((cand_dev, LANE), F32),
                pltpu.VMEM((LANE, cand_dev), BF16), pltpu.VMEM((tok_total, LANE), F32),
                pltpu.VMEM(features.shape, BF16), pltpu.VMEM(w_out.shape, BF16), pltpu.VMEM(pre.shape, F32),
                dma(11), dma(8), dma(8), dma(4, 3 * NPEER), dma(4, 3 * NPEER)],
            compiler_params=params(1), name="grad_reduce",
        )(local, zst, query_all, cand_rows, cidb, logqb, cand_t, te, features, w_out, pre)
        grad_blk, grad_w_in, grad_w_out, loss = pl.pallas_call(
            table_kernel,
            out_shape=[
                jax.ShapeDtypeStruct((block_rows, LANE), F32), jax.ShapeDtypeStruct(w_in.shape, F32), jax.ShapeDtypeStruct(w_out.shape, F32),
                jax.ShapeDtypeStruct((1, 1), F32)],
            in_specs=[smem] + vmem(3) + [anyspec] * 4, out_specs=vmem(3) + [smem],
            scratch_shapes=[pltpu.SMEM((8, LANE), jnp.int32), pltpu.VMEM((cand_dev, LANE), F32), pltpu.VMEM((384, 8, LANE), F32), square, square, dma(4)],
            compiler_params=big, name="table_grad",
        )(codes, grad_tgt, pos, loss_row, cid_rows, dcand, tiles, hc)
        loss = loss.reshape(())
        return loss, grad_blk, grad_w_in, grad_w_out

    return jax.shard_map(local_step, mesh=mesh, in_specs=(P("dp", None), P(), P(), P("dp", None), P(), P(), P("dp")), out_specs=(P(), P("dp", None), P(), P()), check_vma=False)
```

```python
import functools
import jax
import jax.numpy as jnp
from jax import lax
from jax.experimental import pallas as pl
from jax.experimental.pallas import tpu as pltpu
from jax.sharding import PartitionSpec as P

MESH = pl.DeviceIdType.MESH
F32, BF16 = jnp.float32, jnp.bfloat16
COORD = {"core": (1, 2), "x": (2, 4), "y": (8, 4), "z": (32, 4)}
ORDERS = (("x", "y", "z"), ("y", "z", "x"), ("z", "x", "y"))
NDEV = 128
NPEER = 10
LANE, TOK, ALL, KILO, WIDE = 128, 64, 8192, 1024, 256


def one(i):
    return pl.ds(i, 1)


def repeat(n, body, unroll=1):
    lax.fori_loop(0, n, body, 0, unroll=unroll)


def down(v):
    return jnp.sum(v, axis=0, keepdims=True)


def across(v):
    return jnp.sum(v, axis=1, keepdims=True)


def peak(v):
    return jnp.max(v, axis=0, keepdims=True)


def flag(mask):
    return jnp.where(mask, 1.0, 0.0)


def iota(shape, dim):
    return lax.broadcasted_iota(jnp.int32, shape, dim)


def coord(me, axis):
    stride, radix = COORD[axis]
    return (me // stride) % radix


def peer(me, axis, k):
    stride, radix = COORD[axis]
    c = coord(me, axis)
    return me + ((c + k) % radix - c) * stride


def block_index(me, order):
    idx, weight = 0, 1
    for axis in order:
        idx = idx + coord(me, axis) * weight
        weight *= COORD[axis][1]
    return idx


def greet(me):
    barrier = pltpu.get_barrier_semaphore()
    for axis in COORD:
        for k in range(1, COORD[axis][1]):
            pl.semaphore_signal(barrier, inc=1, device_id=(peer(me, axis, k),), device_id_type=MESH)
    return barrier


def remote(src, dst, send, recv, dev):
    return pltpu.make_async_remote_copy(src_ref=src, dst_ref=dst, send_sem=send, recv_sem=recv, device_id=(dev,), device_id_type=MESH)


def gather_streams(me, streams, bulk, send_sem, recv_sem, between=None):
    pending, sent = [None] * len(streams), []
    for phase in range(4):
        for s, (ref, off, unit, order) in enumerate(streams):
            if pending[s]:
                for c in pending[s]:
                    c.wait_recv()
            if phase == 3:
                continue
            span = 4 ** phase
            idx = block_index(me, order)
            where = ref.at[pl.ds(off + (idx - idx % span) * unit, span * unit)]
            pending[s] = []
            for k in range(1, 4):
                n = s * 9 + phase * 3 + k - 1
                c = remote(where, where, send_sem.at[n], recv_sem.at[n], peer(me, order[phase], k))
                c.start()
                pending[s].append(c)
                sent.append(c)
        if between and phase < 3:
            between(phase)
    last = []
    for i, (ref, count) in enumerate(bulk):
        n = len(streams) * 9 + i
        where = ref.at[pl.ds(coord(me, "core") * count, count)]
        c = remote(where, where, send_sem.at[n], recv_sem.at[n], peer(me, "core", 1))
        c.start()
        last.append(c)
    if between:
        between(3)
    for c in last:
        c.wait_recv()
    return sent + last


def add_rows(ref, start, rref, base, count, parts):
    def add(i, carry):
        acc = ref[start + i]
        for k in range(parts):
            acc = acc + rref[base + k * count + i]
        ref[start + i] = acc
        return carry

    lax.fori_loop(0, count, add, 0, unroll=4)


class Scatter:
    def __init__(self, me, ref, first, rref, rbase, streams, send_sem, recv_sem):
        self.me, self.ref, self.first, self.rref, self.rbase = me, ref, first, rref, rbase
        self.streams, self.sems = streams, (send_sem, recv_sem)
        self.step, self.pending, self.sent = [0] * 3, [None] * 3, []

    def send(self, s):
        off, unit, order = self.streams[s]
        step, me = self.step[s], self.me
        span = 4 ** (2 - step)
        axis = order[2 - step]
        idx = block_index(me, order)
        start = self.first + off + (idx - idx % (4 * span)) * unit
        d = coord(me, axis)
        copies = []
        for k in range(1, 4):
            n = s * 9 + step * 3 + k - 1
            src = self.ref.at[pl.ds(start + (d + k) % 4 * span * unit, span * unit)]
            dst = self.rref.at[pl.ds(self.rbase + (k - 1) * span * unit, span * unit)]
            c = remote(src, dst, self.sems[0].at[n], self.sems[1].at[n], peer(me, axis, k))
            c.start()
            copies.append(c)
        self.sent += copies
        self.pending[s] = (copies, start + d * span * unit, self.rbase, span * unit)
        self.rbase += 3 * span * unit
        self.step[s] += 1

    def receive(self, s):
        copies, start, base, count = self.pending[s]
        for c in copies:
            c.wait_recv()
        add_rows(self.ref, start, self.rref, base, count, 3)

    def rest(self):
        for step in range(3):
            for s in range(3):
                self.receive(s)
                if step < 2:
                    self.send(s)


def gelu_parts(a):
    c = 0.7978845608028654
    inner = jnp.tanh(c * (a + 0.044715 * (a * a * a)))
    half = 0.5 * (1.0 + inner)
    return a * half, half + 0.5 * a * (1.0 - inner * inner) * (c * (1.0 + 3.0 * 0.044715 * (a * a)))


def nt_dot(a, b):
    return lax.dot_general(a, b, (((1,), (1,)), ((), ())), preferred_element_type=F32)


def tn_dot(a, b):
    return lax.dot_general(a, b, (((0,), (0,)), ((), ())), preferred_element_type=F32)


H_OFF = (0, 192, 384)
H_UNIT = (3, 3, 2)
H_FIRST = (0, 3, 6)


def column(row):
    return jnp.transpose(jnp.broadcast_to(row, (LANE, LANE)))


def query_kernel(x_hbm, win_hbm, wout_hbm, tgt_ref, blk_ref, cid_ref, logq_ref, tall_ref, h_out, pre_out, cand_out, candt_out, cidb_out, logqb_out,
                 x_ref, win_ref, wout_ref, blk, ids, lqs, rows, h_ref, pre_ref, cand_ref, candt_ref, cidb_ref, logqb_ref, load_sem, out_sem, send_sem, recv_sem):
    me = lax.axis_index("dp")
    mine = pl.ds(pl.multiple_of(me * 8, 8), 8)
    loads = [
        pltpu.make_async_copy(cid_ref.at[mine], ids, load_sem.at[0]), pltpu.make_async_copy(logq_ref.at[mine], lqs, load_sem.at[1]),
        pltpu.make_async_copy(blk_ref, blk, load_sem.at[2])]
    tower = [pltpu.make_async_copy(a, b, load_sem.at[3 + i]) for i, (a, b) in enumerate([(x_hbm, x_ref), (win_hbm, win_ref), (wout_hbm, wout_ref)])]
    for c in tower + loads:
        c.start()
    barrier = greet(me)
    for c in tower:
        c.wait()
    pre = jnp.dot(x_ref[...], win_ref[...], preferred_element_type=F32)
    pre_ref[0] = pre[:, :PART]
    pre_ref[1] = pre[:, PART:]
    act = gelu_parts(pre)[0].astype(BF16)
    query = jnp.dot(act, wout_ref[...], preferred_element_type=F32)
    core = coord(me, "core")
    streams = []
    for s in range(3):
        idx = block_index(me, ORDERS[s])
        for g in range(H_UNIT[s]):
            row = 8 * (H_FIRST[s] + g)
            h_ref[core * 512 + H_OFF[s] + idx * H_UNIT[s] + g] = query[row : row + 8, :].astype(BF16)
        streams.append((h_ref, core * 512 + H_OFF[s], H_UNIT[s], ORDERS[s]))
    tall_ref[core * TOK + block_index(me, ORDERS[2])] = tgt_ref[...]
    streams.append((tall_ref, core * TOK, 1, ORDERS[2]))
    lane = iota((1, LANE), 1)
    pl.semaphore_wait(barrier, NPEER)

    def pick(n, carry):
        part = pl.ds(pl.multiple_of(n // 8 * WIDE, WIDE), WIDE)
        first = n % 8 * KILO
        want = cidb_ref[part, :]
        picks = [flag(want == (lane + (first + u * LANE)).astype(F32)).astype(BF16) for u in range(8)]
        rows[part, :] += jnp.dot(jnp.concatenate(picks, axis=1), blk[pl.ds(pl.multiple_of(first, KILO), KILO), :], preferred_element_type=F32)
        return carry

    def fill(phase):
        if phase == 0:
            for c in loads:
                c.wait()
            for c in range(8):
                at = slice(c * LANE, c * LANE + LANE)
                cidb_ref[at, :] = column((ids[c : c + 1, :] - me * ALL).astype(F32))
                logqb_ref[at, :] = column(lqs[c : c + 1, :])
            rows[...] = jnp.zeros_like(rows)
        bounds = (0, 8, 17, 32, 32)
        lax.fori_loop(bounds[phase], bounds[phase + 1], pick, 0)
        if phase == 2:
            cand_ref[...] = rows[...].astype(BF16)
            candt_ref[...] = jnp.transpose(rows[...]).astype(BF16)
            for c in outs:
                c.start()
        if phase == 3:
            half(core).start()

    outs = [
        pltpu.make_async_copy(a, b, out_sem.at[i]) for i, (a, b) in enumerate([
            (pre_ref, pre_out), (cand_ref, cand_out), (candt_ref, candt_out), (cidb_ref, cidb_out), (logqb_ref, logqb_out)])]

    def half(c):
        where = pl.ds(c * 512, 512)
        return pltpu.make_async_copy(h_ref.at[where], h_out.at[where], out_sem.at[5 + c])

    sent = gather_streams(me, streams, [(h_ref, 512), (tall_ref, TOK)], send_sem, recv_sem, fill)
    half(1 - core).start()
    for c in outs:
        c.wait()
    for c in sent:
        c.wait_send()
    half(core).wait()
    half(1 - core).wait()


class Stats:
    def __init__(self, me, recv, cur, send_sem, recv_sem):
        self.me, self.recv, self.cur, self.sems = me, recv, cur, (send_sem, recv_sem)
        self.phase, self.pending, self.sent = [0] * 3, [None] * 3, []

    def send(self, s):
        phase, g0, ng = self.phase[s], H_FIRST[s], H_UNIT[s]
        axis = (ORDERS[s] + ("core",))[phase]
        src = self.cur.at[pl.ds(8 * phase + g0, ng)]
        self.pending[s] = []
        for k in range(1, COORD[axis][1]):
            n = s * NPEER + phase * 3 + k - 1
            dst = self.recv.at[pl.ds(8 * (3 * phase + k - 1) + g0, ng)]
            c = remote(src, dst, self.sems[0].at[n], self.sems[1].at[n], peer(self.me, axis, k))
            c.start()
            self.pending[s].append(c)
        self.sent += self.pending[s]

    def receive(self, s):
        phase, cur, recv, npart = self.phase[s], self.cur, self.recv, len(self.pending[s])
        for c in self.pending[s]:
            c.wait_recv()

        def merge(g, carry):
            old = cur[8 * phase + g]
            parts = [recv[8 * (3 * phase + k) + g] for k in range(npart)]
            top, z = old[0], old[2]
            for p in parts:
                top = jnp.maximum(top, p[0])
                z = jnp.maximum(z, p[2])
            total = old[1] * jnp.exp(old[0] - top)
            for p in parts:
                total = total + p[1] * jnp.exp(p[0] - top)
            row = 8 * (phase + 1) + g
            cur[row, 0] = top
            cur[row, 1] = total
            cur[row, 2] = z
            return carry

        lax.fori_loop(H_FIRST[s], H_FIRST[s] + H_UNIT[s], merge, 0)
        self.phase[s] += 1

    def advance(self, s):
        self.receive(s)
        self.send(s)


def arrange(tall_ref, square, tok_ref):
    def row(b, carry):
        square[one(b), :] = tall_ref[b]
        return carry

    repeat(LANE, row)
    ids = square[...]
    pieces = jnp.concatenate([lax.shift_right_logical(ids, 14), lax.shift_right_logical(ids, 7) & 127, ids & 127], axis=0).astype(F32).astype(BF16)
    b = iota((LANE, 1), 0)
    bt = iota((1, LANE), 1)

    def place(v, s):
        c = [lax.shift_right_logical(v, n) & 3 for n in (0, 2, 4)]
        z, x, y = c
        first, second, third = ((x, y, z), (y, z, x), (z, x, y))[s]
        return (v & TOK) + first + 4 * second + 16 * third

    for s in range(3):
        width, per = 8 * H_UNIT[s], (16, 16, 8)[s]
        span = width * per
        pick = iota((TOK, span), 0) == iota((TOK, span), 1) % width + 8 * H_FIRST[s]
        lanes = jnp.dot(pieces, flag(pick).astype(BF16), preferred_element_type=F32)
        mask = place(b, s) % per == iota((LANE, span), 1) // width
        group = flag(place(bt, s) // per == iota((LANE // per, LANE), 0)).astype(BF16)
        got = [
            jnp.dot(group, jnp.where(mask, lanes[LANE * p : LANE * p + LANE, :], 0.0).astype(BF16), preferred_element_type=F32).astype(jnp.int32)
            for p in range(3)]
        full = (got[0] * LANE + got[1]) * LANE + got[2]
        rows = span // LANE
        for a in range(LANE // per):
            half, rest = divmod(a, TOK // per)
            for r in range(rows):
                at = 32 * half + H_OFF[s] // 16 + rest * rows + r
                tok_ref[at : at + 1, :] = full[a : a + 1, LANE * r : LANE * r + LANE]


def target_kernel(tall_ref, h_hbm, blk_hbm, zst_ref, pos_ref, code_ref, local_ref, hc_ref, te_out, h_ref, blk_ref, te_ref, zd, hs, es, square, tgt_ref, codes, load_sem, sem):
    block_rows = blk_ref.shape[0]
    loads = [pltpu.make_async_copy(h_hbm, h_ref, load_sem.at[0]), pltpu.make_async_copy(blk_hbm, blk_ref, load_sem.at[1])]
    for c in loads:
        c.start()
    arrange(tall_ref, square, tgt_ref)
    rel = tgt_ref[...] - lax.axis_index("dp") * block_rows
    local_ref[...] = rel.astype(F32)
    own = (rel >= 0) & (rel < block_rows)
    own_f = flag(own)
    own_b = own_f.astype(BF16)
    up = iota((LANE, LANE), 0) < iota((LANE, LANE), 1)
    prefix = jnp.dot(own_b, flag(up).astype(BF16), preferred_element_type=F32)
    total = jnp.dot(own_b, jnp.ones((LANE, LANE), BF16), preferred_element_type=F32)
    low = iota((TOK, TOK), 0) > iota((TOK, TOK), 1)
    offset = jnp.dot(flag(low).astype(BF16), total.astype(BF16), preferred_element_type=F32)
    pos_ref[...] = jnp.where(own, prefix + offset, -1.0)
    zd[...] = jnp.zeros_like(zd)

    def clear(i, carry):
        te_ref[pl.ds(pl.multiple_of(i * LANE, LANE), LANE), :] = jnp.zeros((LANE, LANE), F32)
        return carry

    repeat(TOK, clear)
    count = jnp.sum(own_f).astype(jnp.int32)
    slot0 = iota((LANE, LANE), 0).astype(F32)
    lane = iota((1, LANE), 1)
    sub = iota((16, LANE), 0)

    def one_row(ref, i):
        tile = ref[pl.ds(pl.multiple_of(i & -16, 16), 16), :].astype(F32)
        return down(jnp.where(sub == (i & 15), tile, 0.0))

    def compact(c, carry):
        slot = slot0 + (c * LANE).astype(F32)

        def collect(r, code):
            mark = (tgt_ref[one(r), :] % block_rows) * ALL + (lane + r * LANE)
            return code + jnp.where(pos_ref[one(r), :] == slot, mark, 0)

        code = lax.fori_loop(0, TOK, collect, jnp.zeros((LANE, LANE), jnp.int32), unroll=8)
        row = across((code // ALL).astype(F32))
        tok = across((code % ALL).astype(F32))
        both = row.astype(jnp.int32) * ALL + tok.astype(jnp.int32)
        code_ref[one(c), :] = jnp.transpose(jnp.broadcast_to(both, (LANE, LANE)))[0:1, :]
        return carry

    chunks = (count + 127) // LANE
    repeat(chunks, compact)
    copy = pltpu.make_async_copy(code_ref, codes, sem)
    copy.start()
    for c in loads:
        c.wait()
    copy.wait()

    def chunk(c, carry):
        slot = slot0 + (c * LANE).astype(F32)
        left = count - c * LANE

        def fetch(i, carry2):
            for u in range(8):
                n = i * 8 + u
                v = codes[c, n]
                tok, at = v & (ALL - 1), lax.shift_right_logical(v, 13)
                hs[one(n), :] = one_row(h_ref, tok)
                row = one_row(blk_ref, at)
                es[one(n), :] = row
                te_ref[one(jnp.where(n < left, tok, ALL)), :] = row
            return carry2

        repeat((jnp.minimum(left, LANE) + 7) // 8, fetch)
        keep = pltpu.make_async_copy(hs, hc_ref.at[pl.ds(pl.multiple_of(c * LANE, LANE), LANE)], load_sem.at[3])
        keep.start()
        z = jnp.broadcast_to(across(hs[...] * es[...]), (LANE, LANE))

        def spread(r, carry2):
            hit = pos_ref[one(r), :] == slot
            zd[one(r), :] += down(jnp.where(hit, z, 0.0))
            return carry2

        repeat(TOK, spread, 8)
        keep.wait()
        return carry

    repeat(chunks, chunk)
    copy = pltpu.make_async_copy(te_ref.at[pl.ds(0, ALL)], te_out, load_sem.at[2])
    copy.start()
    zst_ref[...] = jnp.where(pos_ref[...] >= 0.0, zd[...], -jnp.inf)
    copy.wait()


def table_kernel(code_ref, g_ref, pos_ref, lossrow_ref, cid_hbm, dcand_hbm, tiles_hbm, hc_ref, de_ref, dwin_out, dwout_out, loss_ref, cidx, dcand, whole, hc, gh, dwin_ref, dwout_ref, sem):
    me = lax.axis_index("dp")
    loads = [pltpu.make_async_copy(cid_hbm.at[pl.ds(pl.multiple_of(me * 8, 8), 8)], cidx, sem.at[3]), pltpu.make_async_copy(dcand_hbm, dcand, sem.at[0]), pltpu.make_async_copy(tiles_hbm, whole, sem.at[1])]
    for c in loads:
        c.start()
    loss_ref[0, 0] = jnp.max(lossrow_ref[...])

    def clear(i, carry):
        de_ref[pl.ds(pl.multiple_of(i * LANE, LANE), LANE), :] = jnp.zeros((LANE, LANE), F32)
        return carry

    repeat(de_ref.shape[0] // LANE, clear)
    for c in loads:
        c.wait()
    for half in range(2):
        base = 192 * half
        dwout_ref[PART * half : PART * half + PART, :] = whole[base : base + TOK].reshape(PART, LANE)
        for j in range(4):
            at = base + TOK + 32 * j
            col = PART * half + LANE * j
            dwin_ref[:, col : col + LANE] = whole[at : at + 32].reshape(WIDE, LANE)
    outs = [pltpu.make_async_copy(dwin_ref, dwin_out, sem.at[4]), pltpu.make_async_copy(dwout_ref, dwout_out, sem.at[5])]
    for c in outs:
        c.start()

    base = me * ALL

    def place(i, carry):
        for u in range(32):
            de_ref[one(cidx[lax.shift_right_logical(i, 2), (i & 3) * 32 + u] - base), :] = dcand[one(i * 32 + u), :]
        return carry

    repeat(32, place)
    count = jnp.sum(flag(pos_ref[...] >= 0.0)).astype(jnp.int32)
    slot0 = iota((LANE, LANE), 0).astype(F32)

    def chunk(c, carry):
        slot = slot0 + (c * LANE).astype(F32)
        copy = pltpu.make_async_copy(hc_ref.at[pl.ds(pl.multiple_of(c * LANE, LANE), LANE)], hc, sem.at[2])
        copy.start()

        def collect(r, acc):
            return acc + jnp.where(pos_ref[one(r), :] == slot, g_ref[one(r), :], 0.0)

        g = jnp.sum(lax.fori_loop(0, TOK, collect, jnp.zeros((LANE, LANE), F32), unroll=8), axis=1, keepdims=True)
        copy.wait()
        gh[...] = g * hc[...]

        def put(i, carry2):
            de_ref[one(lax.shift_right_logical(code_ref[c, i], 13)), :] += gh[one(i), :]
            return carry2

        repeat(jnp.minimum(count - c * LANE, LANE), put)
        return carry

    repeat((count + 127) // LANE, chunk)
    for c in outs:
        c.wait()


LAST = 27
PART = 512


def grad_kernel(local, zst_ref, h_hbm, cand_hbm, cidb_hbm, logqb_hbm, candt_hbm, te_hbm, x_hbm, wout_hbm, pre_hbm, g_ref, loss_ref, tiles_out, dcand_out,
                ebuf, mc_ref, part, total, srecv, cur, norm, acc, recv, tiles, trecv, whole, dcand_ref,
                h_ref, cand_ref, cidb, logqb, candt_ref, te_ref, x_ref, wout_ref, pre_ref, xp_ref, prep_ref, dh_ref, dhp_ref,
                load_sem, core_send, core_recv, send_sem, recv_sem):
    me = lax.axis_index("dp")
    core = coord(me, "core")
    loads = [
        pltpu.make_async_copy(a, b, load_sem.at[i]) for i, (a, b) in enumerate([
            (cand_hbm, cand_ref), (cidb_hbm, cidb), (logqb_hbm, logqb), (h_hbm, h_ref),
            (candt_hbm, candt_ref), (te_hbm, te_ref), (x_hbm, x_ref), (wout_hbm, wout_ref), (pre_hbm, pre_ref)])]
    for c in loads:
        c.start()
    barrier = greet(me)
    for g in range(8):
        for half in range(2):
            cur[g, 2, 4 * half : 4 * half + 4, :] = zst_ref[32 * half + 4 * g : 32 * half + 4 * g + 4, :]
    for c in loads[:4]:
        c.wait()

    def score(t, carry):
        for j in range(2):
            dots = nt_dot(cand_ref[...], h_ref[pl.ds(pl.multiple_of(t * PART + WIDE * j, WIDE), WIDE), :])
            for half in range(2):
                q = 2 * j + half
                r = t * 4 + q
                tgt = local[one(r), :]
                for c in range(8):
                    rows = slice(LANE * c, LANE * c + LANE)
                    s = dots[rows, LANE * half : LANE * half + LANE] - logqb[rows, :]
                    s = jnp.where(cidb[rows, :] == tgt, -1e9, s)
                    m = peak(s)
                    e = jnp.exp(s - m)
                    ebuf[t, rows, LANE * q : LANE * q + LANE] = e
                    mc_ref[r, c : c + 1, :] = m
                    part[q, c : c + 1, :] = down(e)
                most = mc_ref[r]
                top = peak(most)
                row = one(t // 8 * 4 + q)
                cur[t % 8, 0, row, :] = top
                cur[t % 8, 1, row, :] = down(part[q] * jnp.exp(most - top))
        return carry

    def part_loop(s, base, body):
        lax.fori_loop(base + H_FIRST[s], base + H_FIRST[s] + H_UNIT[s], body, 0)

    def score_part(s):
        part_loop(s, 0, score)
        part_loop(s, 8, score)

    def finish(s):
        stats.receive(s)

        def norms(g, carry):
            m, t, z = cur[32 + g, 0], cur[32 + g, 1], cur[32 + g, 2]
            top = jnp.maximum(m, z)
            log_norm = top + jnp.log(t * jnp.exp(m - top) + jnp.exp(z - top))
            grad = (jnp.exp(z - log_norm) - 1.0) / ALL
            total[...] += log_norm - z
            for half in range(2):
                rows = pl.ds(32 * half + 4 * g, 4)
                norm[rows, :] = log_norm[4 * half : 4 * half + 4, :]
                g_ref[rows, :] = grad[4 * half : 4 * half + 4, :]
            return carry

        part_loop(s, 0, norms)

    total[...] = jnp.zeros_like(total)

    def probs(t):
        blocks = []
        for q in range(4):
            r = t * 4 + q
            scale = jnp.exp(mc_ref[r] - norm[one(r), :]) / ALL
            blocks.append(jnp.concatenate([
                (ebuf[t, LANE * c : LANE * c + LANE, LANE * q : LANE * q + LANE] * scale[c : c + 1, :]).astype(BF16) for c in range(8)], axis=0))
        return jnp.concatenate(blocks, axis=1)

    def query_grad(t):
        dqt = jnp.dot(candt_ref[...], probs(t), preferred_element_type=F32)
        gcol = jnp.concatenate([column(g_ref[one(t * 4 + q), :]) for q in range(4)], axis=0)
        dq = jnp.transpose(dqt) + gcol * te_ref[pl.ds(pl.multiple_of(t * PART, PART), PART), :]
        return dq.reshape(TOK, 8, LANE)

    def swap(i):
        return remote(acc.at[pl.ds(((1 - core) * 8 + i) * TOK, TOK)], recv.at[pl.ds(i * TOK, TOK)], core_send.at[i], core_recv.at[i], peer(me, "core", 1))

    def give(i, carry):
        t = (1 - core) * 8 + i
        acc[pl.ds(t * TOK, TOK)] = query_grad(t)
        swap(i).start()
        return carry

    def keep(i, carry):
        t = core * 8 + i
        val = query_grad(t)
        swap(i).wait_recv()
        acc[pl.ds(t * TOK, TOK)] = val + recv[pl.ds(i * TOK, TOK)]
        return carry

    def cand_grad():
        dcand_ref[...] = jnp.zeros_like(dcand_ref)

        def accumulate(t, carry):
            dcand_ref[...] += jnp.dot(probs(t), h_ref[pl.ds(pl.multiple_of(t * PART, PART), PART), :], preferred_element_type=F32)
            return carry

        repeat(16, accumulate)
        dcand_copy.start()

    dcand_copy = pltpu.make_async_copy(dcand_ref, dcand_out, load_sem.at[9])
    streams = [(H_OFF[s], H_UNIT[s], ORDERS[s]) for s in range(3)]
    scatter = Scatter(me, acc, core * 512, recv, 512, streams, send_sem.at[0], recv_sem.at[0])
    stats = Stats(me, srecv, cur, send_sem.at[3], recv_sem.at[3])
    a, b, c = range(3)

    def to_partner(src, dst, n):
        return remote(src, dst, send_sem.at[n, LAST + 1], recv_sem.at[n, LAST + 1], peer(me, "core", 1))

    give_x, give_pre = to_partner(x_ref, xp_ref, 0), to_partner(pre_ref.at[1 - core], prep_ref, 1)

    def keep_part(s):
        part_loop(s, 0, keep)
        scatter.send(s)

    score_part(a)
    pl.semaphore_wait(barrier, NPEER)
    stats.send(a)
    score_part(b)
    stats.advance(a)
    stats.send(b)
    score_part(c)
    stats.advance(a)
    stats.advance(b)
    stats.send(c)
    for s in (a, b, c):
        stats.advance(s)
    finish(a)
    for load in loads[4:]:
        load.wait()
    give_x.start()
    give_pre.start()
    part_loop(a, 0, give)
    stats.advance(b)
    stats.advance(c)
    keep_part(a)
    finish(b)
    part_loop(b, 0, give)
    stats.advance(c)
    keep_part(b)
    finish(c)
    part_loop(c, 0, give)
    keep_part(c)
    give_x.wait_recv()
    give_pre.wait_recv()
    loss_ref[...] = jnp.broadcast_to(jnp.sum(total[...], keepdims=True) / ALL, loss_ref.shape)
    cand_grad()
    scatter.rest()
    sent = stats.sent + scatter.sent
    for s in range(3):
        idx = block_index(me, ORDERS[s])
        for g in range(H_UNIT[s]):
            dh_ref[H_FIRST[s] + g] = acc[core * 512 + H_OFF[s] + idx * H_UNIT[s] + g].astype(BF16)
    give_dh = to_partner(dh_ref, dhp_ref, 2)
    give_dh.start()
    act, slope = gelu_parts(jnp.concatenate([pre_ref[core], prep_ref[...]], axis=0))
    give_dh.wait_recv()
    dh = jnp.concatenate([dh_ref[...].reshape(TOK, LANE), dhp_ref[...].reshape(TOK, LANE)], axis=0)
    d_pre = (slope * nt_dot(dh, wout_ref[pl.ds(pl.multiple_of(core * PART, PART), PART), :])).astype(BF16)
    dw_out = tn_dot(act.astype(BF16), dh)
    mine = core * 192
    tiles[pl.ds(mine, TOK)] = dw_out.reshape(TOK, 8, LANE)
    dw_in = tn_dot(jnp.concatenate([x_ref[...], xp_ref[...]], axis=0), d_pre)
    for j in range(4):
        tiles[pl.ds(mine + TOK + 32 * j, 32)] = dw_in[:, LANE * j : LANE * j + LANE].reshape(32, 8, LANE)
    streams = [(TOK * s, 1, ORDERS[s]) for s in range(3)]
    sent += [give_x, give_pre, give_dh]
    scatter = Scatter(me, tiles, core * 192, trecv, 0, streams, send_sem.at[1], recv_sem.at[1])
    for s in range(3):
        scatter.send(s)
    scatter.rest()
    sent += scatter.sent
    streams = []
    for s in range(3):
        own = core * 192 + TOK * s + block_index(me, ORDERS[s])
        whole[own] = tiles[own]
        streams.append((whole, core * 192 + TOK * s, 1, ORDERS[s]))
    sent += gather_streams(me, streams, [(whole, 192)], send_sem.at[2], recv_sem.at[2])
    tiles_copy = pltpu.make_async_copy(whole, tiles_out, load_sem.at[10])
    tiles_copy.start()
    dcand_copy.wait()
    for c in sent:
        c.wait_send()

    def swap_done(i, carry):
        swap(i).wait_send()
        return carry

    repeat(8, swap_done)
    tiles_copy.wait()


def vmem(n):
    return [pl.BlockSpec(memory_space=pltpu.VMEM)] * n


def params(cid):
    return pltpu.CompilerParams(collective_id=cid, has_side_effects=True, vmem_limit_bytes=63 * KILO * KILO)


def dma(*shape):
    return pltpu.SemaphoreType.DMA(shape)


def solution(mesh):
    num_dev = mesh.shape["dp"]

    def local_step(features, w_in, w_out, table_blk, cand_ids, log_q, targets):
        dev_index = lax.axis_index("dp")
        block_rows = table_blk.shape[0]
        cand_dev = cand_ids.shape[0] // num_dev
        tok_total = features.shape[0] * num_dev
        anyspec = pl.BlockSpec(memory_space=pl.ANY)
        cid_rows, logq_rows = cand_ids.reshape(KILO, LANE), log_q.reshape(KILO, LANE)
        tall, h_all, pre, cand_rows, cand_t, cidb, logqb = pl.pallas_call(
            query_kernel,
            out_shape=[
                jax.ShapeDtypeStruct((LANE, 1, TOK), jnp.int32), jax.ShapeDtypeStruct((KILO, 8, LANE), BF16), jax.ShapeDtypeStruct((2, TOK, PART), F32),
                jax.ShapeDtypeStruct((cand_dev, LANE), BF16), jax.ShapeDtypeStruct((LANE, cand_dev), BF16),
                jax.ShapeDtypeStruct((cand_dev, LANE), F32), jax.ShapeDtypeStruct((cand_dev, LANE), F32)],
            in_specs=[anyspec] * 3 + vmem(1) + [anyspec] * 3, out_specs=vmem(1) + [anyspec] * 6,
            scratch_shapes=[
                pltpu.VMEM(features.shape, BF16), pltpu.VMEM(w_in.shape, BF16), pltpu.VMEM(w_out.shape, BF16),
                pltpu.VMEM((block_rows, LANE), BF16), pltpu.VMEM((8, LANE), jnp.int32), pltpu.VMEM((8, LANE), F32), pltpu.VMEM((cand_dev, LANE), F32),
                pltpu.VMEM((KILO, 8, LANE), BF16), pltpu.VMEM((2, TOK, PART), F32), pltpu.VMEM((cand_dev, LANE), BF16), pltpu.VMEM((LANE, cand_dev), BF16),
                pltpu.VMEM((cand_dev, LANE), F32), pltpu.VMEM((cand_dev, LANE), F32),
                dma(6), dma(7), dma(4 * NPEER), dma(4 * NPEER)],
            compiler_params=params(0), name="query_gather",
        )(features, w_in, w_out, targets[None, :], table_blk, cid_rows, logq_rows)
        query_all = h_all.reshape(ALL, LANE)
        smem = pl.BlockSpec(memory_space=pltpu.SMEM)
        square = pltpu.VMEM((LANE, LANE), F32)
        big = pltpu.CompilerParams(vmem_limit_bytes=63 * KILO * KILO)
        zst, pos, codes, local, hc, te = pl.pallas_call(
            target_kernel,
            out_shape=[
                jax.ShapeDtypeStruct((TOK, LANE), F32), jax.ShapeDtypeStruct((TOK, LANE), F32), jax.ShapeDtypeStruct((TOK, LANE), jnp.int32), jax.ShapeDtypeStruct((TOK, LANE), F32),
                jax.ShapeDtypeStruct((tok_total, LANE), F32), jax.ShapeDtypeStruct((tok_total, LANE), F32)],
            in_specs=vmem(1) + [anyspec] * 2, out_specs=vmem(4) + [anyspec] * 2,
            scratch_shapes=[
                pltpu.VMEM((tok_total, LANE), BF16), pltpu.VMEM((block_rows, LANE), BF16), pltpu.VMEM((tok_total + 8, LANE), F32), pltpu.VMEM((TOK, LANE), F32),
                square, square, pltpu.VMEM((LANE, TOK), jnp.int32), pltpu.VMEM((TOK, LANE), jnp.int32), pltpu.SMEM((TOK, LANE), jnp.int32), dma(4), pltpu.SemaphoreType.DMA],
            compiler_params=big, name="target_rows",
        )(tall, query_all, table_blk)
        grad_tgt, loss_row, tiles, dcand = pl.pallas_call(
            grad_kernel,
            out_shape=[
                jax.ShapeDtypeStruct((TOK, LANE), F32), jax.ShapeDtypeStruct((8, LANE), F32),
                jax.ShapeDtypeStruct((384, 8, LANE), F32), jax.ShapeDtypeStruct((cand_dev, LANE), F32)],
            in_specs=vmem(2) + [anyspec] * 9, out_specs=vmem(2) + [anyspec] * 2,
            scratch_shapes=[
                pltpu.VMEM((16, cand_dev, PART), F32), pltpu.VMEM((TOK, 8, LANE), F32), pltpu.VMEM((4, 8, LANE), F32), pltpu.VMEM((8, LANE), F32),
                pltpu.VMEM((80, 3, 8, LANE), F32), pltpu.VMEM((40, 3, 8, LANE), F32), pltpu.VMEM((TOK, LANE), F32),
                pltpu.VMEM((KILO, 8, LANE), F32), pltpu.VMEM((KILO, 8, LANE), F32),
                pltpu.VMEM((384, 8, LANE), F32), pltpu.VMEM((384, 8, LANE), F32), pltpu.VMEM((384, 8, LANE), F32), pltpu.VMEM((cand_dev, LANE), F32),
                pltpu.VMEM((tok_total, LANE), BF16), pltpu.VMEM((cand_dev, LANE), BF16), pltpu.VMEM((cand_dev, LANE), F32), pltpu.VMEM((cand_dev, LANE), F32),
                pltpu.VMEM((LANE, cand_dev), BF16), pltpu.VMEM((tok_total, LANE), F32),
                pltpu.VMEM(features.shape, BF16), pltpu.VMEM(w_out.shape, BF16), pltpu.VMEM(pre.shape, F32),
                pltpu.VMEM(features.shape, BF16), pltpu.VMEM((TOK, PART), F32), pltpu.VMEM((8, 8, LANE), BF16), pltpu.VMEM((8, 8, LANE), BF16),
                dma(11), dma(8), dma(8), dma(4, 3 * NPEER), dma(4, 3 * NPEER)],
            compiler_params=params(1), name="grad_reduce",
        )(local, zst, query_all, cand_rows, cidb, logqb, cand_t, te, features, w_out, pre)
        grad_blk, grad_w_in, grad_w_out, loss = pl.pallas_call(
            table_kernel,
            out_shape=[
                jax.ShapeDtypeStruct((block_rows, LANE), F32), jax.ShapeDtypeStruct(w_in.shape, F32), jax.ShapeDtypeStruct(w_out.shape, F32),
                jax.ShapeDtypeStruct((1, 1), F32)],
            in_specs=[smem] + vmem(3) + [anyspec] * 4, out_specs=vmem(1) + [anyspec] * 2 + [smem],
            scratch_shapes=[pltpu.SMEM((8, LANE), jnp.int32), pltpu.VMEM((cand_dev, LANE), F32), pltpu.VMEM((384, 8, LANE), F32), square, square, pltpu.VMEM(w_in.shape, F32), pltpu.VMEM(w_out.shape, F32), dma(6)],
            compiler_params=big, name="table_grad",
        )(codes, grad_tgt, pos, loss_row, cid_rows, dcand, tiles, hc)
        loss = loss.reshape(())
        return loss, grad_blk, grad_w_in, grad_w_out

    return jax.shard_map(local_step, mesh=mesh, in_specs=(P("dp", None), P(), P(), P("dp", None), P(), P(), P("dp")), out_specs=(P(), P("dp", None), P(), P()), check_vma=False)
```

```python
import functools
import jax
import jax.numpy as jnp
from jax import lax
from jax.experimental import pallas as pl
from jax.experimental.pallas import tpu as pltpu
from jax.sharding import PartitionSpec as P

MESH = pl.DeviceIdType.MESH
F32, BF16 = jnp.float32, jnp.bfloat16
COORD = {"core": (1, 2), "x": (2, 4), "y": (8, 4), "z": (32, 4)}
ORDERS = (("x", "y", "z"), ("y", "z", "x"), ("z", "x", "y"))
NDEV = 128
NPEER = 10
LANE, TOK, ALL, KILO, WIDE = 128, 64, 8192, 1024, 256
HALF, SUB = 192, 32


def one(i):
    return pl.ds(i, 1)


def repeat(n, body, unroll=1):
    lax.fori_loop(0, n, body, 0, unroll=unroll)


def down(v):
    return jnp.sum(v, axis=0, keepdims=True)


def across(v):
    return jnp.sum(v, axis=1, keepdims=True)


def peak(v):
    return jnp.max(v, axis=0, keepdims=True)


def flag(mask):
    return jnp.where(mask, 1.0, 0.0)


def iota(shape, dim):
    return lax.broadcasted_iota(jnp.int32, shape, dim)


def coord(me, axis):
    stride, radix = COORD[axis]
    return (me // stride) % radix


def peer(me, axis, k):
    stride, radix = COORD[axis]
    c = coord(me, axis)
    return me + ((c + k) % radix - c) * stride


def block_index(me, order):
    idx, weight = 0, 1
    for axis in order:
        idx = idx + coord(me, axis) * weight
        weight *= COORD[axis][1]
    return idx


def greet(me):
    barrier = pltpu.get_barrier_semaphore()
    for axis in COORD:
        for k in range(1, COORD[axis][1]):
            pl.semaphore_signal(barrier, inc=1, device_id=(peer(me, axis, k),), device_id_type=MESH)
    return barrier


def remote(src, dst, send, recv, dev):
    return pltpu.make_async_remote_copy(src_ref=src, dst_ref=dst, send_sem=send, recv_sem=recv, device_id=(dev,), device_id_type=MESH)


def gather_streams(me, streams, bulk, send_sem, recv_sem, between=None, early=None):
    pending, sent = [None] * len(streams), []
    for phase in range(4):
        for s, (ref, off, unit, order) in enumerate(streams):
            if pending[s]:
                for c in pending[s]:
                    c.wait_recv()
            if phase == 3:
                if early and s == 0:
                    early()
                continue
            span = 4 ** phase
            idx = block_index(me, order)
            where = ref.at[pl.ds(off + (idx - idx % span) * unit, span * unit)]
            pending[s] = []
            for k in range(1, 4):
                n = s * 9 + phase * 3 + k - 1
                c = remote(where, where, send_sem.at[n], recv_sem.at[n], peer(me, order[phase], k))
                c.start()
                pending[s].append(c)
                sent.append(c)
        if between and phase < 3:
            between(phase)
    last = []
    for i, (ref, count) in enumerate(bulk):
        n = len(streams) * 9 + i
        where = ref.at[pl.ds(coord(me, "core") * count, count)]
        c = remote(where, where, send_sem.at[n], recv_sem.at[n], peer(me, "core", 1))
        c.start()
        last.append(c)
    if between:
        between(3)
    for c in last:
        c.wait_recv()
    return sent + last


def add_rows(ref, start, rref, base, count, parts):
    def add(i, carry):
        acc = ref[start + i]
        for k in range(parts):
            acc = acc + rref[base + k * count + i]
        ref[start + i] = acc
        return carry

    lax.fori_loop(0, count, add, 0, unroll=4)


class Scatter:
    def __init__(self, me, ref, first, rref, rbase, streams, send_sem, recv_sem):
        self.me, self.ref, self.first, self.rref, self.rbase = me, ref, first, rref, rbase
        self.streams, self.sems = streams, (send_sem, recv_sem)
        self.step, self.pending, self.sent = [0] * 3, [None] * 3, []

    def send(self, s):
        off, unit, order = self.streams[s]
        step, me = self.step[s], self.me
        span = 4 ** (2 - step)
        axis = order[2 - step]
        idx = block_index(me, order)
        start = self.first + off + (idx - idx % (4 * span)) * unit
        d = coord(me, axis)
        copies = []
        for k in range(1, 4):
            n = s * 9 + step * 3 + k - 1
            src = self.ref.at[pl.ds(start + (d + k) % 4 * span * unit, span * unit)]
            dst = self.rref.at[pl.ds(self.rbase + (k - 1) * span * unit, span * unit)]
            c = remote(src, dst, self.sems[0].at[n], self.sems[1].at[n], peer(me, axis, k))
            c.start()
            copies.append(c)
        self.sent += copies
        self.pending[s] = (copies, start + d * span * unit, self.rbase, span * unit)
        self.rbase += 3 * span * unit
        self.step[s] += 1

    def receive(self, s):
        copies, start, base, count = self.pending[s]
        for c in copies:
            c.wait_recv()
        add_rows(self.ref, start, self.rref, base, count, 3)

    def rest(self):
        for step in range(3):
            for s in range(3):
                self.receive(s)
                if step < 2:
                    self.send(s)


def gelu_parts(a):
    c = 0.7978845608028654
    inner = jnp.tanh(c * (a + 0.044715 * (a * a * a)))
    half = 0.5 * (1.0 + inner)
    return a * half, half + 0.5 * a * (1.0 - inner * inner) * (c * (1.0 + 3.0 * 0.044715 * (a * a)))


def nt_dot(a, b):
    return lax.dot_general(a, b, (((1,), (1,)), ((), ())), preferred_element_type=F32)


def tn_dot(a, b):
    return lax.dot_general(a, b, (((0,), (0,)), ((), ())), preferred_element_type=F32)


H_OFF = (0, HALF, 384)
H_UNIT = (3, 3, 2)
H_FIRST = (0, 3, 6)


def column(row):
    return jnp.transpose(jnp.broadcast_to(row, (LANE, LANE)))


def query_kernel(x_hbm, win_hbm, wout_hbm, tgt_ref, blk_ref, cid_ref, logq_ref, tok_ref, h_out, pre_out, cand_out, candt_out, cidb_out, logqb_out,
                 tall_ref, square, x_ref, win_ref, wout_ref, blk, ids, lqs, rows, h_ref, pre_ref, cand_ref, candt_ref, cidb_ref, logqb_ref, load_sem, out_sem, send_sem, recv_sem):
    me = lax.axis_index("dp")
    mine = pl.ds(pl.multiple_of(me * 8, 8), 8)
    loads = [
        pltpu.make_async_copy(cid_ref.at[mine], ids, load_sem.at[0]), pltpu.make_async_copy(logq_ref.at[mine], lqs, load_sem.at[1]),
        pltpu.make_async_copy(blk_ref, blk, load_sem.at[2])]
    tower = [pltpu.make_async_copy(a, b, load_sem.at[3 + i]) for i, (a, b) in enumerate([(x_hbm, x_ref), (win_hbm, win_ref), (wout_hbm, wout_ref)])]
    for c in tower + loads:
        c.start()
    barrier = greet(me)
    for c in tower:
        c.wait()
    pre = jnp.dot(x_ref[...], win_ref[...], preferred_element_type=F32)
    pre_ref[0] = pre[:, :PART]
    pre_ref[1] = pre[:, PART:]
    act = gelu_parts(pre)[0].astype(BF16)
    query = jnp.dot(act, wout_ref[...], preferred_element_type=F32)
    core = coord(me, "core")
    streams = [(tall_ref, core * TOK, 1, ORDERS[2])]
    for s in range(3):
        idx = block_index(me, ORDERS[s])
        for g in range(H_UNIT[s]):
            row = 8 * (H_FIRST[s] + g)
            h_ref[core * 512 + H_OFF[s] + idx * H_UNIT[s] + g] = query[row : row + 8, :].astype(BF16)
        streams.append((h_ref, core * 512 + H_OFF[s], H_UNIT[s], ORDERS[s]))
    tall_ref[core * TOK + block_index(me, ORDERS[2])] = tgt_ref[...]
    lane = iota((1, LANE), 1)
    pl.semaphore_wait(barrier, NPEER)

    def pick(n, carry):
        part = pl.ds(pl.multiple_of(n // 8 * WIDE, WIDE), WIDE)
        first = n % 8 * KILO
        want = cidb_ref[part, :]
        picks = [flag(want == (lane + (first + u * LANE)).astype(F32)).astype(BF16) for u in range(8)]
        rows[part, :] += jnp.dot(jnp.concatenate(picks, axis=1), blk[pl.ds(pl.multiple_of(first, KILO), KILO), :], preferred_element_type=F32)
        return carry

    def fill(phase):
        if phase == 0:
            for c in loads:
                c.wait()
            for c in range(8):
                at = slice(c * LANE, c * LANE + LANE)
                cidb_ref[at, :] = column((ids[c : c + 1, :] - me * ALL).astype(F32))
                logqb_ref[at, :] = column(lqs[c : c + 1, :])
            rows[...] = jnp.zeros_like(rows)
        bounds = (0, 8, 17, SUB, SUB)
        lax.fori_loop(bounds[phase], bounds[phase + 1], pick, 0)
        if phase == 2:
            cand_ref[...] = rows[...].astype(BF16)
            candt_ref[...] = jnp.transpose(rows[...]).astype(BF16)
            for c in outs:
                c.start()
        if phase == 3:
            half(core).start()

    outs = [
        pltpu.make_async_copy(a, b, out_sem.at[i]) for i, (a, b) in enumerate([
            (pre_ref, pre_out), (cand_ref, cand_out), (candt_ref, candt_out), (cidb_ref, cidb_out), (logqb_ref, logqb_out)])]

    def half(c):
        where = pl.ds(c * 512, 512)
        return pltpu.make_async_copy(h_ref.at[where], h_out.at[where], out_sem.at[5 + c])

    where = tall_ref.at[pl.ds(core * TOK, TOK)]
    swap = remote(where, where, send_sem.at[39], recv_sem.at[39], peer(me, "core", 1))

    def early():
        swap.start()
        swap.wait_recv()
        arrange(tall_ref, square, tok_ref)

    sent = gather_streams(me, streams, [(h_ref, 512)], send_sem, recv_sem, fill, early) + [swap]
    half(1 - core).start()
    for c in outs:
        c.wait()
    for c in sent:
        c.wait_send()
    half(core).wait()
    half(1 - core).wait()


class Stats:
    def __init__(self, me, recv, cur, send_sem, recv_sem):
        self.me, self.recv, self.cur, self.sems = me, recv, cur, (send_sem, recv_sem)
        self.phase, self.pending, self.sent = [0] * 3, [None] * 3, []

    def send(self, s):
        phase, g0, ng = self.phase[s], H_FIRST[s], H_UNIT[s]
        axis = (ORDERS[s] + ("core",))[phase]
        src = self.cur.at[pl.ds(8 * phase + g0, ng)]
        self.pending[s] = []
        for k in range(1, COORD[axis][1]):
            n = s * NPEER + phase * 3 + k - 1
            dst = self.recv.at[pl.ds(8 * (3 * phase + k - 1) + g0, ng)]
            c = remote(src, dst, self.sems[0].at[n], self.sems[1].at[n], peer(self.me, axis, k))
            c.start()
            self.pending[s].append(c)
        self.sent += self.pending[s]

    def receive(self, s):
        phase, cur, recv, npart = self.phase[s], self.cur, self.recv, len(self.pending[s])
        for c in self.pending[s]:
            c.wait_recv()

        def merge(g, carry):
            old = cur[8 * phase + g]
            parts = [recv[8 * (3 * phase + k) + g] for k in range(npart)]
            top, z = old[0], old[2]
            for p in parts:
                top = jnp.maximum(top, p[0])
                z = jnp.maximum(z, p[2])
            total = old[1] * jnp.exp(old[0] - top)
            for p in parts:
                total = total + p[1] * jnp.exp(p[0] - top)
            row = 8 * (phase + 1) + g
            cur[row, 0] = top
            cur[row, 1] = total
            cur[row, 2] = z
            return carry

        lax.fori_loop(H_FIRST[s], H_FIRST[s] + H_UNIT[s], merge, 0)
        self.phase[s] += 1

    def advance(self, s):
        self.receive(s)
        self.send(s)


def arrange(tall_ref, square, tok_ref):
    def row(b, carry):
        square[one(b), :] = tall_ref[b]
        return carry

    repeat(LANE, row)
    ids = square[...]
    pieces = jnp.concatenate([lax.shift_right_logical(ids, 14), lax.shift_right_logical(ids, 7) & 127, ids & 127], axis=0).astype(F32).astype(BF16)
    b = iota((LANE, 1), 0)
    bt = iota((1, LANE), 1)

    def place(v, s):
        c = [lax.shift_right_logical(v, n) & 3 for n in (0, 2, 4)]
        z, x, y = c
        first, second, third = ((x, y, z), (y, z, x), (z, x, y))[s]
        return (v & TOK) + first + 4 * second + 16 * third

    for s in range(3):
        width, per = 8 * H_UNIT[s], (16, 16, 8)[s]
        span = width * per
        pick = iota((TOK, span), 0) == iota((TOK, span), 1) % width + 8 * H_FIRST[s]
        lanes = jnp.dot(pieces, flag(pick).astype(BF16), preferred_element_type=F32)
        mask = place(b, s) % per == iota((LANE, span), 1) // width
        group = flag(place(bt, s) // per == iota((LANE // per, LANE), 0)).astype(BF16)
        got = [
            jnp.dot(group, jnp.where(mask, lanes[LANE * p : LANE * p + LANE, :], 0.0).astype(BF16), preferred_element_type=F32).astype(jnp.int32)
            for p in range(3)]
        full = (got[0] * LANE + got[1]) * LANE + got[2]
        rows = span // LANE
        for a in range(LANE // per):
            half, rest = divmod(a, TOK // per)
            for r in range(rows):
                at = SUB * half + H_OFF[s] // 16 + rest * rows + r
                tok_ref[at : at + 1, :] = full[a : a + 1, LANE * r : LANE * r + LANE]


def target_kernel(tgt_ref, h_hbm, blk_hbm, zst_ref, pos_ref, code_ref, local_ref, hc_ref, te_out, h_ref, blk_ref, te_ref, zd, hs, es, codes, load_sem, sem):
    block_rows = blk_ref.shape[0]
    loads = [pltpu.make_async_copy(h_hbm, h_ref, load_sem.at[0]), pltpu.make_async_copy(blk_hbm, blk_ref, load_sem.at[1])]
    for c in loads:
        c.start()
    rel = tgt_ref[...] - lax.axis_index("dp") * block_rows
    local_ref[...] = rel.astype(F32)
    own = (rel >= 0) & (rel < block_rows)
    own_f = flag(own)
    own_b = own_f.astype(BF16)
    up = iota((LANE, LANE), 0) < iota((LANE, LANE), 1)
    prefix = jnp.dot(own_b, flag(up).astype(BF16), preferred_element_type=F32)
    total = jnp.dot(own_b, jnp.ones((LANE, LANE), BF16), preferred_element_type=F32)
    low = iota((TOK, TOK), 0) > iota((TOK, TOK), 1)
    offset = jnp.dot(flag(low).astype(BF16), total.astype(BF16), preferred_element_type=F32)
    pos_ref[...] = jnp.where(own, prefix + offset, -1.0)
    zd[...] = jnp.zeros_like(zd)

    def clear(i, carry):
        te_ref[pl.ds(pl.multiple_of(i * LANE, LANE), LANE), :] = jnp.zeros((LANE, LANE), F32)
        return carry

    repeat(TOK, clear)
    count = jnp.sum(own_f).astype(jnp.int32)
    slot0 = iota((LANE, LANE), 0).astype(F32)
    lane = iota((1, LANE), 1)
    sub = iota((16, LANE), 0)

    def one_row(ref, i):
        tile = ref[pl.ds(pl.multiple_of(i & -16, 16), 16), :].astype(F32)
        return down(jnp.where(sub == (i & 15), tile, 0.0))

    def compact(c, carry):
        slot = slot0 + (c * LANE).astype(F32)

        def collect(r, code):
            mark = (tgt_ref[one(r), :] % block_rows) * ALL + (lane + r * LANE)
            return code + jnp.where(pos_ref[one(r), :] == slot, mark, 0)

        code = lax.fori_loop(0, TOK, collect, jnp.zeros((LANE, LANE), jnp.int32), unroll=8)
        row = across((code // ALL).astype(F32))
        tok = across((code % ALL).astype(F32))
        both = row.astype(jnp.int32) * ALL + tok.astype(jnp.int32)
        code_ref[one(c), :] = jnp.transpose(jnp.broadcast_to(both, (LANE, LANE)))[0:1, :]
        return carry

    chunks = (count + 127) // LANE
    repeat(chunks, compact)
    copy = pltpu.make_async_copy(code_ref, codes, sem)
    copy.start()
    for c in loads:
        c.wait()
    copy.wait()

    def chunk(c, carry):
        slot = slot0 + (c * LANE).astype(F32)
        left = count - c * LANE

        def fetch(i, carry2):
            for u in range(8):
                n = i * 8 + u
                v = codes[c, n]
                tok, at = v & (ALL - 1), lax.shift_right_logical(v, 13)
                hs[one(n), :] = one_row(h_ref, tok)
                row = one_row(blk_ref, at)
                es[one(n), :] = row
                te_ref[one(jnp.where(n < left, tok, ALL)), :] = row
            return carry2

        repeat((jnp.minimum(left, LANE) + 7) // 8, fetch)
        keep = pltpu.make_async_copy(hs, hc_ref.at[pl.ds(pl.multiple_of(c * LANE, LANE), LANE)], load_sem.at[3])
        keep.start()
        z = jnp.broadcast_to(across(hs[...] * es[...]), (LANE, LANE))

        def spread(r, carry2):
            hit = pos_ref[one(r), :] == slot
            zd[one(r), :] += down(jnp.where(hit, z, 0.0))
            return carry2

        repeat(TOK, spread, 8)
        keep.wait()
        return carry

    repeat(chunks, chunk)
    copy = pltpu.make_async_copy(te_ref.at[pl.ds(0, ALL)], te_out, load_sem.at[2])
    copy.start()
    zst_ref[...] = jnp.where(pos_ref[...] >= 0.0, zd[...], -jnp.inf)
    copy.wait()


def table_kernel(code_ref, g_ref, pos_ref, lossrow_ref, cid_hbm, dcand_hbm, tiles_hbm, hc_ref, de_ref, dwin_out, dwout_out, loss_ref, cidx, dcand, whole, hc, gh, dwin_ref, dwout_ref, sem):
    me = lax.axis_index("dp")
    loads = [pltpu.make_async_copy(cid_hbm.at[pl.ds(pl.multiple_of(me * 8, 8), 8)], cidx, sem.at[3]), pltpu.make_async_copy(dcand_hbm, dcand, sem.at[0]), pltpu.make_async_copy(tiles_hbm, whole, sem.at[1])]
    for c in loads:
        c.start()
    loss_ref[0, 0] = jnp.max(lossrow_ref[...])

    def clear(i, carry):
        de_ref[pl.ds(pl.multiple_of(i * LANE, LANE), LANE), :] = jnp.zeros((LANE, LANE), F32)
        return carry

    repeat(de_ref.shape[0] // LANE, clear)
    for c in loads[:2]:
        c.wait()
    base = me * ALL

    def place(i, carry):
        for u in range(SUB):
            de_ref[one(cidx[lax.shift_right_logical(i, 2), (i & 3) * SUB + u] - base), :] = dcand[one(i * SUB + u), :]
        return carry

    repeat(SUB, place)
    loads[-1].wait()
    for half in range(2):
        base = HALF * half
        dwout_ref[PART * half : PART * half + PART, :] = whole[base : base + TOK].reshape(PART, LANE)
        for j in range(4):
            at = base + TOK + SUB * j
            col = PART * half + LANE * j
            dwin_ref[:, col : col + LANE] = whole[at : at + SUB].reshape(WIDE, LANE)
    outs = [pltpu.make_async_copy(dwin_ref, dwin_out, sem.at[4]), pltpu.make_async_copy(dwout_ref, dwout_out, sem.at[5])]
    for c in outs:
        c.start()
    count = jnp.sum(flag(pos_ref[...] >= 0.0)).astype(jnp.int32)
    slot0 = iota((LANE, LANE), 0).astype(F32)

    def chunk(c, carry):
        slot = slot0 + (c * LANE).astype(F32)
        copy = pltpu.make_async_copy(hc_ref.at[pl.ds(pl.multiple_of(c * LANE, LANE), LANE)], hc, sem.at[2])
        copy.start()

        def collect(r, acc):
            return acc + jnp.where(pos_ref[one(r), :] == slot, g_ref[one(r), :], 0.0)

        g = jnp.sum(lax.fori_loop(0, TOK, collect, jnp.zeros((LANE, LANE), F32), unroll=8), axis=1, keepdims=True)
        copy.wait()
        gh[...] = g * hc[...]

        def put(i, carry2):
            de_ref[one(lax.shift_right_logical(code_ref[c, i], 13)), :] += gh[one(i), :]
            return carry2

        repeat(jnp.minimum(count - c * LANE, LANE), put)
        return carry

    repeat((count + 127) // LANE, chunk)
    for c in outs:
        c.wait()


LAST = 27
PART = 512


def grad_kernel(local, zst_ref, h_hbm, cand_hbm, cidb_hbm, logqb_hbm, candt_hbm, te_hbm, x_hbm, wout_hbm, pre_hbm, g_ref, loss_ref, tiles_out, dcand_out,
                ebuf, mc_ref, part, total, srecv, cur, norm, acc, recv, tiles, trecv, whole, dcand_ref,
                h_ref, cand_ref, cidb, logqb, candt_ref, te_ref, x_ref, wout_ref, pre_ref, xp_ref, prep_ref, dh_ref, dhp_ref,
                load_sem, core_send, core_recv, send_sem, recv_sem):
    me = lax.axis_index("dp")
    core = coord(me, "core")
    loads = [
        pltpu.make_async_copy(a, b, load_sem.at[i]) for i, (a, b) in enumerate([
            (cand_hbm, cand_ref), (cidb_hbm, cidb), (logqb_hbm, logqb), (h_hbm, h_ref),
            (candt_hbm, candt_ref), (te_hbm, te_ref), (x_hbm, x_ref), (wout_hbm, wout_ref), (pre_hbm, pre_ref)])]
    for c in loads:
        c.start()
    barrier = greet(me)
    for g in range(8):
        for half in range(2):
            cur[g, 2, 4 * half : 4 * half + 4, :] = zst_ref[SUB * half + 4 * g : SUB * half + 4 * g + 4, :]
    for c in loads[:4]:
        c.wait()

    def score(t, carry):
        for j in range(2):
            dots = nt_dot(cand_ref[...], h_ref[pl.ds(pl.multiple_of(t * PART + WIDE * j, WIDE), WIDE), :])
            for half in range(2):
                q = 2 * j + half
                r = t * 4 + q
                tgt = local[one(r), :]
                for c in range(8):
                    rows = slice(LANE * c, LANE * c + LANE)
                    s = dots[rows, LANE * half : LANE * half + LANE] - logqb[rows, :]
                    s = jnp.where(cidb[rows, :] == tgt, -1e9, s)
                    m = peak(s)
                    e = jnp.exp(s - m)
                    ebuf[t, rows, LANE * q : LANE * q + LANE] = e
                    mc_ref[r, c : c + 1, :] = m
                    part[q, c : c + 1, :] = down(e)
                most = mc_ref[r]
                top = peak(most)
                row = one(t // 8 * 4 + q)
                cur[t % 8, 0, row, :] = top
                cur[t % 8, 1, row, :] = down(part[q] * jnp.exp(most - top))
        return carry

    def part_loop(s, base, body):
        lax.fori_loop(base + H_FIRST[s], base + H_FIRST[s] + H_UNIT[s], body, 0)

    def score_part(s):
        part_loop(s, 0, score)
        part_loop(s, 8, score)

    def finish(s):
        stats.receive(s)

        def norms(g, carry):
            m, t, z = cur[SUB + g, 0], cur[SUB + g, 1], cur[SUB + g, 2]
            top = jnp.maximum(m, z)
            log_norm = top + jnp.log(t * jnp.exp(m - top) + jnp.exp(z - top))
            grad = (jnp.exp(z - log_norm) - 1.0) / ALL
            total[...] += log_norm - z
            for half in range(2):
                rows = pl.ds(SUB * half + 4 * g, 4)
                norm[rows, :] = log_norm[4 * half : 4 * half + 4, :]
                g_ref[rows, :] = grad[4 * half : 4 * half + 4, :]
            return carry

        part_loop(s, 0, norms)

    total[...] = jnp.zeros_like(total)

    def probs(t):
        blocks = []
        for q in range(4):
            r = t * 4 + q
            scale = jnp.exp(mc_ref[r] - norm[one(r), :]) / ALL
            blocks.append(jnp.concatenate([
                (ebuf[t, LANE * c : LANE * c + LANE, LANE * q : LANE * q + LANE] * scale[c : c + 1, :]).astype(BF16) for c in range(8)], axis=0))
        return jnp.concatenate(blocks, axis=1)

    def query_grad(t):
        dqt = jnp.dot(candt_ref[...], probs(t), preferred_element_type=F32)
        gcol = jnp.concatenate([column(g_ref[one(t * 4 + q), :]) for q in range(4)], axis=0)
        dq = jnp.transpose(dqt) + gcol * te_ref[pl.ds(pl.multiple_of(t * PART, PART), PART), :]
        return dq.reshape(TOK, 8, LANE)

    def swap(i):
        return remote(acc.at[pl.ds(((1 - core) * 8 + i) * TOK, TOK)], recv.at[pl.ds(i * TOK, TOK)], core_send.at[i], core_recv.at[i], peer(me, "core", 1))

    def give(i, carry):
        t = (1 - core) * 8 + i
        acc[pl.ds(t * TOK, TOK)] = query_grad(t)
        swap(i).start()
        return carry

    def keep(i, carry):
        t = core * 8 + i
        val = query_grad(t)
        swap(i).wait_recv()
        acc[pl.ds(t * TOK, TOK)] = val + recv[pl.ds(i * TOK, TOK)]
        return carry

    def cand_grad():
        dcand_ref[...] = jnp.zeros_like(dcand_ref)

        def accumulate(t, carry):
            dcand_ref[...] += jnp.dot(probs(t), h_ref[pl.ds(pl.multiple_of(t * PART, PART), PART), :], preferred_element_type=F32)
            return carry

        repeat(16, accumulate)
        dcand_copy.start()

    dcand_copy = pltpu.make_async_copy(dcand_ref, dcand_out, load_sem.at[9])
    streams = [(H_OFF[s], H_UNIT[s], ORDERS[s]) for s in range(3)]
    scatter = Scatter(me, acc, core * 512, recv, 512, streams, send_sem.at[0], recv_sem.at[0])
    stats = Stats(me, srecv, cur, send_sem.at[3], recv_sem.at[3])
    a, b, c = range(3)

    def to_partner(src, dst, n):
        return remote(src, dst, send_sem.at[n, LAST + 1], recv_sem.at[n, LAST + 1], peer(me, "core", 1))

    give_x, give_pre = to_partner(x_ref, xp_ref, 0), to_partner(pre_ref.at[1 - core], prep_ref, 1)

    def keep_part(s):
        part_loop(s, 0, keep)
        scatter.send(s)

    score_part(a)
    pl.semaphore_wait(barrier, NPEER)
    stats.send(a)
    score_part(b)
    stats.advance(a)
    stats.send(b)
    score_part(c)
    stats.advance(a)
    stats.advance(b)
    stats.send(c)
    for s in (a, b, c):
        stats.advance(s)
    finish(a)
    for load in loads[4:]:
        load.wait()
    give_x.start()
    give_pre.start()
    part_loop(a, 0, give)
    stats.advance(b)
    stats.advance(c)
    keep_part(a)
    finish(b)
    part_loop(b, 0, give)
    stats.advance(c)
    keep_part(b)
    finish(c)
    part_loop(c, 0, give)
    keep_part(c)
    give_x.wait_recv()
    give_pre.wait_recv()
    loss_ref[...] = jnp.broadcast_to(jnp.sum(total[...], keepdims=True) / ALL, loss_ref.shape)
    cand_grad()
    scatter.rest()
    sent = stats.sent + scatter.sent
    for s in range(3):
        idx = block_index(me, ORDERS[s])
        for g in range(H_UNIT[s]):
            dh_ref[H_FIRST[s] + g] = acc[core * 512 + H_OFF[s] + idx * H_UNIT[s] + g].astype(BF16)
    give_dh = to_partner(dh_ref, dhp_ref, 2)
    give_dh.start()
    act, slope = gelu_parts(jnp.concatenate([pre_ref[core], prep_ref[...]], axis=0))
    give_dh.wait_recv()
    dh = jnp.concatenate([dh_ref[...].reshape(TOK, LANE), dhp_ref[...].reshape(TOK, LANE)], axis=0)
    d_pre = (slope * nt_dot(dh, wout_ref[pl.ds(pl.multiple_of(core * PART, PART), PART), :])).astype(BF16)
    dw_out = tn_dot(act.astype(BF16), dh)
    mine = core * HALF
    tiles[pl.ds(mine, TOK)] = dw_out.reshape(TOK, 8, LANE)
    dw_in = tn_dot(jnp.concatenate([x_ref[...], xp_ref[...]], axis=0), d_pre)
    for j in range(4):
        tiles[pl.ds(mine + TOK + SUB * j, SUB)] = dw_in[:, LANE * j : LANE * j + LANE].reshape(SUB, 8, LANE)
    streams = [(TOK * s, 1, ORDERS[s]) for s in range(3)]
    sent += [give_x, give_pre, give_dh]
    scatter = Scatter(me, tiles, core * HALF, trecv, 0, streams, send_sem.at[1], recv_sem.at[1])
    for s in range(3):
        scatter.send(s)
    scatter.rest()
    sent += scatter.sent
    streams = []
    for s in range(3):
        own = core * HALF + TOK * s + block_index(me, ORDERS[s])
        whole[own] = tiles[own]
        streams.append((whole, core * HALF + TOK * s, 1, ORDERS[s]))
    def leave(c):
        where = pl.ds(c * HALF, HALF)
        return pltpu.make_async_copy(whole.at[where], tiles_out.at[where], load_sem.at[10 + c])

    def push(phase):
        if phase == 3:
            leave(core).start()

    sent += gather_streams(me, streams, [(whole, HALF)], send_sem.at[2], recv_sem.at[2], push)
    leave(1 - core).start()
    dcand_copy.wait()
    for c in sent:
        c.wait_send()

    def swap_done(i, carry):
        swap(i).wait_send()
        return carry

    repeat(8, swap_done)
    leave(core).wait()
    leave(1 - core).wait()


def vmem(n):
    return [pl.BlockSpec(memory_space=pltpu.VMEM)] * n


def params(cid):
    return pltpu.CompilerParams(collective_id=cid, has_side_effects=True, vmem_limit_bytes=63 * KILO * KILO)


def dma(*shape):
    return pltpu.SemaphoreType.DMA(shape)


def solution(mesh):
    num_dev = mesh.shape["dp"]

    def local_step(features, w_in, w_out, table_blk, cand_ids, log_q, targets):
        dev_index = lax.axis_index("dp")
        block_rows = table_blk.shape[0]
        cand_dev = cand_ids.shape[0] // num_dev
        tok_total = features.shape[0] * num_dev
        anyspec = pl.BlockSpec(memory_space=pl.ANY)
        cid_rows, logq_rows = cand_ids.reshape(KILO, LANE), log_q.reshape(KILO, LANE)
        tgt_all, h_all, pre, cand_rows, cand_t, cidb, logqb = pl.pallas_call(
            query_kernel,
            out_shape=[
                jax.ShapeDtypeStruct((TOK, LANE), jnp.int32), jax.ShapeDtypeStruct((KILO, 8, LANE), BF16), jax.ShapeDtypeStruct((2, TOK, PART), F32),
                jax.ShapeDtypeStruct((cand_dev, LANE), BF16), jax.ShapeDtypeStruct((LANE, cand_dev), BF16),
                jax.ShapeDtypeStruct((cand_dev, LANE), F32), jax.ShapeDtypeStruct((cand_dev, LANE), F32)],
            in_specs=[anyspec] * 3 + vmem(1) + [anyspec] * 3, out_specs=vmem(1) + [anyspec] * 6,
            scratch_shapes=[
                pltpu.VMEM((LANE, 1, TOK), jnp.int32), pltpu.VMEM((LANE, TOK), jnp.int32),
                pltpu.VMEM(features.shape, BF16), pltpu.VMEM(w_in.shape, BF16), pltpu.VMEM(w_out.shape, BF16),
                pltpu.VMEM((block_rows, LANE), BF16), pltpu.VMEM((8, LANE), jnp.int32), pltpu.VMEM((8, LANE), F32), pltpu.VMEM((cand_dev, LANE), F32),
                pltpu.VMEM((KILO, 8, LANE), BF16), pltpu.VMEM((2, TOK, PART), F32), pltpu.VMEM((cand_dev, LANE), BF16), pltpu.VMEM((LANE, cand_dev), BF16),
                pltpu.VMEM((cand_dev, LANE), F32), pltpu.VMEM((cand_dev, LANE), F32),
                dma(6), dma(7), dma(4 * NPEER), dma(4 * NPEER)],
            compiler_params=params(0), name="query_gather",
        )(features, w_in, w_out, targets[None, :], table_blk, cid_rows, logq_rows)
        query_all = h_all.reshape(ALL, LANE)
        smem = pl.BlockSpec(memory_space=pltpu.SMEM)
        square = pltpu.VMEM((LANE, LANE), F32)
        big = pltpu.CompilerParams(vmem_limit_bytes=63 * KILO * KILO)
        zst, pos, codes, local, hc, te = pl.pallas_call(
            target_kernel,
            out_shape=[
                jax.ShapeDtypeStruct((TOK, LANE), F32), jax.ShapeDtypeStruct((TOK, LANE), F32), jax.ShapeDtypeStruct((TOK, LANE), jnp.int32), jax.ShapeDtypeStruct((TOK, LANE), F32),
                jax.ShapeDtypeStruct((tok_total, LANE), F32), jax.ShapeDtypeStruct((tok_total, LANE), F32)],
            in_specs=vmem(1) + [anyspec] * 2, out_specs=vmem(4) + [anyspec] * 2,
            scratch_shapes=[
                pltpu.VMEM((tok_total, LANE), BF16), pltpu.VMEM((block_rows, LANE), BF16), pltpu.VMEM((tok_total + 8, LANE), F32), pltpu.VMEM((TOK, LANE), F32),
                square, square, pltpu.SMEM((TOK, LANE), jnp.int32), dma(4), pltpu.SemaphoreType.DMA],
            compiler_params=big, name="target_rows",
        )(tgt_all, query_all, table_blk)
        grad_tgt, loss_row, tiles, dcand = pl.pallas_call(
            grad_kernel,
            out_shape=[
                jax.ShapeDtypeStruct((TOK, LANE), F32), jax.ShapeDtypeStruct((8, LANE), F32),
                jax.ShapeDtypeStruct((384, 8, LANE), F32), jax.ShapeDtypeStruct((cand_dev, LANE), F32)],
            in_specs=vmem(2) + [anyspec] * 9, out_specs=vmem(2) + [anyspec] * 2,
            scratch_shapes=[
                pltpu.VMEM((16, cand_dev, PART), F32), pltpu.VMEM((TOK, 8, LANE), F32), pltpu.VMEM((4, 8, LANE), F32), pltpu.VMEM((8, LANE), F32),
                pltpu.VMEM((80, 3, 8, LANE), F32), pltpu.VMEM((40, 3, 8, LANE), F32), pltpu.VMEM((TOK, LANE), F32),
                pltpu.VMEM((KILO, 8, LANE), F32), pltpu.VMEM((KILO, 8, LANE), F32),
                pltpu.VMEM((384, 8, LANE), F32), pltpu.VMEM((384, 8, LANE), F32), pltpu.VMEM((384, 8, LANE), F32), pltpu.VMEM((cand_dev, LANE), F32),
                pltpu.VMEM((tok_total, LANE), BF16), pltpu.VMEM((cand_dev, LANE), BF16), pltpu.VMEM((cand_dev, LANE), F32), pltpu.VMEM((cand_dev, LANE), F32),
                pltpu.VMEM((LANE, cand_dev), BF16), pltpu.VMEM((tok_total, LANE), F32),
                pltpu.VMEM(features.shape, BF16), pltpu.VMEM(w_out.shape, BF16), pltpu.VMEM(pre.shape, F32),
                pltpu.VMEM(features.shape, BF16), pltpu.VMEM((TOK, PART), F32), pltpu.VMEM((8, 8, LANE), BF16), pltpu.VMEM((8, 8, LANE), BF16),
                dma(12), dma(8), dma(8), dma(4, 3 * NPEER), dma(4, 3 * NPEER)],
            compiler_params=params(1), name="grad_reduce",
        )(local, zst, query_all, cand_rows, cidb, logqb, cand_t, te, features, w_out, pre)
        grad_blk, grad_w_in, grad_w_out, loss = pl.pallas_call(
            table_kernel,
            out_shape=[
                jax.ShapeDtypeStruct((block_rows, LANE), F32), jax.ShapeDtypeStruct(w_in.shape, F32), jax.ShapeDtypeStruct(w_out.shape, F32),
                jax.ShapeDtypeStruct((1, 1), F32)],
            in_specs=[smem] + vmem(3) + [anyspec] * 4, out_specs=vmem(1) + [anyspec] * 2 + [smem],
            scratch_shapes=[pltpu.SMEM((8, LANE), jnp.int32), pltpu.VMEM((cand_dev, LANE), F32), pltpu.VMEM((384, 8, LANE), F32), square, square, pltpu.VMEM(w_in.shape, F32), pltpu.VMEM(w_out.shape, F32), dma(6)],
            compiler_params=big, name="table_grad",
        )(codes, grad_tgt, pos, loss_row, cid_rows, dcand, tiles, hc)
        loss = loss.reshape(())
        return loss, grad_blk, grad_w_in, grad_w_out

    return jax.shard_map(local_step, mesh=mesh, in_specs=(P("dp", None), P(), P(), P("dp", None), P(), P(), P("dp")), out_specs=(P(), P("dp", None), P(), P()), check_vma=False)
```

```python
import functools
import jax
import jax.numpy as jnp
from jax import lax
from jax.experimental import pallas as pl
from jax.experimental.pallas import tpu as pltpu
from jax.sharding import PartitionSpec as P

MESH = pl.DeviceIdType.MESH
F32, BF16 = jnp.float32, jnp.bfloat16
COORD = {"core": (1, 2), "x": (2, 4), "y": (8, 4), "z": (32, 4)}
ORDERS = (("x", "y", "z"), ("y", "z", "x"), ("z", "x", "y"))
NDEV = 128
NPEER = 10
LANE, TOK, ALL, KILO, WIDE = 128, 64, 8192, 1024, 256
HALF, SUB = 192, 32


def one(i):
    return pl.ds(i, 1)


def repeat(n, body, unroll=1):
    lax.fori_loop(0, n, body, 0, unroll=unroll)


def down(v):
    return jnp.sum(v, axis=0, keepdims=True)


def across(v):
    return jnp.sum(v, axis=1, keepdims=True)


def peak(v):
    return jnp.max(v, axis=0, keepdims=True)


def flag(mask):
    return jnp.where(mask, 1.0, 0.0)


def iota(shape, dim):
    return lax.broadcasted_iota(jnp.int32, shape, dim)


def coord(me, axis):
    stride, radix = COORD[axis]
    return (me // stride) % radix


def peer(me, axis, k):
    stride, radix = COORD[axis]
    c = coord(me, axis)
    return me + ((c + k) % radix - c) * stride


def block_index(me, order):
    idx, weight = 0, 1
    for axis in order:
        idx = idx + coord(me, axis) * weight
        weight *= COORD[axis][1]
    return idx


def greet(me):
    barrier = pltpu.get_barrier_semaphore()
    for axis in COORD:
        for k in range(1, COORD[axis][1]):
            pl.semaphore_signal(barrier, inc=1, device_id=(peer(me, axis, k),), device_id_type=MESH)
    return barrier


def remote(src, dst, send, recv, dev):
    return pltpu.make_async_remote_copy(src_ref=src, dst_ref=dst, send_sem=send, recv_sem=recv, device_id=(dev,), device_id_type=MESH)


def gather_streams(me, streams, bulk, send_sem, recv_sem, between=None, early=None):
    pending, sent = [None] * len(streams), []
    for phase in range(4):
        for s, (ref, off, unit, order) in enumerate(streams):
            if pending[s]:
                for c in pending[s]:
                    c.wait_recv()
            if phase == 3:
                if early and s == 3:
                    early()
                continue
            span = 4 ** phase
            idx = block_index(me, order)
            where = ref.at[pl.ds(off + (idx - idx % span) * unit, span * unit)]
            pending[s] = []
            for k in range(1, 4):
                n = s * 9 + phase * 3 + k - 1
                c = remote(where, where, send_sem.at[n], recv_sem.at[n], peer(me, order[phase], k))
                c.start()
                pending[s].append(c)
                sent.append(c)
        if between and phase < 3:
            between(phase)
    last = []
    for i, (ref, count) in enumerate(bulk):
        n = len(streams) * 9 + i
        where = ref.at[pl.ds(coord(me, "core") * count, count)]
        c = remote(where, where, send_sem.at[n], recv_sem.at[n], peer(me, "core", 1))
        c.start()
        last.append(c)
    if between:
        between(3)
    for c in last:
        c.wait_recv()
    return sent + last


def add_rows(ref, start, rref, base, count, parts):
    def add(i, carry):
        acc = ref[start + i]
        for k in range(parts):
            acc = acc + rref[base + k * count + i]
        ref[start + i] = acc
        return carry

    lax.fori_loop(0, count, add, 0, unroll=4)


class Scatter:
    def __init__(self, me, ref, first, rref, rbase, streams, send_sem, recv_sem):
        self.me, self.ref, self.first, self.rref, self.rbase = me, ref, first, rref, rbase
        self.streams, self.sems = streams, (send_sem, recv_sem)
        self.step, self.pending, self.sent = [0] * 3, [None] * 3, []

    def send(self, s):
        off, unit, order = self.streams[s]
        step, me = self.step[s], self.me
        span = 4 ** (2 - step)
        axis = order[2 - step]
        idx = block_index(me, order)
        start = self.first + off + (idx - idx % (4 * span)) * unit
        d = coord(me, axis)
        copies = []
        for k in range(1, 4):
            n = s * 9 + step * 3 + k - 1
            src = self.ref.at[pl.ds(start + (d + k) % 4 * span * unit, span * unit)]
            dst = self.rref.at[pl.ds(self.rbase + (k - 1) * span * unit, span * unit)]
            c = remote(src, dst, self.sems[0].at[n], self.sems[1].at[n], peer(me, axis, k))
            c.start()
            copies.append(c)
        self.sent += copies
        self.pending[s] = (copies, start + d * span * unit, self.rbase, span * unit)
        self.rbase += 3 * span * unit
        self.step[s] += 1

    def receive(self, s):
        copies, start, base, count = self.pending[s]
        for c in copies:
            c.wait_recv()
        add_rows(self.ref, start, self.rref, base, count, 3)

    def rest(self):
        for step in range(3):
            for s in range(3):
                self.receive(s)
                if step < 2:
                    self.send(s)


def gelu_parts(a):
    c = 0.7978845608028654
    inner = jnp.tanh(c * (a + 0.044715 * (a * a * a)))
    half = 0.5 * (1.0 + inner)
    return a * half, half + 0.5 * a * (1.0 - inner * inner) * (c * (1.0 + 3.0 * 0.044715 * (a * a)))


def nt_dot(a, b):
    return lax.dot_general(a, b, (((1,), (1,)), ((), ())), preferred_element_type=F32)


def tn_dot(a, b):
    return lax.dot_general(a, b, (((0,), (0,)), ((), ())), preferred_element_type=F32)


H_OFF = (0, HALF, 384)
H_UNIT = (3, 3, 2)
H_FIRST = (0, 3, 6)


def column(row):
    return jnp.transpose(jnp.broadcast_to(row, (LANE, LANE)))


def query_kernel(x_hbm, win_hbm, wout_hbm, tgt_ref, blk_ref, cid_ref, logq_ref, tok_ref, h_out, pre_out, cand_out, candt_out, cidb_out, logqb_out,
                 tall_ref, square, x_ref, win_ref, wout_ref, blk, ids, lqs, rows, h_ref, pre_ref, cand_ref, candt_ref, cidb_ref, logqb_ref, load_sem, out_sem, send_sem, recv_sem):
    me = lax.axis_index("dp")
    mine = pl.ds(pl.multiple_of(me * 8, 8), 8)
    loads = [
        pltpu.make_async_copy(cid_ref.at[mine], ids, load_sem.at[0]), pltpu.make_async_copy(logq_ref.at[mine], lqs, load_sem.at[1]),
        pltpu.make_async_copy(blk_ref, blk, load_sem.at[2])]
    tower = [pltpu.make_async_copy(a, b, load_sem.at[3 + i]) for i, (a, b) in enumerate([(x_hbm, x_ref), (win_hbm, win_ref), (wout_hbm, wout_ref)])]
    for c in tower + loads:
        c.start()
    barrier = greet(me)
    for c in tower:
        c.wait()
    pre = jnp.dot(x_ref[...], win_ref[...], preferred_element_type=F32)
    pre_ref[0] = pre[:, :PART]
    pre_ref[1] = pre[:, PART:]
    act = gelu_parts(pre)[0].astype(BF16)
    query = jnp.dot(act, wout_ref[...], preferred_element_type=F32)
    core = coord(me, "core")
    streams = []
    for s in range(3):
        idx = block_index(me, ORDERS[s])
        for g in range(H_UNIT[s]):
            row = 8 * (H_FIRST[s] + g)
            h_ref[core * 512 + H_OFF[s] + idx * H_UNIT[s] + g] = query[row : row + 8, :].astype(BF16)
        streams.append((h_ref, core * 512 + H_OFF[s], H_UNIT[s], ORDERS[s]))
    streams.append((tall_ref, core * TOK, 1, ORDERS[2]))
    tall_ref[core * TOK + block_index(me, ORDERS[2])] = tgt_ref[...]
    lane = iota((1, LANE), 1)
    pl.semaphore_wait(barrier, NPEER)

    def pick(n, carry):
        part = pl.ds(pl.multiple_of(n // 8 * WIDE, WIDE), WIDE)
        first = n % 8 * KILO
        want = cidb_ref[part, :]
        picks = [flag(want == (lane + (first + u * LANE)).astype(F32)).astype(BF16) for u in range(8)]
        rows[part, :] += jnp.dot(jnp.concatenate(picks, axis=1), blk[pl.ds(pl.multiple_of(first, KILO), KILO), :], preferred_element_type=F32)
        return carry

    def fill(phase):
        if phase == 0:
            for c in loads:
                c.wait()
            for c in range(8):
                at = slice(c * LANE, c * LANE + LANE)
                cidb_ref[at, :] = column((ids[c : c + 1, :] - me * ALL).astype(F32))
                logqb_ref[at, :] = column(lqs[c : c + 1, :])
            rows[...] = jnp.zeros_like(rows)
        bounds = (0, 8, 17, SUB, SUB)
        lax.fori_loop(bounds[phase], bounds[phase + 1], pick, 0)
        if phase == 2:
            cand_ref[...] = rows[...].astype(BF16)
            candt_ref[...] = jnp.transpose(rows[...]).astype(BF16)
            for c in outs:
                c.start()
        if phase == 3:
            half(core).start()
            swap.wait_recv()
            arrange(tall_ref, square, tok_ref)

    outs = [
        pltpu.make_async_copy(a, b, out_sem.at[i]) for i, (a, b) in enumerate([
            (pre_ref, pre_out), (cand_ref, cand_out), (candt_ref, candt_out), (cidb_ref, cidb_out), (logqb_ref, logqb_out)])]

    def half(c):
        where = pl.ds(c * 512, 512)
        return pltpu.make_async_copy(h_ref.at[where], h_out.at[where], out_sem.at[5 + c])

    where = tall_ref.at[pl.ds(core * TOK, TOK)]
    swap = remote(where, where, send_sem.at[39], recv_sem.at[39], peer(me, "core", 1))

    sent = gather_streams(me, streams, [(h_ref, 512)], send_sem, recv_sem, fill, swap.start) + [swap]
    half(1 - core).start()
    for c in outs:
        c.wait()
    for c in sent:
        c.wait_send()
    half(core).wait()
    half(1 - core).wait()


class Stats:
    def __init__(self, me, recv, cur, send_sem, recv_sem):
        self.me, self.recv, self.cur, self.sems = me, recv, cur, (send_sem, recv_sem)
        self.phase, self.pending, self.sent = [0] * 3, [None] * 3, []

    def send(self, s):
        phase, g0, ng = self.phase[s], H_FIRST[s], H_UNIT[s]
        axis = (ORDERS[s] + ("core",))[phase]
        src = self.cur.at[pl.ds(8 * phase + g0, ng)]
        self.pending[s] = []
        for k in range(1, COORD[axis][1]):
            n = s * NPEER + phase * 3 + k - 1
            dst = self.recv.at[pl.ds(8 * (3 * phase + k - 1) + g0, ng)]
            c = remote(src, dst, self.sems[0].at[n], self.sems[1].at[n], peer(self.me, axis, k))
            c.start()
            self.pending[s].append(c)
        self.sent += self.pending[s]

    def receive(self, s):
        phase, cur, recv, npart = self.phase[s], self.cur, self.recv, len(self.pending[s])
        for c in self.pending[s]:
            c.wait_recv()

        def merge(g, carry):
            old = cur[8 * phase + g]
            parts = [recv[8 * (3 * phase + k) + g] for k in range(npart)]
            top, z = old[0], old[2]
            for p in parts:
                top = jnp.maximum(top, p[0])
                z = jnp.maximum(z, p[2])
            total = old[1] * jnp.exp(old[0] - top)
            for p in parts:
                total = total + p[1] * jnp.exp(p[0] - top)
            row = 8 * (phase + 1) + g
            cur[row, 0] = top
            cur[row, 1] = total
            cur[row, 2] = z
            return carry

        lax.fori_loop(H_FIRST[s], H_FIRST[s] + H_UNIT[s], merge, 0)
        self.phase[s] += 1

    def advance(self, s):
        self.receive(s)
        self.send(s)


def arrange(tall_ref, square, tok_ref):
    def row(b, carry):
        square[one(b), :] = tall_ref[b]
        return carry

    repeat(LANE, row)
    ids = square[...]
    pieces = jnp.concatenate([lax.shift_right_logical(ids, 14), lax.shift_right_logical(ids, 7) & 127, ids & 127], axis=0).astype(F32).astype(BF16)
    b = iota((LANE, 1), 0)
    bt = iota((1, LANE), 1)

    def place(v, s):
        c = [lax.shift_right_logical(v, n) & 3 for n in (0, 2, 4)]
        z, x, y = c
        first, second, third = ((x, y, z), (y, z, x), (z, x, y))[s]
        return (v & TOK) + first + 4 * second + 16 * third

    for s in range(3):
        width, per = 8 * H_UNIT[s], (16, 16, 8)[s]
        span = width * per
        pick = iota((TOK, span), 0) == iota((TOK, span), 1) % width + 8 * H_FIRST[s]
        lanes = jnp.dot(pieces, flag(pick).astype(BF16), preferred_element_type=F32)
        mask = place(b, s) % per == iota((LANE, span), 1) // width
        group = flag(place(bt, s) // per == iota((LANE // per, LANE), 0)).astype(BF16)
        got = [
            jnp.dot(group, jnp.where(mask, lanes[LANE * p : LANE * p + LANE, :], 0.0).astype(BF16), preferred_element_type=F32).astype(jnp.int32)
            for p in range(3)]
        full = (got[0] * LANE + got[1]) * LANE + got[2]
        rows = span // LANE
        for a in range(LANE // per):
            half, rest = divmod(a, TOK // per)
            for r in range(rows):
                at = SUB * half + H_OFF[s] // 16 + rest * rows + r
                tok_ref[at : at + 1, :] = full[a : a + 1, LANE * r : LANE * r + LANE]


def target_kernel(tgt_ref, h_hbm, blk_hbm, zst_ref, pos_ref, code_ref, local_ref, hc_ref, te_out, h_ref, blk_ref, te_ref, zd, hs, es, codes, load_sem, sem):
    block_rows = blk_ref.shape[0]
    loads = [pltpu.make_async_copy(h_hbm, h_ref, load_sem.at[0]), pltpu.make_async_copy(blk_hbm, blk_ref, load_sem.at[1])]
    for c in loads:
        c.start()
    rel = tgt_ref[...] - lax.axis_index("dp") * block_rows
    local_ref[...] = rel.astype(F32)
    own = (rel >= 0) & (rel < block_rows)
    own_f = flag(own)
    own_b = own_f.astype(BF16)
    up = iota((LANE, LANE), 0) < iota((LANE, LANE), 1)
    prefix = jnp.dot(own_b, flag(up).astype(BF16), preferred_element_type=F32)
    total = jnp.dot(own_b, jnp.ones((LANE, LANE), BF16), preferred_element_type=F32)
    low = iota((TOK, TOK), 0) > iota((TOK, TOK), 1)
    offset = jnp.dot(flag(low).astype(BF16), total.astype(BF16), preferred_element_type=F32)
    pos_ref[...] = jnp.where(own, prefix + offset, -1.0)
    zd[...] = jnp.zeros_like(zd)

    def clear(i, carry):
        te_ref[pl.ds(pl.multiple_of(i * LANE, LANE), LANE), :] = jnp.zeros((LANE, LANE), F32)
        return carry

    repeat(TOK, clear)
    count = jnp.sum(own_f).astype(jnp.int32)
    slot0 = iota((LANE, LANE), 0).astype(F32)
    lane = iota((1, LANE), 1)
    sub = iota((16, LANE), 0)

    def one_row(ref, i):
        tile = ref[pl.ds(pl.multiple_of(i & -16, 16), 16), :].astype(F32)
        return down(jnp.where(sub == (i & 15), tile, 0.0))

    def compact(c, carry):
        slot = slot0 + (c * LANE).astype(F32)

        def collect(r, code):
            mark = (tgt_ref[one(r), :] % block_rows) * ALL + (lane + r * LANE)
            return code + jnp.where(pos_ref[one(r), :] == slot, mark, 0)

        code = lax.fori_loop(0, TOK, collect, jnp.zeros((LANE, LANE), jnp.int32), unroll=8)
        row = across((code // ALL).astype(F32))
        tok = across((code % ALL).astype(F32))
        both = row.astype(jnp.int32) * ALL + tok.astype(jnp.int32)
        code_ref[one(c), :] = jnp.transpose(jnp.broadcast_to(both, (LANE, LANE)))[0:1, :]
        return carry

    chunks = (count + 127) // LANE
    repeat(chunks, compact)
    copy = pltpu.make_async_copy(code_ref, codes, sem)
    copy.start()
    for c in loads:
        c.wait()
    copy.wait()

    def chunk(c, carry):
        slot = slot0 + (c * LANE).astype(F32)
        left = count - c * LANE

        def fetch(i, carry2):
            for u in range(8):
                n = i * 8 + u
                v = codes[c, n]
                tok, at = v & (ALL - 1), lax.shift_right_logical(v, 13)
                hs[one(n), :] = one_row(h_ref, tok)
                row = one_row(blk_ref, at)
                es[one(n), :] = row
                te_ref[one(jnp.where(n < left, tok, ALL)), :] = row
            return carry2

        repeat((jnp.minimum(left, LANE) + 7) // 8, fetch)
        keep = pltpu.make_async_copy(hs, hc_ref.at[pl.ds(pl.multiple_of(c * LANE, LANE), LANE)], load_sem.at[3])
        keep.start()
        z = jnp.broadcast_to(across(hs[...] * es[...]), (LANE, LANE))

        def spread(r, carry2):
            hit = pos_ref[one(r), :] == slot
            zd[one(r), :] += down(jnp.where(hit, z, 0.0))
            return carry2

        repeat(TOK, spread, 8)
        keep.wait()
        return carry

    repeat(chunks, chunk)
    copy = pltpu.make_async_copy(te_ref.at[pl.ds(0, ALL)], te_out, load_sem.at[2])
    copy.start()
    zst_ref[...] = jnp.where(pos_ref[...] >= 0.0, zd[...], -jnp.inf)
    copy.wait()


def table_kernel(code_ref, g_ref, pos_ref, lossrow_ref, cid_hbm, dcand_hbm, tiles_hbm, hc_ref, de_ref, dwin_out, dwout_out, loss_ref, cidx, dcand, whole, hc, gh, dwin_ref, dwout_ref, sem):
    me = lax.axis_index("dp")
    loads = [pltpu.make_async_copy(cid_hbm.at[pl.ds(pl.multiple_of(me * 8, 8), 8)], cidx, sem.at[3]), pltpu.make_async_copy(dcand_hbm, dcand, sem.at[0]), pltpu.make_async_copy(tiles_hbm, whole, sem.at[1])]
    for c in loads:
        c.start()
    loss_ref[0, 0] = jnp.max(lossrow_ref[...])

    def clear(i, carry):
        de_ref[pl.ds(pl.multiple_of(i * LANE, LANE), LANE), :] = jnp.zeros((LANE, LANE), F32)
        return carry

    repeat(de_ref.shape[0] // LANE, clear)
    for c in loads[:2]:
        c.wait()
    base = me * ALL

    def place(i, carry):
        for u in range(SUB):
            de_ref[one(cidx[lax.shift_right_logical(i, 2), (i & 3) * SUB + u] - base), :] = dcand[one(i * SUB + u), :]
        return carry

    repeat(SUB, place)
    loads[-1].wait()
    for half in range(2):
        base = HALF * half
        dwout_ref[PART * half : PART * half + PART, :] = whole[base : base + TOK].reshape(PART, LANE)
        for j in range(4):
            at = base + TOK + SUB * j
            col = PART * half + LANE * j
            dwin_ref[:, col : col + LANE] = whole[at : at + SUB].reshape(WIDE, LANE)
    outs = [pltpu.make_async_copy(dwin_ref, dwin_out, sem.at[4]), pltpu.make_async_copy(dwout_ref, dwout_out, sem.at[5])]
    for c in outs:
        c.start()
    count = jnp.sum(flag(pos_ref[...] >= 0.0)).astype(jnp.int32)
    slot0 = iota((LANE, LANE), 0).astype(F32)

    def chunk(c, carry):
        slot = slot0 + (c * LANE).astype(F32)
        copy = pltpu.make_async_copy(hc_ref.at[pl.ds(pl.multiple_of(c * LANE, LANE), LANE)], hc, sem.at[2])
        copy.start()

        def collect(r, acc):
            return acc + jnp.where(pos_ref[one(r), :] == slot, g_ref[one(r), :], 0.0)

        g = jnp.sum(lax.fori_loop(0, TOK, collect, jnp.zeros((LANE, LANE), F32), unroll=8), axis=1, keepdims=True)
        copy.wait()
        gh[...] = g * hc[...]

        def put(i, carry2):
            de_ref[one(lax.shift_right_logical(code_ref[c, i], 13)), :] += gh[one(i), :]
            return carry2

        repeat(jnp.minimum(count - c * LANE, LANE), put)
        return carry

    repeat((count + 127) // LANE, chunk)
    for c in outs:
        c.wait()


LAST = 27
PART = 512


def grad_kernel(local, zst_ref, h_hbm, cand_hbm, cidb_hbm, logqb_hbm, candt_hbm, te_hbm, x_hbm, wout_hbm, pre_hbm, g_ref, loss_ref, tiles_out, dcand_out,
                ebuf, mc_ref, part, total, srecv, cur, norm, acc, recv, tiles, trecv, whole, dcand_ref,
                h_ref, cand_ref, cidb, logqb, candt_ref, te_ref, x_ref, wout_ref, pre_ref, xp_ref, prep_ref, dh_ref, dhp_ref,
                load_sem, core_send, core_recv, send_sem, recv_sem):
    me = lax.axis_index("dp")
    core = coord(me, "core")
    loads = [
        pltpu.make_async_copy(a, b, load_sem.at[i]) for i, (a, b) in enumerate([
            (cand_hbm, cand_ref), (cidb_hbm, cidb), (logqb_hbm, logqb), (h_hbm, h_ref),
            (candt_hbm, candt_ref), (te_hbm, te_ref), (x_hbm, x_ref), (wout_hbm, wout_ref), (pre_hbm, pre_ref)])]
    for c in loads:
        c.start()
    barrier = greet(me)
    for g in range(8):
        for half in range(2):
            cur[g, 2, 4 * half : 4 * half + 4, :] = zst_ref[SUB * half + 4 * g : SUB * half + 4 * g + 4, :]
    for c in loads[:4]:
        c.wait()

    def score(t, carry):
        for j in range(2):
            dots = nt_dot(cand_ref[...], h_ref[pl.ds(pl.multiple_of(t * PART + WIDE * j, WIDE), WIDE), :])
            for half in range(2):
                q = 2 * j + half
                r = t * 4 + q
                tgt = local[one(r), :]
                for c in range(8):
                    rows = slice(LANE * c, LANE * c + LANE)
                    s = dots[rows, LANE * half : LANE * half + LANE] - logqb[rows, :]
                    s = jnp.where(cidb[rows, :] == tgt, -1e9, s)
                    m = peak(s)
                    e = jnp.exp(s - m)
                    ebuf[t, rows, LANE * q : LANE * q + LANE] = e
                    mc_ref[r, c : c + 1, :] = m
                    part[q, c : c + 1, :] = down(e)
                most = mc_ref[r]
                top = peak(most)
                row = one(t // 8 * 4 + q)
                cur[t % 8, 0, row, :] = top
                cur[t % 8, 1, row, :] = down(part[q] * jnp.exp(most - top))
        return carry

    def part_loop(s, base, body):
        lax.fori_loop(base + H_FIRST[s], base + H_FIRST[s] + H_UNIT[s], body, 0)

    def score_part(s):
        part_loop(s, 0, score)
        part_loop(s, 8, score)

    def finish(s):
        stats.receive(s)

        def norms(g, carry):
            m, t, z = cur[SUB + g, 0], cur[SUB + g, 1], cur[SUB + g, 2]
            top = jnp.maximum(m, z)
            log_norm = top + jnp.log(t * jnp.exp(m - top) + jnp.exp(z - top))
            grad = (jnp.exp(z - log_norm) - 1.0) / ALL
            total[...] += log_norm - z
            for half in range(2):
                rows = pl.ds(SUB * half + 4 * g, 4)
                norm[rows, :] = log_norm[4 * half : 4 * half + 4, :]
                g_ref[rows, :] = grad[4 * half : 4 * half + 4, :]
            return carry

        part_loop(s, 0, norms)

    total[...] = jnp.zeros_like(total)

    def probs(t):
        blocks = []
        for q in range(4):
            r = t * 4 + q
            scale = jnp.exp(mc_ref[r] - norm[one(r), :]) / ALL
            blocks.append(jnp.concatenate([
                (ebuf[t, LANE * c : LANE * c + LANE, LANE * q : LANE * q + LANE] * scale[c : c + 1, :]).astype(BF16) for c in range(8)], axis=0))
        return jnp.concatenate(blocks, axis=1)

    def query_grad(t):
        dqt = jnp.dot(candt_ref[...], probs(t), preferred_element_type=F32)
        gcol = jnp.concatenate([column(g_ref[one(t * 4 + q), :]) for q in range(4)], axis=0)
        dq = jnp.transpose(dqt) + gcol * te_ref[pl.ds(pl.multiple_of(t * PART, PART), PART), :]
        return dq.reshape(TOK, 8, LANE)

    def swap(i):
        return remote(acc.at[pl.ds(((1 - core) * 8 + i) * TOK, TOK)], recv.at[pl.ds(i * TOK, TOK)], core_send.at[i], core_recv.at[i], peer(me, "core", 1))

    def give(i, carry):
        t = (1 - core) * 8 + i
        acc[pl.ds(t * TOK, TOK)] = query_grad(t)
        swap(i).start()
        return carry

    def keep(i, carry):
        t = core * 8 + i
        val = query_grad(t)
        swap(i).wait_recv()
        acc[pl.ds(t * TOK, TOK)] = val + recv[pl.ds(i * TOK, TOK)]
        return carry

    def cand_grad():
        dcand_ref[...] = jnp.zeros_like(dcand_ref)

        def accumulate(t, carry):
            dcand_ref[...] += jnp.dot(probs(t), h_ref[pl.ds(pl.multiple_of(t * PART, PART), PART), :], preferred_element_type=F32)
            return carry

        repeat(16, accumulate)
        dcand_copy.start()

    dcand_copy = pltpu.make_async_copy(dcand_ref, dcand_out, load_sem.at[9])
    streams = [(H_OFF[s], H_UNIT[s], ORDERS[s]) for s in range(3)]
    scatter = Scatter(me, acc, core * 512, recv, 512, streams, send_sem.at[0], recv_sem.at[0])
    stats = Stats(me, srecv, cur, send_sem.at[3], recv_sem.at[3])
    a, b, c = range(3)

    def to_partner(src, dst, n):
        return remote(src, dst, send_sem.at[n, LAST + 1], recv_sem.at[n, LAST + 1], peer(me, "core", 1))

    give_x, give_pre = to_partner(x_ref, xp_ref, 0), to_partner(pre_ref.at[1 - core], prep_ref, 1)

    def keep_part(s):
        part_loop(s, 0, keep)
        scatter.send(s)

    score_part(a)
    pl.semaphore_wait(barrier, NPEER)
    stats.send(a)
    score_part(b)
    stats.advance(a)
    stats.send(b)
    score_part(c)
    stats.advance(a)
    stats.advance(b)
    stats.send(c)
    for s in (a, b, c):
        stats.advance(s)
    finish(a)
    for load in loads[4:]:
        load.wait()
    give_x.start()
    give_pre.start()
    part_loop(a, 0, give)
    stats.advance(b)
    stats.advance(c)
    keep_part(a)
    finish(b)
    part_loop(b, 0, give)
    stats.advance(c)
    keep_part(b)
    finish(c)
    part_loop(c, 0, give)
    keep_part(c)
    give_x.wait_recv()
    give_pre.wait_recv()
    loss_ref[...] = jnp.broadcast_to(jnp.sum(total[...], keepdims=True) / ALL, loss_ref.shape)
    cand_grad()
    scatter.rest()
    sent = stats.sent + scatter.sent
    for s in range(3):
        idx = block_index(me, ORDERS[s])
        for g in range(H_UNIT[s]):
            dh_ref[H_FIRST[s] + g] = acc[core * 512 + H_OFF[s] + idx * H_UNIT[s] + g].astype(BF16)
    give_dh = to_partner(dh_ref, dhp_ref, 2)
    give_dh.start()
    act, slope = gelu_parts(jnp.concatenate([pre_ref[core], prep_ref[...]], axis=0))
    give_dh.wait_recv()
    dh = jnp.concatenate([dh_ref[...].reshape(TOK, LANE), dhp_ref[...].reshape(TOK, LANE)], axis=0)
    d_pre = (slope * nt_dot(dh, wout_ref[pl.ds(pl.multiple_of(core * PART, PART), PART), :])).astype(BF16)
    dw_out = tn_dot(act.astype(BF16), dh)
    mine = core * HALF
    tiles[pl.ds(mine, TOK)] = dw_out.reshape(TOK, 8, LANE)
    dw_in = tn_dot(jnp.concatenate([x_ref[...], xp_ref[...]], axis=0), d_pre)
    for j in range(4):
        tiles[pl.ds(mine + TOK + SUB * j, SUB)] = dw_in[:, LANE * j : LANE * j + LANE].reshape(SUB, 8, LANE)
    streams = [(TOK * s, 1, ORDERS[s]) for s in range(3)]
    sent += [give_x, give_pre, give_dh]
    scatter = Scatter(me, tiles, core * HALF, trecv, 0, streams, send_sem.at[1], recv_sem.at[1])
    for s in range(3):
        scatter.send(s)
    scatter.rest()
    sent += scatter.sent
    streams = []
    for s in range(3):
        own = core * HALF + TOK * s + block_index(me, ORDERS[s])
        whole[own] = tiles[own]
        streams.append((whole, core * HALF + TOK * s, 1, ORDERS[s]))
    def leave(c):
        where = pl.ds(c * HALF, HALF)
        return pltpu.make_async_copy(whole.at[where], tiles_out.at[where], load_sem.at[10 + c])

    def push(phase):
        if phase == 3:
            leave(core).start()

    sent += gather_streams(me, streams, [(whole, HALF)], send_sem.at[2], recv_sem.at[2], push)
    leave(1 - core).start()
    dcand_copy.wait()
    for c in sent:
        c.wait_send()

    def swap_done(i, carry):
        swap(i).wait_send()
        return carry

    repeat(8, swap_done)
    leave(core).wait()
    leave(1 - core).wait()


def vmem(n):
    return [pl.BlockSpec(memory_space=pltpu.VMEM)] * n


def params(cid):
    return pltpu.CompilerParams(collective_id=cid, has_side_effects=True, vmem_limit_bytes=63 * KILO * KILO)


def dma(*shape):
    return pltpu.SemaphoreType.DMA(shape)


def solution(mesh):
    num_dev = mesh.shape["dp"]

    def local_step(features, w_in, w_out, table_blk, cand_ids, log_q, targets):
        dev_index = lax.axis_index("dp")
        block_rows = table_blk.shape[0]
        cand_dev = cand_ids.shape[0] // num_dev
        tok_total = features.shape[0] * num_dev
        anyspec = pl.BlockSpec(memory_space=pl.ANY)
        cid_rows, logq_rows = cand_ids.reshape(KILO, LANE), log_q.reshape(KILO, LANE)
        tgt_all, h_all, pre, cand_rows, cand_t, cidb, logqb = pl.pallas_call(
            query_kernel,
            out_shape=[
                jax.ShapeDtypeStruct((TOK, LANE), jnp.int32), jax.ShapeDtypeStruct((KILO, 8, LANE), BF16), jax.ShapeDtypeStruct((2, TOK, PART), F32),
                jax.ShapeDtypeStruct((cand_dev, LANE), BF16), jax.ShapeDtypeStruct((LANE, cand_dev), BF16),
                jax.ShapeDtypeStruct((cand_dev, LANE), F32), jax.ShapeDtypeStruct((cand_dev, LANE), F32)],
            in_specs=[anyspec] * 3 + vmem(1) + [anyspec] * 3, out_specs=vmem(1) + [anyspec] * 6,
            scratch_shapes=[
                pltpu.VMEM((LANE, 1, TOK), jnp.int32), pltpu.VMEM((LANE, TOK), jnp.int32),
                pltpu.VMEM(features.shape, BF16), pltpu.VMEM(w_in.shape, BF16), pltpu.VMEM(w_out.shape, BF16),
                pltpu.VMEM((block_rows, LANE), BF16), pltpu.VMEM((8, LANE), jnp.int32), pltpu.VMEM((8, LANE), F32), pltpu.VMEM((cand_dev, LANE), F32),
                pltpu.VMEM((KILO, 8, LANE), BF16), pltpu.VMEM((2, TOK, PART), F32), pltpu.VMEM((cand_dev, LANE), BF16), pltpu.VMEM((LANE, cand_dev), BF16),
                pltpu.VMEM((cand_dev, LANE), F32), pltpu.VMEM((cand_dev, LANE), F32),
                dma(6), dma(7), dma(4 * NPEER), dma(4 * NPEER)],
            compiler_params=params(0), name="query_gather",
        )(features, w_in, w_out, targets[None, :], table_blk, cid_rows, logq_rows)
        query_all = h_all.reshape(ALL, LANE)
        smem = pl.BlockSpec(memory_space=pltpu.SMEM)
        square = pltpu.VMEM((LANE, LANE), F32)
        big = pltpu.CompilerParams(vmem_limit_bytes=63 * KILO * KILO)
        zst, pos, codes, local, hc, te = pl.pallas_call(
            target_kernel,
            out_shape=[
                jax.ShapeDtypeStruct((TOK, LANE), F32), jax.ShapeDtypeStruct((TOK, LANE), F32), jax.ShapeDtypeStruct((TOK, LANE), jnp.int32), jax.ShapeDtypeStruct((TOK, LANE), F32),
                jax.ShapeDtypeStruct((tok_total, LANE), F32), jax.ShapeDtypeStruct((tok_total, LANE), F32)],
            in_specs=vmem(1) + [anyspec] * 2, out_specs=vmem(4) + [anyspec] * 2,
            scratch_shapes=[
                pltpu.VMEM((tok_total, LANE), BF16), pltpu.VMEM((block_rows, LANE), BF16), pltpu.VMEM((tok_total + 8, LANE), F32), pltpu.VMEM((TOK, LANE), F32),
                square, square, pltpu.SMEM((TOK, LANE), jnp.int32), dma(4), pltpu.SemaphoreType.DMA],
            compiler_params=big, name="target_rows",
        )(tgt_all, query_all, table_blk)
        grad_tgt, loss_row, tiles, dcand = pl.pallas_call(
            grad_kernel,
            out_shape=[
                jax.ShapeDtypeStruct((TOK, LANE), F32), jax.ShapeDtypeStruct((8, LANE), F32),
                jax.ShapeDtypeStruct((384, 8, LANE), F32), jax.ShapeDtypeStruct((cand_dev, LANE), F32)],
            in_specs=vmem(2) + [anyspec] * 9, out_specs=vmem(2) + [anyspec] * 2,
            scratch_shapes=[
                pltpu.VMEM((16, cand_dev, PART), F32), pltpu.VMEM((TOK, 8, LANE), F32), pltpu.VMEM((4, 8, LANE), F32), pltpu.VMEM((8, LANE), F32),
                pltpu.VMEM((80, 3, 8, LANE), F32), pltpu.VMEM((40, 3, 8, LANE), F32), pltpu.VMEM((TOK, LANE), F32),
                pltpu.VMEM((KILO, 8, LANE), F32), pltpu.VMEM((KILO, 8, LANE), F32),
                pltpu.VMEM((384, 8, LANE), F32), pltpu.VMEM((384, 8, LANE), F32), pltpu.VMEM((384, 8, LANE), F32), pltpu.VMEM((cand_dev, LANE), F32),
                pltpu.VMEM((tok_total, LANE), BF16), pltpu.VMEM((cand_dev, LANE), BF16), pltpu.VMEM((cand_dev, LANE), F32), pltpu.VMEM((cand_dev, LANE), F32),
                pltpu.VMEM((LANE, cand_dev), BF16), pltpu.VMEM((tok_total, LANE), F32),
                pltpu.VMEM(features.shape, BF16), pltpu.VMEM(w_out.shape, BF16), pltpu.VMEM(pre.shape, F32),
                pltpu.VMEM(features.shape, BF16), pltpu.VMEM((TOK, PART), F32), pltpu.VMEM((8, 8, LANE), BF16), pltpu.VMEM((8, 8, LANE), BF16),
                dma(12), dma(8), dma(8), dma(4, 3 * NPEER), dma(4, 3 * NPEER)],
            compiler_params=params(1), name="grad_reduce",
        )(local, zst, query_all, cand_rows, cidb, logqb, cand_t, te, features, w_out, pre)
        grad_blk, grad_w_in, grad_w_out, loss = pl.pallas_call(
            table_kernel,
            out_shape=[
                jax.ShapeDtypeStruct((block_rows, LANE), F32), jax.ShapeDtypeStruct(w_in.shape, F32), jax.ShapeDtypeStruct(w_out.shape, F32),
                jax.ShapeDtypeStruct((1, 1), F32)],
            in_specs=[smem] + vmem(3) + [anyspec] * 4, out_specs=vmem(1) + [anyspec] * 2 + [smem],
            scratch_shapes=[pltpu.SMEM((8, LANE), jnp.int32), pltpu.VMEM((cand_dev, LANE), F32), pltpu.VMEM((384, 8, LANE), F32), square, square, pltpu.VMEM(w_in.shape, F32), pltpu.VMEM(w_out.shape, F32), dma(6)],
            compiler_params=big, name="table_grad",
        )(codes, grad_tgt, pos, loss_row, cid_rows, dcand, tiles, hc)
        loss = loss.reshape(())
        return loss, grad_blk, grad_w_in, grad_w_out

    return jax.shard_map(local_step, mesh=mesh, in_specs=(P("dp", None), P(), P(), P("dp", None), P(), P(), P("dp")), out_specs=(P(), P("dp", None), P(), P()), check_vma=False)
```

```python
import functools
import jax
import jax.numpy as jnp
from jax import lax
from jax.experimental import pallas as pl
from jax.experimental.pallas import tpu as pltpu
from jax.sharding import PartitionSpec as P

MESH = pl.DeviceIdType.MESH
F32, BF16 = jnp.float32, jnp.bfloat16
COORD = {"core": (1, 2), "x": (2, 4), "y": (8, 4), "z": (32, 4)}
ORDERS = (("x", "y", "z"), ("y", "z", "x"), ("z", "x", "y"))
NDEV = 128
NPEER = 10
LANE, TOK, ALL, KILO, WIDE = 128, 64, 8192, 1024, 256
HALF, SUB = 192, 32


def one(i):
    return pl.ds(i, 1)


def repeat(n, body, unroll=1):
    lax.fori_loop(0, n, body, 0, unroll=unroll)


def down(v):
    return jnp.sum(v, axis=0, keepdims=True)


def across(v):
    return jnp.sum(v, axis=1, keepdims=True)


def peak(v):
    return jnp.max(v, axis=0, keepdims=True)


def flag(mask):
    return jnp.where(mask, 1.0, 0.0)


def iota(shape, dim):
    return lax.broadcasted_iota(jnp.int32, shape, dim)


def coord(me, axis):
    stride, radix = COORD[axis]
    return (me // stride) % radix


def peer(me, axis, k):
    stride, radix = COORD[axis]
    c = coord(me, axis)
    return me + ((c + k) % radix - c) * stride


def block_index(me, order):
    idx, weight = 0, 1
    for axis in order:
        idx = idx + coord(me, axis) * weight
        weight *= COORD[axis][1]
    return idx


def greet(me):
    barrier = pltpu.get_barrier_semaphore()
    for axis in COORD:
        for k in range(1, COORD[axis][1]):
            pl.semaphore_signal(barrier, inc=1, device_id=(peer(me, axis, k),), device_id_type=MESH)
    return barrier


def remote(src, dst, send, recv, dev):
    return pltpu.make_async_remote_copy(src_ref=src, dst_ref=dst, send_sem=send, recv_sem=recv, device_id=(dev,), device_id_type=MESH)


def gather_streams(me, streams, bulk, send_sem, recv_sem, between=None, early=None):
    pending, sent = [None] * len(streams), []
    for phase in range(4):
        for s, (ref, off, unit, order) in enumerate(streams):
            if pending[s]:
                for c in pending[s]:
                    c.wait_recv()
            if phase == 3:
                if early and s == 3:
                    early()
                continue
            span = 4 ** phase
            idx = block_index(me, order)
            where = ref.at[pl.ds(off + (idx - idx % span) * unit, span * unit)]
            pending[s] = []
            for k in range(1, 4):
                n = s * 9 + phase * 3 + k - 1
                c = remote(where, where, send_sem.at[n], recv_sem.at[n], peer(me, order[phase], k))
                c.start()
                pending[s].append(c)
                sent.append(c)
        if between and phase < 3:
            between(phase)
    last = []
    for i, (ref, count) in enumerate(bulk):
        n = len(streams) * 9 + i
        where = ref.at[pl.ds(coord(me, "core") * count, count)]
        c = remote(where, where, send_sem.at[n], recv_sem.at[n], peer(me, "core", 1))
        c.start()
        last.append(c)
    if between:
        between(3)
    for c in last:
        c.wait_recv()
    return sent + last


def add_rows(ref, start, rref, base, count, parts):
    def add(i, carry):
        acc = ref[start + i]
        for k in range(parts):
            acc = acc + rref[base + k * count + i]
        ref[start + i] = acc
        return carry

    lax.fori_loop(0, count, add, 0, unroll=4)


class Scatter:
    def __init__(self, me, ref, first, rref, rbase, streams, send_sem, recv_sem):
        self.me, self.ref, self.first, self.rref, self.rbase = me, ref, first, rref, rbase
        self.streams, self.sems = streams, (send_sem, recv_sem)
        self.step, self.pending, self.sent = [0] * 3, [None] * 3, []

    def send(self, s):
        off, unit, order = self.streams[s]
        step, me = self.step[s], self.me
        span = 4 ** (2 - step)
        axis = order[2 - step]
        idx = block_index(me, order)
        start = self.first + off + (idx - idx % (4 * span)) * unit
        d = coord(me, axis)
        copies = []
        for k in range(1, 4):
            n = s * 9 + step * 3 + k - 1
            src = self.ref.at[pl.ds(start + (d + k) % 4 * span * unit, span * unit)]
            dst = self.rref.at[pl.ds(self.rbase + (k - 1) * span * unit, span * unit)]
            c = remote(src, dst, self.sems[0].at[n], self.sems[1].at[n], peer(me, axis, k))
            c.start()
            copies.append(c)
        self.sent += copies
        self.pending[s] = (copies, start + d * span * unit, self.rbase, span * unit)
        self.rbase += 3 * span * unit
        self.step[s] += 1

    def receive(self, s):
        copies, start, base, count = self.pending[s]
        for c in copies:
            c.wait_recv()
        add_rows(self.ref, start, self.rref, base, count, 3)

    def rest(self):
        for step in range(3):
            for s in range(3):
                self.receive(s)
                if step < 2:
                    self.send(s)


def gelu_parts(a):
    c = 0.7978845608028654
    inner = jnp.tanh(c * (a + 0.044715 * (a * a * a)))
    half = 0.5 * (1.0 + inner)
    return a * half, half + 0.5 * a * (1.0 - inner * inner) * (c * (1.0 + 3.0 * 0.044715 * (a * a)))


def nt_dot(a, b):
    return lax.dot_general(a, b, (((1,), (1,)), ((), ())), preferred_element_type=F32)


def tn_dot(a, b):
    return lax.dot_general(a, b, (((0,), (0,)), ((), ())), preferred_element_type=F32)


H_OFF = (0, HALF, 384)
H_UNIT = (3, 3, 2)
H_FIRST = (0, 3, 6)


def column(row):
    return jnp.transpose(jnp.broadcast_to(row, (LANE, LANE)))


def query_kernel(x_hbm, win_hbm, wout_hbm, tgt_ref, blk_ref, cid_ref, logq_ref, tok_ref, h_out, pre_out, cand_out, candt_out, cidb_out, logqb_out,
                 tall_ref, square, x_ref, win_ref, wout_ref, blk, ids, lqs, rows, h_ref, pre_ref, cand_ref, candt_ref, cidb_ref, logqb_ref, load_sem, out_sem, send_sem, recv_sem):
    me = lax.axis_index("dp")
    mine = pl.ds(pl.multiple_of(me * 8, 8), 8)
    loads = [
        pltpu.make_async_copy(cid_ref.at[mine], ids, load_sem.at[0]), pltpu.make_async_copy(logq_ref.at[mine], lqs, load_sem.at[1]),
        pltpu.make_async_copy(blk_ref, blk, load_sem.at[2])]
    tower = [pltpu.make_async_copy(a, b, load_sem.at[3 + i]) for i, (a, b) in enumerate([(x_hbm, x_ref), (win_hbm, win_ref), (wout_hbm, wout_ref)])]
    for c in tower + loads:
        c.start()
    barrier = greet(me)
    for c in tower:
        c.wait()
    pre = jnp.dot(x_ref[...], win_ref[...], preferred_element_type=F32)
    pre_ref[0] = pre[:, :PART]
    pre_ref[1] = pre[:, PART:]
    act = gelu_parts(pre)[0].astype(BF16)
    query = jnp.dot(act, wout_ref[...], preferred_element_type=F32)
    core = coord(me, "core")
    streams = []
    for s in range(3):
        idx = block_index(me, ORDERS[s])
        for g in range(H_UNIT[s]):
            row = 8 * (H_FIRST[s] + g)
            h_ref[core * 512 + H_OFF[s] + idx * H_UNIT[s] + g] = query[row : row + 8, :].astype(BF16)
        streams.append((h_ref, core * 512 + H_OFF[s], H_UNIT[s], ORDERS[s]))
    streams.append((tall_ref, core * TOK, 1, ORDERS[2]))
    tall_ref[core * TOK + block_index(me, ORDERS[2])] = tgt_ref[...]
    lane = iota((1, LANE), 1)
    pl.semaphore_wait(barrier, NPEER)

    def pick(n, carry):
        part = pl.ds(pl.multiple_of(n // 8 * WIDE, WIDE), WIDE)
        first = n % 8 * KILO
        want = cidb_ref[part, :]
        picks = [flag(want == (lane + (first + u * LANE)).astype(F32)).astype(BF16) for u in range(8)]
        rows[part, :] += jnp.dot(jnp.concatenate(picks, axis=1), blk[pl.ds(pl.multiple_of(first, KILO), KILO), :], preferred_element_type=F32)
        return carry

    def fill(phase):
        if phase == 0:
            for c in loads:
                c.wait()
            for c in range(8):
                at = slice(c * LANE, c * LANE + LANE)
                cidb_ref[at, :] = column((ids[c : c + 1, :] - me * ALL).astype(F32))
                logqb_ref[at, :] = column(lqs[c : c + 1, :])
            rows[...] = jnp.zeros_like(rows)
        bounds = (0, 8, 17, SUB, SUB)
        lax.fori_loop(bounds[phase], bounds[phase + 1], pick, 0)
        if phase == 2:
            cand_ref[...] = rows[...].astype(BF16)
            candt_ref[...] = jnp.transpose(rows[...]).astype(BF16)
            for c in outs:
                c.start()
        if phase == 3:
            half(core).start()
            swap.wait_recv()
            arrange(tall_ref, square, tok_ref)

    outs = [
        pltpu.make_async_copy(a, b, out_sem.at[i]) for i, (a, b) in enumerate([
            (pre_ref, pre_out), (cand_ref, cand_out), (candt_ref, candt_out), (cidb_ref, cidb_out), (logqb_ref, logqb_out)])]

    def half(c):
        where = pl.ds(c * 512, 512)
        return pltpu.make_async_copy(h_ref.at[where], h_out.at[where], out_sem.at[5 + c])

    where = tall_ref.at[pl.ds(core * TOK, TOK)]
    swap = remote(where, where, send_sem.at[39], recv_sem.at[39], peer(me, "core", 1))

    sent = gather_streams(me, streams, [(h_ref, 512)], send_sem, recv_sem, fill, swap.start) + [swap]
    half(1 - core).start()
    for c in outs:
        c.wait()
    for c in sent:
        c.wait_send()
    half(core).wait()
    half(1 - core).wait()


class Stats:
    def __init__(self, me, recv, cur, send_sem, recv_sem):
        self.me, self.recv, self.cur, self.sems = me, recv, cur, (send_sem, recv_sem)
        self.phase, self.pending, self.sent = [0] * 3, [None] * 3, []

    def send(self, s):
        phase, g0, ng = self.phase[s], H_FIRST[s], H_UNIT[s]
        axis = (ORDERS[s] + ("core",))[phase]
        src = self.cur.at[pl.ds(8 * phase + g0, ng)]
        self.pending[s] = []
        for k in range(1, COORD[axis][1]):
            n = s * NPEER + phase * 3 + k - 1
            dst = self.recv.at[pl.ds(8 * (3 * phase + k - 1) + g0, ng)]
            c = remote(src, dst, self.sems[0].at[n], self.sems[1].at[n], peer(self.me, axis, k))
            c.start()
            self.pending[s].append(c)
        self.sent += self.pending[s]

    def receive(self, s):
        phase, cur, recv, npart = self.phase[s], self.cur, self.recv, len(self.pending[s])
        for c in self.pending[s]:
            c.wait_recv()

        def merge(g, carry):
            old = cur[8 * phase + g]
            parts = [recv[8 * (3 * phase + k) + g] for k in range(npart)]
            top, z = old[0], old[2]
            for p in parts:
                top = jnp.maximum(top, p[0])
                z = jnp.maximum(z, p[2])
            total = old[1] * jnp.exp(old[0] - top)
            for p in parts:
                total = total + p[1] * jnp.exp(p[0] - top)
            row = 8 * (phase + 1) + g
            cur[row, 0] = top
            cur[row, 1] = total
            cur[row, 2] = z
            return carry

        lax.fori_loop(H_FIRST[s], H_FIRST[s] + H_UNIT[s], merge, 0)
        self.phase[s] += 1

    def advance(self, s):
        self.receive(s)
        self.send(s)


def arrange(tall_ref, square, tok_ref):
    def row(b, carry):
        square[one(b), :] = tall_ref[b]
        return carry

    repeat(LANE, row)
    ids = square[...]
    pieces = jnp.concatenate([lax.shift_right_logical(ids, 14), lax.shift_right_logical(ids, 7) & 127, ids & 127], axis=0).astype(F32).astype(BF16)
    b = iota((LANE, 1), 0)
    bt = iota((1, LANE), 1)

    def place(v, s):
        c = [lax.shift_right_logical(v, n) & 3 for n in (0, 2, 4)]
        z, x, y = c
        first, second, third = ((x, y, z), (y, z, x), (z, x, y))[s]
        return (v & TOK) + first + 4 * second + 16 * third

    for s in range(3):
        width, per = 8 * H_UNIT[s], (16, 16, 8)[s]
        span = width * per
        pick = iota((TOK, span), 0) == iota((TOK, span), 1) % width + 8 * H_FIRST[s]
        lanes = jnp.dot(pieces, flag(pick).astype(BF16), preferred_element_type=F32)
        mask = place(b, s) % per == iota((LANE, span), 1) // width
        group = flag(place(bt, s) // per == iota((LANE // per, LANE), 0)).astype(BF16)
        got = [
            jnp.dot(group, jnp.where(mask, lanes[LANE * p : LANE * p + LANE, :], 0.0).astype(BF16), preferred_element_type=F32).astype(jnp.int32)
            for p in range(3)]
        full = (got[0] * LANE + got[1]) * LANE + got[2]
        rows = span // LANE
        for a in range(LANE // per):
            half, rest = divmod(a, TOK // per)
            for r in range(rows):
                at = SUB * half + H_OFF[s] // 16 + rest * rows + r
                tok_ref[at : at + 1, :] = full[a : a + 1, LANE * r : LANE * r + LANE]


def target_kernel(tgt_ref, h_hbm, blk_hbm, zst_ref, pos_ref, code_ref, local_ref, hc_ref, te_out, h_ref, blk_ref, te_ref, zd, hs, es, codes, load_sem, sem):
    block_rows = blk_ref.shape[0]
    loads = [pltpu.make_async_copy(h_hbm, h_ref, load_sem.at[0]), pltpu.make_async_copy(blk_hbm, blk_ref, load_sem.at[1])]
    for c in loads:
        c.start()
    rel = tgt_ref[...] - lax.axis_index("dp") * block_rows
    local_ref[...] = rel.astype(F32)
    own = (rel >= 0) & (rel < block_rows)
    own_f = flag(own)
    own_b = own_f.astype(BF16)
    up = iota((LANE, LANE), 0) < iota((LANE, LANE), 1)
    prefix = jnp.dot(own_b, flag(up).astype(BF16), preferred_element_type=F32)
    total = jnp.dot(own_b, jnp.ones((LANE, LANE), BF16), preferred_element_type=F32)
    low = iota((TOK, TOK), 0) > iota((TOK, TOK), 1)
    offset = jnp.dot(flag(low).astype(BF16), total.astype(BF16), preferred_element_type=F32)
    pos_ref[...] = jnp.where(own, prefix + offset, -1.0)
    zd[...] = jnp.zeros_like(zd)

    def clear(i, carry):
        te_ref[pl.ds(pl.multiple_of(i * LANE, LANE), LANE), :] = jnp.zeros((LANE, LANE), F32)
        return carry

    repeat(TOK, clear)
    count = jnp.sum(own_f).astype(jnp.int32)
    slot0 = iota((LANE, LANE), 0).astype(F32)
    lane = iota((1, LANE), 1)
    sub = iota((16, LANE), 0)

    def one_row(ref, i):
        tile = ref[pl.ds(pl.multiple_of(i & -16, 16), 16), :].astype(F32)
        return down(jnp.where(sub == (i & 15), tile, 0.0))

    def compact(c, carry):
        slot = slot0 + (c * LANE).astype(F32)

        def collect(r, code):
            mark = (tgt_ref[one(r), :] % block_rows) * ALL + (lane + r * LANE)
            return code + jnp.where(pos_ref[one(r), :] == slot, mark, 0)

        code = lax.fori_loop(0, TOK, collect, jnp.zeros((LANE, LANE), jnp.int32), unroll=8)
        row = across((code // ALL).astype(F32))
        tok = across((code % ALL).astype(F32))
        both = row.astype(jnp.int32) * ALL + tok.astype(jnp.int32)
        code_ref[one(c), :] = jnp.transpose(jnp.broadcast_to(both, (LANE, LANE)))[0:1, :]
        return carry

    chunks = (count + 127) // LANE
    repeat(chunks, compact)
    copy = pltpu.make_async_copy(code_ref, codes, sem)
    copy.start()
    for c in loads:
        c.wait()
    copy.wait()

    def chunk(c, carry):
        slot = slot0 + (c * LANE).astype(F32)
        left = count - c * LANE

        def fetch(i, carry2):
            for u in range(8):
                n = i * 8 + u
                v = codes[c, n]
                tok, at = v & (ALL - 1), lax.shift_right_logical(v, 13)
                hs[one(n), :] = one_row(h_ref, tok)
                row = one_row(blk_ref, at)
                es[one(n), :] = row
                te_ref[one(jnp.where(n < left, tok, ALL)), :] = row
            return carry2

        repeat((jnp.minimum(left, LANE) + 7) // 8, fetch)
        keep = pltpu.make_async_copy(hs, hc_ref.at[pl.ds(pl.multiple_of(c * LANE, LANE), LANE)], load_sem.at[3])
        keep.start()
        z = jnp.broadcast_to(across(hs[...] * es[...]), (LANE, LANE))

        def spread(r, carry2):
            hit = pos_ref[one(r), :] == slot
            zd[one(r), :] += down(jnp.where(hit, z, 0.0))
            return carry2

        repeat(TOK, spread, 8)
        keep.wait()
        return carry

    repeat(chunks, chunk)
    copy = pltpu.make_async_copy(te_ref.at[pl.ds(0, ALL)], te_out, load_sem.at[2])
    copy.start()
    zst_ref[...] = jnp.where(pos_ref[...] >= 0.0, zd[...], -jnp.inf)
    copy.wait()


def table_kernel(code_ref, g_ref, pos_ref, lossrow_ref, cid_hbm, dcand_hbm, tiles_hbm, hc_ref, de_ref, dwin_out, dwout_out, loss_ref, cidx, dcand, whole, hc, gh, dwin_ref, dwout_ref, sem):
    me = lax.axis_index("dp")
    loads = [pltpu.make_async_copy(cid_hbm.at[pl.ds(pl.multiple_of(me * 8, 8), 8)], cidx, sem.at[3]), pltpu.make_async_copy(dcand_hbm, dcand, sem.at[0]), pltpu.make_async_copy(tiles_hbm, whole, sem.at[1])]
    for c in loads:
        c.start()
    loss_ref[0, 0] = jnp.max(lossrow_ref[...])

    def clear(i, carry):
        de_ref[pl.ds(pl.multiple_of(i * LANE, LANE), LANE), :] = jnp.zeros((LANE, LANE), F32)
        return carry

    repeat(de_ref.shape[0] // LANE, clear)
    for c in loads[:2]:
        c.wait()
    base = me * ALL

    def place(i, carry):
        for u in range(SUB):
            de_ref[one(cidx[lax.shift_right_logical(i, 2), (i & 3) * SUB + u] - base), :] = dcand[one(i * SUB + u), :]
        return carry

    repeat(SUB, place)
    loads[-1].wait()
    for half in range(2):
        base = HALF * half
        dwout_ref[PART * half : PART * half + PART, :] = whole[base : base + TOK].reshape(PART, LANE)
        for j in range(4):
            at = base + TOK + SUB * j
            col = PART * half + LANE * j
            dwin_ref[:, col : col + LANE] = whole[at : at + SUB].reshape(WIDE, LANE)
    outs = [pltpu.make_async_copy(dwin_ref, dwin_out, sem.at[4]), pltpu.make_async_copy(dwout_ref, dwout_out, sem.at[5])]
    for c in outs:
        c.start()
    count = jnp.sum(flag(pos_ref[...] >= 0.0)).astype(jnp.int32)
    slot0 = iota((LANE, LANE), 0).astype(F32)

    def chunk(c, carry):
        slot = slot0 + (c * LANE).astype(F32)
        copy = pltpu.make_async_copy(hc_ref.at[pl.ds(pl.multiple_of(c * LANE, LANE), LANE)], hc, sem.at[2])
        copy.start()

        def collect(r, acc):
            return acc + jnp.where(pos_ref[one(r), :] == slot, g_ref[one(r), :], 0.0)

        g = jnp.sum(lax.fori_loop(0, TOK, collect, jnp.zeros((LANE, LANE), F32), unroll=8), axis=1, keepdims=True)
        copy.wait()
        gh[...] = g * hc[...]

        def put(i, carry2):
            de_ref[one(lax.shift_right_logical(code_ref[c, i], 13)), :] += gh[one(i), :]
            return carry2

        repeat(jnp.minimum(count - c * LANE, LANE), put)
        return carry

    repeat((count + 127) // LANE, chunk)
    for c in outs:
        c.wait()


LAST = 27
PART = 512


def grad_kernel(local, zst_ref, h_hbm, cand_hbm, cidb_hbm, logqb_hbm, candt_hbm, te_hbm, x_hbm, wout_hbm, pre_hbm, g_ref, loss_ref, tiles_out, dcand_out,
                ebuf, mc_ref, part, total, srecv, cur, norm, acc, recv, tiles, trecv, whole, dcand_ref,
                h_ref, cand_ref, cidb, logqb, candt_ref, te_ref, x_ref, wout_ref, pre_ref, xp_ref, prep_ref, dh_ref, dhp_ref,
                load_sem, core_send, core_recv, send_sem, recv_sem):
    me = lax.axis_index("dp")
    core = coord(me, "core")
    loads = [
        pltpu.make_async_copy(a, b, load_sem.at[i]) for i, (a, b) in enumerate([
            (cand_hbm, cand_ref), (cidb_hbm, cidb), (logqb_hbm, logqb), (h_hbm, h_ref),
            (candt_hbm, candt_ref), (te_hbm, te_ref), (x_hbm, x_ref), (wout_hbm, wout_ref), (pre_hbm, pre_ref)])]
    for c in loads[:4]:
        c.start()
    barrier = greet(me)
    for g in range(8):
        for half in range(2):
            cur[g, 2, 4 * half : 4 * half + 4, :] = zst_ref[SUB * half + 4 * g : SUB * half + 4 * g + 4, :]
    for c in loads[:4]:
        c.wait()
    for c in loads[4:]:
        c.start()

    def score(t, carry):
        for j in range(2):
            dots = nt_dot(cand_ref[...], h_ref[pl.ds(pl.multiple_of(t * PART + WIDE * j, WIDE), WIDE), :])
            for half in range(2):
                q = 2 * j + half
                r = t * 4 + q
                tgt = local[one(r), :]
                for c in range(8):
                    rows = slice(LANE * c, LANE * c + LANE)
                    s = dots[rows, LANE * half : LANE * half + LANE] - logqb[rows, :]
                    s = jnp.where(cidb[rows, :] == tgt, -1e9, s)
                    m = peak(s)
                    e = jnp.exp(s - m)
                    ebuf[t, rows, LANE * q : LANE * q + LANE] = e
                    mc_ref[r, c : c + 1, :] = m
                    part[q, c : c + 1, :] = down(e)
                most = mc_ref[r]
                top = peak(most)
                row = one(t // 8 * 4 + q)
                cur[t % 8, 0, row, :] = top
                cur[t % 8, 1, row, :] = down(part[q] * jnp.exp(most - top))
        return carry

    def part_loop(s, base, body):
        lax.fori_loop(base + H_FIRST[s], base + H_FIRST[s] + H_UNIT[s], body, 0)

    def score_part(s):
        part_loop(s, 0, score)
        part_loop(s, 8, score)

    def finish(s):
        stats.receive(s)

        def norms(g, carry):
            m, t, z = cur[SUB + g, 0], cur[SUB + g, 1], cur[SUB + g, 2]
            top = jnp.maximum(m, z)
            log_norm = top + jnp.log(t * jnp.exp(m - top) + jnp.exp(z - top))
            grad = (jnp.exp(z - log_norm) - 1.0) / ALL
            total[...] += log_norm - z
            for half in range(2):
                rows = pl.ds(SUB * half + 4 * g, 4)
                norm[rows, :] = log_norm[4 * half : 4 * half + 4, :]
                g_ref[rows, :] = grad[4 * half : 4 * half + 4, :]
            return carry

        part_loop(s, 0, norms)

    total[...] = jnp.zeros_like(total)

    def probs(t):
        blocks = []
        for q in range(4):
            r = t * 4 + q
            scale = jnp.exp(mc_ref[r] - norm[one(r), :]) / ALL
            blocks.append(jnp.concatenate([
                (ebuf[t, LANE * c : LANE * c + LANE, LANE * q : LANE * q + LANE] * scale[c : c + 1, :]).astype(BF16) for c in range(8)], axis=0))
        return jnp.concatenate(blocks, axis=1)

    def query_grad(t):
        dqt = jnp.dot(candt_ref[...], probs(t), preferred_element_type=F32)
        gcol = jnp.concatenate([column(g_ref[one(t * 4 + q), :]) for q in range(4)], axis=0)
        dq = jnp.transpose(dqt) + gcol * te_ref[pl.ds(pl.multiple_of(t * PART, PART), PART), :]
        return dq.reshape(TOK, 8, LANE)

    def swap(i):
        return remote(acc.at[pl.ds(((1 - core) * 8 + i) * TOK, TOK)], recv.at[pl.ds(i * TOK, TOK)], core_send.at[i], core_recv.at[i], peer(me, "core", 1))

    def give(i, carry):
        t = (1 - core) * 8 + i
        acc[pl.ds(t * TOK, TOK)] = query_grad(t)
        swap(i).start()
        return carry

    def keep(i, carry):
        t = core * 8 + i
        val = query_grad(t)
        swap(i).wait_recv()
        acc[pl.ds(t * TOK, TOK)] = val + recv[pl.ds(i * TOK, TOK)]
        return carry

    def cand_grad():
        dcand_ref[...] = jnp.zeros_like(dcand_ref)

        def accumulate(t, carry):
            dcand_ref[...] += jnp.dot(probs(t), h_ref[pl.ds(pl.multiple_of(t * PART, PART), PART), :], preferred_element_type=F32)
            return carry

        repeat(16, accumulate)
        dcand_copy.start()

    dcand_copy = pltpu.make_async_copy(dcand_ref, dcand_out, load_sem.at[9])
    streams = [(H_OFF[s], H_UNIT[s], ORDERS[s]) for s in range(3)]
    scatter = Scatter(me, acc, core * 512, recv, 512, streams, send_sem.at[0], recv_sem.at[0])
    stats = Stats(me, srecv, cur, send_sem.at[3], recv_sem.at[3])
    a, b, c = range(3)

    def to_partner(src, dst, n):
        return remote(src, dst, send_sem.at[n, LAST + 1], recv_sem.at[n, LAST + 1], peer(me, "core", 1))

    give_x, give_pre = to_partner(x_ref, xp_ref, 0), to_partner(pre_ref.at[1 - core], prep_ref, 1)

    def keep_part(s):
        part_loop(s, 0, keep)
        scatter.send(s)

    score_part(a)
    pl.semaphore_wait(barrier, NPEER)
    stats.send(a)
    score_part(b)
    stats.advance(a)
    stats.send(b)
    score_part(c)
    stats.advance(a)
    stats.advance(b)
    stats.send(c)
    for s in (a, b, c):
        stats.advance(s)
    finish(a)
    for load in loads[4:]:
        load.wait()
    give_x.start()
    give_pre.start()
    part_loop(a, 0, give)
    stats.advance(b)
    stats.advance(c)
    keep_part(a)
    finish(b)
    part_loop(b, 0, give)
    stats.advance(c)
    keep_part(b)
    finish(c)
    part_loop(c, 0, give)
    keep_part(c)
    give_x.wait_recv()
    give_pre.wait_recv()
    loss_ref[...] = jnp.broadcast_to(jnp.sum(total[...], keepdims=True) / ALL, loss_ref.shape)
    cand_grad()
    scatter.rest()
    sent = stats.sent + scatter.sent
    for s in range(3):
        idx = block_index(me, ORDERS[s])
        for g in range(H_UNIT[s]):
            dh_ref[H_FIRST[s] + g] = acc[core * 512 + H_OFF[s] + idx * H_UNIT[s] + g].astype(BF16)
    give_dh = to_partner(dh_ref, dhp_ref, 2)
    give_dh.start()
    act, slope = gelu_parts(jnp.concatenate([pre_ref[core], prep_ref[...]], axis=0))
    give_dh.wait_recv()
    dh = jnp.concatenate([dh_ref[...].reshape(TOK, LANE), dhp_ref[...].reshape(TOK, LANE)], axis=0)
    d_pre = (slope * nt_dot(dh, wout_ref[pl.ds(pl.multiple_of(core * PART, PART), PART), :])).astype(BF16)
    dw_out = tn_dot(act.astype(BF16), dh)
    mine = core * HALF
    tiles[pl.ds(mine, TOK)] = dw_out.reshape(TOK, 8, LANE)
    dw_in = tn_dot(jnp.concatenate([x_ref[...], xp_ref[...]], axis=0), d_pre)
    for j in range(4):
        tiles[pl.ds(mine + TOK + SUB * j, SUB)] = dw_in[:, LANE * j : LANE * j + LANE].reshape(SUB, 8, LANE)
    streams = [(TOK * s, 1, ORDERS[s]) for s in range(3)]
    sent += [give_x, give_pre, give_dh]
    scatter = Scatter(me, tiles, core * HALF, trecv, 0, streams, send_sem.at[1], recv_sem.at[1])
    for s in range(3):
        scatter.send(s)
    scatter.rest()
    sent += scatter.sent
    streams = []
    for s in range(3):
        own = core * HALF + TOK * s + block_index(me, ORDERS[s])
        whole[own] = tiles[own]
        streams.append((whole, core * HALF + TOK * s, 1, ORDERS[s]))
    def leave(c):
        where = pl.ds(c * HALF, HALF)
        return pltpu.make_async_copy(whole.at[where], tiles_out.at[where], load_sem.at[10 + c])

    def push(phase):
        if phase == 3:
            leave(core).start()

    sent += gather_streams(me, streams, [(whole, HALF)], send_sem.at[2], recv_sem.at[2], push)
    leave(1 - core).start()
    dcand_copy.wait()
    for c in sent:
        c.wait_send()

    def swap_done(i, carry):
        swap(i).wait_send()
        return carry

    repeat(8, swap_done)
    leave(core).wait()
    leave(1 - core).wait()


def vmem(n):
    return [pl.BlockSpec(memory_space=pltpu.VMEM)] * n


def params(cid):
    return pltpu.CompilerParams(collective_id=cid, has_side_effects=True, vmem_limit_bytes=63 * KILO * KILO)


def dma(*shape):
    return pltpu.SemaphoreType.DMA(shape)


def solution(mesh):
    num_dev = mesh.shape["dp"]

    def local_step(features, w_in, w_out, table_blk, cand_ids, log_q, targets):
        dev_index = lax.axis_index("dp")
        block_rows = table_blk.shape[0]
        cand_dev = cand_ids.shape[0] // num_dev
        tok_total = features.shape[0] * num_dev
        anyspec = pl.BlockSpec(memory_space=pl.ANY)
        cid_rows, logq_rows = cand_ids.reshape(KILO, LANE), log_q.reshape(KILO, LANE)
        tgt_all, h_all, pre, cand_rows, cand_t, cidb, logqb = pl.pallas_call(
            query_kernel,
            out_shape=[
                jax.ShapeDtypeStruct((TOK, LANE), jnp.int32), jax.ShapeDtypeStruct((KILO, 8, LANE), BF16), jax.ShapeDtypeStruct((2, TOK, PART), F32),
                jax.ShapeDtypeStruct((cand_dev, LANE), BF16), jax.ShapeDtypeStruct((LANE, cand_dev), BF16),
                jax.ShapeDtypeStruct((cand_dev, LANE), F32), jax.ShapeDtypeStruct((cand_dev, LANE), F32)],
            in_specs=[anyspec] * 3 + vmem(1) + [anyspec] * 3, out_specs=vmem(1) + [anyspec] * 6,
            scratch_shapes=[
                pltpu.VMEM((LANE, 1, TOK), jnp.int32), pltpu.VMEM((LANE, TOK), jnp.int32),
                pltpu.VMEM(features.shape, BF16), pltpu.VMEM(w_in.shape, BF16), pltpu.VMEM(w_out.shape, BF16),
                pltpu.VMEM((block_rows, LANE), BF16), pltpu.VMEM((8, LANE), jnp.int32), pltpu.VMEM((8, LANE), F32), pltpu.VMEM((cand_dev, LANE), F32),
                pltpu.VMEM((KILO, 8, LANE), BF16), pltpu.VMEM((2, TOK, PART), F32), pltpu.VMEM((cand_dev, LANE), BF16), pltpu.VMEM((LANE, cand_dev), BF16),
                pltpu.VMEM((cand_dev, LANE), F32), pltpu.VMEM((cand_dev, LANE), F32),
                dma(6), dma(7), dma(4 * NPEER), dma(4 * NPEER)],
            compiler_params=params(0), name="query_gather",
        )(features, w_in, w_out, targets[None, :], table_blk, cid_rows, logq_rows)
        query_all = h_all.reshape(ALL, LANE)
        smem = pl.BlockSpec(memory_space=pltpu.SMEM)
        square = pltpu.VMEM((LANE, LANE), F32)
        big = pltpu.CompilerParams(vmem_limit_bytes=63 * KILO * KILO)
        zst, pos, codes, local, hc, te = pl.pallas_call(
            target_kernel,
            out_shape=[
                jax.ShapeDtypeStruct((TOK, LANE), F32), jax.ShapeDtypeStruct((TOK, LANE), F32), jax.ShapeDtypeStruct((TOK, LANE), jnp.int32), jax.ShapeDtypeStruct((TOK, LANE), F32),
                jax.ShapeDtypeStruct((tok_total, LANE), F32), jax.ShapeDtypeStruct((tok_total, LANE), F32)],
            in_specs=vmem(1) + [anyspec] * 2, out_specs=vmem(4) + [anyspec] * 2,
            scratch_shapes=[
                pltpu.VMEM((tok_total, LANE), BF16), pltpu.VMEM((block_rows, LANE), BF16), pltpu.VMEM((tok_total + 8, LANE), F32), pltpu.VMEM((TOK, LANE), F32),
                square, square, pltpu.SMEM((TOK, LANE), jnp.int32), dma(4), pltpu.SemaphoreType.DMA],
            compiler_params=big, name="target_rows",
        )(tgt_all, query_all, table_blk)
        grad_tgt, loss_row, tiles, dcand = pl.pallas_call(
            grad_kernel,
            out_shape=[
                jax.ShapeDtypeStruct((TOK, LANE), F32), jax.ShapeDtypeStruct((8, LANE), F32),
                jax.ShapeDtypeStruct((384, 8, LANE), F32), jax.ShapeDtypeStruct((cand_dev, LANE), F32)],
            in_specs=vmem(2) + [anyspec] * 9, out_specs=vmem(2) + [anyspec] * 2,
            scratch_shapes=[
                pltpu.VMEM((16, cand_dev, PART), F32), pltpu.VMEM((TOK, 8, LANE), F32), pltpu.VMEM((4, 8, LANE), F32), pltpu.VMEM((8, LANE), F32),
                pltpu.VMEM((80, 3, 8, LANE), F32), pltpu.VMEM((40, 3, 8, LANE), F32), pltpu.VMEM((TOK, LANE), F32),
                pltpu.VMEM((KILO, 8, LANE), F32), pltpu.VMEM((KILO, 8, LANE), F32),
                pltpu.VMEM((384, 8, LANE), F32), pltpu.VMEM((384, 8, LANE), F32), pltpu.VMEM((384, 8, LANE), F32), pltpu.VMEM((cand_dev, LANE), F32),
                pltpu.VMEM((tok_total, LANE), BF16), pltpu.VMEM((cand_dev, LANE), BF16), pltpu.VMEM((cand_dev, LANE), F32), pltpu.VMEM((cand_dev, LANE), F32),
                pltpu.VMEM((LANE, cand_dev), BF16), pltpu.VMEM((tok_total, LANE), F32),
                pltpu.VMEM(features.shape, BF16), pltpu.VMEM(w_out.shape, BF16), pltpu.VMEM(pre.shape, F32),
                pltpu.VMEM(features.shape, BF16), pltpu.VMEM((TOK, PART), F32), pltpu.VMEM((8, 8, LANE), BF16), pltpu.VMEM((8, 8, LANE), BF16),
                dma(12), dma(8), dma(8), dma(4, 3 * NPEER), dma(4, 3 * NPEER)],
            compiler_params=params(1), name="grad_reduce",
        )(local, zst, query_all, cand_rows, cidb, logqb, cand_t, te, features, w_out, pre)
        grad_blk, grad_w_in, grad_w_out, loss = pl.pallas_call(
            table_kernel,
            out_shape=[
                jax.ShapeDtypeStruct((block_rows, LANE), F32), jax.ShapeDtypeStruct(w_in.shape, F32), jax.ShapeDtypeStruct(w_out.shape, F32),
                jax.ShapeDtypeStruct((1, 1), F32)],
            in_specs=[smem] + vmem(3) + [anyspec] * 4, out_specs=vmem(1) + [anyspec] * 2 + [smem],
            scratch_shapes=[pltpu.SMEM((8, LANE), jnp.int32), pltpu.VMEM((cand_dev, LANE), F32), pltpu.VMEM((384, 8, LANE), F32), square, square, pltpu.VMEM(w_in.shape, F32), pltpu.VMEM(w_out.shape, F32), dma(6)],
            compiler_params=big, name="table_grad",
        )(codes, grad_tgt, pos, loss_row, cid_rows, dcand, tiles, hc)
        loss = loss.reshape(())
        return loss, grad_blk, grad_w_in, grad_w_out

    return jax.shard_map(local_step, mesh=mesh, in_specs=(P("dp", None), P(), P(), P("dp", None), P(), P(), P("dp")), out_specs=(P(), P("dp", None), P(), P()), check_vma=False)
```
